256 devices in a mesh: head: 4 (over y_hi, core), seq: 64 (over x, y_lo, z).
Axes of the slice: x: 4, y: 4 (y_hi: 2, y_lo: 2; y = y_hi * 2 + y_lo), z: 8, core: 2. Of those that a mesh axis runs over, the one named last changes fastest.
Arguments:
- keys: bfloat16 [12288, 2560], P('seq', 'head'), may hold values from -6 to 6
- values: bfloat16 [12288, 2560], P('seq', 'head'), may hold values from -6 to 6
- queries: bfloat16 [12288, 2560], P('seq', 'head'), may hold values from -6 to 6
- step_size: float32 [12288, 2], P('seq'), may hold values from 7.564421e-05 to 0.0007564421
- gate_weight: bfloat16 [1280, 3072], P('seq', 'head'), may hold values from -1 to 1
- up_weight: bfloat16 [1280, 3072], P('seq', 'head'), may hold values from -1 to 1
- down_weight: bfloat16 [1280, 3072], P('seq', 'head'), may hold values from -1 to 1
Outputs:
- mixed: bfloat16 [12288, 2560], P('seq', 'head')
The draws below stay inside these ranges and needn't reach their ends.
All inputs are finite; a program needn't handle non-finite values.
Results may differ from the reference program's by a relative error of at most 0.0066.
Values may be sent and summed in bfloat16 or wider, within the bound.
A program may use at most 128 MiB of HBM per device.

```python
import math
import jax
import jax.numpy as jnp
from jax import lax

HEADS = 2
DH = 1280
UNITS = 1536
GROUP = 12288


def fast_weight(key, salt, fan_in):
    mixed_key = jax.random.fold_in(key, salt)
    base_key, rows_key = jax.random.split(mixed_key, 2)
    column_total = HEADS * UNITS
    base = jnp.clip(jax.random.normal(base_key, (DH, column_total), jnp.float32), -6.0, 6.0)
    ramp = jnp.arange(DH, dtype=jnp.float32) / (DH - 1)
    row_scale = (10.0 ** ramp)[:, None] * jnp.exp(jax.random.uniform(rows_key, (DH, 1), jnp.float32, -0.35, 0.35))
    scaled = base * row_scale / jnp.sqrt(jnp.mean(row_scale * row_scale))
    scaled = scaled / jnp.sqrt(jnp.float32(fan_in))
    return jnp.clip(scaled, -1.0, 1.0).astype(jnp.bfloat16)


def draw_gate_weight(key, part):
    return fast_weight(key, 101, DH)


def draw_up_weight(key, part):
    return fast_weight(key, 202, DH)


def draw_down_weight(key, part):
    return fast_weight(key, 303, UNITS)


def draw_values(key, part):
    mixed_key = jax.random.fold_in(key, 404)
    noise_key, direction_key, token_key = jax.random.split(mixed_key, 3)
    width = HEADS * DH
    noise = jnp.clip(jax.random.normal(noise_key, (GROUP, width), jnp.float32), -6.0, 6.0)
    strength = 0.5
    direction = jnp.clip(jax.random.normal(direction_key, (1, width), jnp.float32), -4.0, 4.0)
    token_weight = jax.random.uniform(token_key, (GROUP, 1), jnp.float32, 0.5, 1.5)
    combined = noise + strength * token_weight * direction
    return jnp.clip(combined, -6.0, 6.0).astype(jnp.bfloat16)


def levels(key, dims, pieces, smallest, largest):
    factor_of = 1.0
    for dim, shards_of in pieces:
        draws = jax.random.uniform(jax.random.fold_in(jax.random.fold_in(key, 6), dim), (shards_of,), jnp.float32, smallest / len(pieces), largest / len(pieces))
        factor_of = factor_of * jnp.repeat(jnp.exp(draws), dims[dim] // shards_of).reshape((-1,) + (1,) * (len(dims) - 1 - dim))
    return factor_of


def centred(own_key, dims, scale, bound, shards=(), kind=jnp.bfloat16):
    gain = levels(own_key, dims, shards, -0.22, 0.18) if shards else 1.0
    values = jax.random.normal(own_key, dims, jnp.float32) * scale * gain
    return jnp.minimum(jnp.maximum(values, -bound), bound).astype(kind)


def setup_inputs(seed: int = 0) -> dict:
    arg_keys = jax.random.split(jax.random.key(seed), 8)
    return {
        "keys": centred(arg_keys[0], (GROUP, HEADS * DH), 1.0, 6.0, ((0, 64), (1, 4))),
        "values": draw_values(jax.random.fold_in(arg_keys[7], 71), 0),
        "queries": centred(arg_keys[2], (GROUP, HEADS * DH), 1.0, 6.0, ((0, 64), (1, 4))),
        "step_size": jnp.clip(jnp.exp(math.log(0.0007564421) - 2.3025851 * jax.random.uniform(arg_keys[3], (GROUP, HEADS), jnp.float32) ** levels(arg_keys[3], (GROUP, HEADS), ((0, 64),), -0.2, 0.2)), 7.564420957351103e-05, 0.0007564421),
        "gate_weight": draw_gate_weight(jax.random.fold_in(arg_keys[7], 71), 0),
        "up_weight": draw_up_weight(jax.random.fold_in(arg_keys[7], 71), 0),
        "down_weight": draw_down_weight(jax.random.fold_in(arg_keys[7], 71), 0),
    }


epsilon = 1e-06

def silu_slope(values_in):
    sigma = jax.nn.sigmoid(values_in)
    return sigma * (1.0 + values_in * (1.0 - sigma))

def norm_ratio(old_matrix, new_matrix):
    old_sums = lax.optimization_barrier(jnp.sum(jnp.square(old_matrix.astype(jnp.float32)), axis=0))
    new_sums = lax.optimization_barrier(jnp.sum(jnp.square(new_matrix.astype(jnp.float32)), axis=0))
    return jnp.sqrt((old_sums + epsilon) / (new_sums + epsilon))

def one_head(key_block, value_block, query_block, rates, weight_gate, weight_up, weight_down):
    gate_act = jnp.dot(key_block, weight_gate, preferred_element_type=jnp.float32)
    up_act = jnp.dot(key_block, weight_up, preferred_element_type=jnp.float32)
    silu_gate = jax.nn.silu(gate_act)
    hidden = (silu_gate * up_act).astype(jnp.bfloat16)
    outgrad = (-(rates * value_block.astype(jnp.float32))).astype(jnp.bfloat16)
    hidden_grad = jnp.dot(outgrad, weight_down, preferred_element_type=jnp.float32)
    gate_grad = (hidden_grad * up_act * silu_slope(gate_act)).astype(jnp.bfloat16)
    up_grad = (hidden_grad * silu_gate).astype(jnp.bfloat16)
    grad_gate = jnp.dot(key_block.T, gate_grad, preferred_element_type=jnp.float32)
    grad_up = jnp.dot(key_block.T, up_grad, preferred_element_type=jnp.float32)
    grad_down = jnp.dot(outgrad.T, hidden, preferred_element_type=jnp.float32)
    new_gate = (weight_gate.astype(jnp.float32) - grad_gate).astype(jnp.bfloat16)
    new_up = (weight_up.astype(jnp.float32) - grad_up).astype(jnp.bfloat16)
    new_down = (weight_down.astype(jnp.float32) - grad_down).astype(jnp.bfloat16)
    ratio_gate = norm_ratio(weight_gate, new_gate)
    ratio_up = norm_ratio(weight_up, new_up)
    ratio_down = norm_ratio(weight_down, new_down)
    query_gate = jnp.dot(query_block, new_gate, preferred_element_type=jnp.float32) * ratio_gate
    query_up = jnp.dot(query_block, new_up, preferred_element_type=jnp.float32) * ratio_up
    query_hidden = (jax.nn.silu(query_gate) * query_up * ratio_down).astype(jnp.bfloat16)
    return jnp.dot(query_hidden, new_down.T, preferred_element_type=jnp.float32).astype(jnp.bfloat16)

def reference(keys, values, queries, step_size, gate_weight, up_weight, down_weight):
    results = []
    for head_index in range(HEADS):
        feature_lo = head_index * DH
        unit_lo = head_index * UNITS
        results.append(one_head(keys[:, feature_lo:feature_lo + DH], values[:, feature_lo:feature_lo + DH], queries[:, feature_lo:feature_lo + DH], step_size[:, head_index:head_index + 1], gate_weight[:, unit_lo:unit_lo + UNITS], up_weight[:, unit_lo:unit_lo + UNITS], down_weight[:, unit_lo:unit_lo + UNITS]))
    return jnp.concatenate(results, axis=1)
```

```python
import jax
import jax.numpy as jnp
from jax import lax
from jax.experimental import pallas as pl
from jax.experimental.pallas import tpu as pltpu
from jax.sharding import Mesh
from jax.sharding import PartitionSpec as P

EPS = 1e-06
MESH = pl.DeviceIdType.MESH
F32 = jnp.float32
BF16 = jnp.bfloat16

NX, NZ = 4, 8
TOK = 192
DC = 640
U = 384
ROWS = 80
PIECE = 20
PADDED = 32
HALF = TOK // 2
HR = (48, 32, 48)
OPP, LEFT, RIGHT, OWN = 0, 1, 2, 3


def dot(a, b):
    return jnp.dot(a, b, preferred_element_type=F32)


def dot_nt(a, b):
    return lax.dot_general(a, b, (((1,), (1,)), ((), ())), preferred_element_type=F32)


def square_sums(v):
    f = v.astype(F32)
    return jnp.sum(f * f, axis=0, keepdims=True)


def kernel(
    k_ref, v_ref, q_ref, s_ref, w1_ref, w3_ref, w2_ref, out_ref,
    wsend, warr, wg, perm, wcur, kbuf, obuf, qbuf, kt, ot, ps, pr, gg, hid, gbuf,
    rss, rsr, ys, yr, nw, sms, smr, qs, qr, qh, ob, obr, fin, send_sem, recv_sem, loc_sem,
):
    yh = lax.axis_index("yh")
    c = lax.axis_index("core")
    x = lax.axis_index("x")
    y = lax.axis_index("yl")
    z = lax.axis_index("z")
    xr, xl = {"x": lax.rem(x + 1, NX)}, {"x": lax.rem(x + NX - 1, NX)}
    zr, zl = {"z": lax.rem(z + 1, NZ)}, {"z": lax.rem(z + NZ - 1, NZ)}
    peer, ypeer = {"core": 1 - c}, {"yl": 1 - y}
    xhalf = x // 2
    xlow = lax.rem(x, 2)
    own_w = xhalf == c

    def wtarget(j, dy):
        return {"x": 2 * c + j, "core": xhalf, "yl": y if dy == 0 else 1 - y}

    counter = [0]
    sends = []

    def ids(n):
        first = counter[0]
        counter[0] += n
        return first

    def copy(src, dst, k, to):
        return pltpu.make_async_remote_copy(
            src_ref=src, dst_ref=dst, send_sem=send_sem.at[k], recv_sem=recv_sem.at[k],
            device_id=to, device_id_type=MESH,
        )

    def send(src, dst, k, to):
        cp = copy(src, dst, k, to)
        cp.start()
        sends.append(cp)

    def arrived(ref, k, frm):
        copy(ref, ref, k, frm).wait_recv()

    barrier = pltpu.get_barrier_semaphore()
    for to in (peer, xr, xl, zr, zl, ypeer, wtarget(0, 1), wtarget(1, 1)):
        pl.semaphore_signal(barrier, inc=1, device_id=to, device_id_type=MESH)
    for j in range(2):
        @pl.when(jnp.logical_not(jnp.logical_and(own_w, xlow == j)))
        def _():
            pl.semaphore_signal(barrier, inc=1, device_id=wtarget(j, 0), device_id_type=MESH)

    wsend[...] = jnp.zeros_like(wsend)
    for m, w in enumerate((w1_ref, w3_ref, w2_ref)):
        for j in range(2):
            wsend[j, 0:PIECE, m * U:(m + 1) * U] = w[:, j * U:(j + 1) * U]
    pl.semaphore_wait(barrier, 10 - jnp.where(own_w, 1, 0))

    k_w = ids(4)
    slot = 2 * xlow + y
    w_copies = []
    for j in range(2):
        for dy in (1, 0):
            cp = pltpu.make_async_remote_copy(
                src_ref=wsend.at[j], dst_ref=warr.at[slot],
                send_sem=send_sem.at[k_w + 2 * j + dy], recv_sem=recv_sem.at[k_w + slot],
                device_id=wtarget(j, dy), device_id_type=MESH,
            )
            if dy == 1:
                cp.start()
                sends.append(cp)
            else:
                is_self = jnp.logical_and(own_w, xlow == j)
                w_copies.append((is_self, cp))
                lc = pltpu.make_async_copy(wsend.at[j], warr.at[slot], loc_sem.at[j])
                pl.when(jnp.logical_not(is_self))(cp.start)

                @pl.when(is_self)
                def _():
                    lc.start()
                    lc.wait()

    def x_out(src, buf, k):
        send(src, buf.at[LEFT], k, xr)
        send(src, buf.at[RIGHT], k + 1, xl)

    def x_relay(buf, k):
        arrived(buf.at[LEFT], k, xl)
        send(buf.at[LEFT, 0:HALF], buf.at[OPP, 0:HALF], k + 2, xr)
        arrived(buf.at[RIGHT], k + 1, xr)
        send(buf.at[RIGHT, HALF:TOK], buf.at[OPP, HALF:TOK], k + 3, xl)

    def x_last(buf, k):
        arrived(buf.at[OPP, 0:HALF], k + 2, xl)
        arrived(buf.at[OPP, HALF:TOK], k + 3, xr)

    k_k, k_o, k_q = ids(4), ids(4), ids(4)
    x_out(k_ref, kbuf, k_k)
    rates = jnp.where(yh == 0, s_ref[:, 0:1], s_ref[:, 1:2])
    obuf[OWN] = (-(rates * v_ref[...].astype(F32))).astype(BF16)
    x_out(obuf.at[OWN], obuf, k_o)
    kbuf[OWN] = k_ref[...]
    qbuf[OWN] = q_ref[...]

    row = lax.broadcasted_iota(jnp.int32, (DC, DC), 0)
    col = lax.broadcasted_iota(jnp.int32, (DC, DC), 1)
    group = (row >= 160).astype(jnp.int32) + (row >= 320).astype(jnp.int32) + (row >= 480).astype(jnp.int32)
    rem = row - 160 * group
    step20 = jnp.zeros_like(rem)
    for t in range(1, NZ):
        step20 = step20 + (rem >= PIECE * t).astype(jnp.int32)
    wanted = ROWS * step20 + PIECE * group + rem - PIECE * step20
    perm[...] = jnp.where(col == wanted, 1.0, 0.0).astype(BF16)

    for s in range(4):
        from_x, from_y = s // 2, s % 2
        here = jnp.logical_and(jnp.logical_and(own_w, xlow == from_x), y == from_y)

        @pl.when(jnp.logical_not(here))
        def _():
            copy(warr.at[s], warr.at[s], k_w + s, ypeer).wait_recv()

    prow = lax.broadcasted_iota(jnp.int32, (ROWS, 4 * PADDED), 0)
    pcol = lax.broadcasted_iota(jnp.int32, (ROWS, 4 * PADDED), 1)
    pgroup = (prow >= 20).astype(jnp.int32) + (prow >= 40).astype(jnp.int32) + (prow >= 60).astype(jnp.int32)
    pack = jnp.where(pcol == prow + (PADDED - PIECE) * pgroup, 1.0, 0.0).astype(BF16)
    packed = dot(pack, warr[...].reshape(4 * PADDED, 3 * U)).astype(BF16)
    for m in range(3):
        wg[z, m] = packed[:, m * U:(m + 1) * U]

    def part(buf, at, m, step, way):
        if step < 4:
            return buf.at[at, m]
        lo, hi = (0, HR[m]) if way == 0 else (HR[m], ROWS)
        return buf.at[at, m, lo:hi]

    def zpos(off):
        return lax.rem(z + off + 2 * NZ, NZ)

    def ring_send(buf, k, step, m):
        for way, (sign, to) in enumerate(((-1, zr), (1, zl))):
            ref = part(buf, zpos(sign * (step - 1)), m, step, way)
            send(ref, ref, k + (step - 1) * 6 + 2 * m + way, to)

    def ring_arrived(buf, k, step, m):
        for way, (sign, frm) in enumerate(((-1, zl), (1, zr))):
            ref = part(buf, zpos(sign * step), m, step, way)
            arrived(ref, k + (step - 1) * 6 + 2 * m + way, frm)

    k_g = ids(24)
    for m in range(3):
        ring_send(wg, k_g, 1, m)
    for step in range(2, 5):
        for m in range(3):
            ring_arrived(wg, k_g, step - 1, m)
            ring_send(wg, k_g, step, m)
        if step == 2:
            x_relay(kbuf, k_k)
        if step == 3:
            x_relay(obuf, k_o)
            x_out(q_ref, qbuf, k_q)
            x_last(kbuf, k_k)
            for h in range(2):
                kt[:, h * U:(h + 1) * U] = kbuf[2 * h:2 * h + 2].reshape(2 * TOK, DC).T
    for m in range(3):
        ring_arrived(wg, k_g, 4, m)
    for m in range(3):
        wcur[:, m * U:(m + 1) * U] = dot(perm[...], wg[:, m].reshape(DC, U)).astype(BF16)
    x_last(obuf, k_o)

    k_p = ids(4)

    def p_copy(b):
        return copy(ps.at[b], pr.at[b], k_p + b, peer)

    @pl.loop(0, 4)
    def _(b):
        ps[b, :, 0:2 * U] = dot(kbuf[b], wcur[:, 0:2 * U])
        ps[b, :, 2 * U:3 * U] = dot(obuf[b], wcur[:, 2 * U:3 * U])
        p_copy(b).start()

    for h in range(2):
        ot[:, h * U:(h + 1) * U] = obuf[2 * h:2 * h + 2].reshape(2 * TOK, DC).T

    @pl.loop(0, 4)
    def _(b):
        p_copy(b).wait_recv()

        @pl.loop(0, TOK // 16)
        def _(t):
            r = pl.ds(pl.multiple_of(t * 16, 16), 16)
            o = pl.ds(pl.multiple_of(b * TOK + t * 16, 16), 16)
            gate = ps[b, r, 0:U] + pr[b, r, 0:U]
            up = ps[b, r, U:2 * U] + pr[b, r, U:2 * U]
            hg = ps[b, r, 2 * U:3 * U] + pr[b, r, 2 * U:3 * U]
            sg = jax.nn.sigmoid(gate)
            silu = gate * sg
            hid[o, :] = (silu * up).astype(BF16)
            gg[o, 0:U] = (hg * up * (sg * (1.0 + gate * (1.0 - sg)))).astype(BF16)
            gg[o, U:2 * U] = (hg * silu).astype(BF16)

    k_r = ids(24)

    def rs_id(step, m, way):
        return k_r + (step - 1) * 6 + 2 * m + way

    far = pl.ds(pl.multiple_of(zpos(4) * ROWS, 16), ROWS)
    g13 = dot(kt[far, :], gg[...])
    g2 = dot(ot[far, :], hid[...])
    for m, g in enumerate((g13[:, 0:U], g13[:, U:2 * U], g2)):
        rss[0, 0, m] = g.astype(BF16)
        for way, to in enumerate((zr, zl)):
            lo, hi = (0, HR[m]) if way == 0 else (HR[m], ROWS)
            send(rss.at[0, 0, m, lo:hi], rsr.at[way, 0, m, lo:hi], rs_id(1, m, way), to)
    for m in range(3):
        g = dot(kt[...], gg[:, m * U:(m + 1) * U]) if m < 2 else dot(ot[...], hid[...])
        gbuf[:, m] = g.reshape(NZ, ROWS, U)

    for step in range(2, 5):
        for m in range(3):
            for way, (sign, to, frm) in enumerate(((1, zr, zl), (-1, zl, zr))):
                at = zpos(sign * (5 - step))
                if step == 2:
                    lo, hi = (0, HR[m]) if way == 0 else (HR[m], ROWS)
                    olo, ohi = (HR[m], ROWS) if way == 0 else (0, HR[m])
                    arrived(rsr.at[way, 0, m, lo:hi], rs_id(1, m, way), frm)
                    rss[way, 1, m, lo:hi] = (gbuf[at, m, lo:hi] + rsr[way, 0, m, lo:hi].astype(F32)).astype(BF16)
                    rss[way, 1, m, olo:ohi] = gbuf[at, m, olo:ohi].astype(BF16)
                else:
                    arrived(rsr.at[way, step - 2, m], rs_id(step - 1, m, way), frm)
                    rss[way, step - 1, m] = (gbuf[at, m] + rsr[way, step - 2, m].astype(F32)).astype(BF16)
                send(rss.at[way, step - 1, m], rsr.at[way, step - 1, m], rs_id(step, m, way), to)
        if step == 2:
            old = [square_sums(wcur[:, m * U:(m + 1) * U]) for m in range(3)]
            for m in range(3):
                sms[m:m + 1, :] = old[m]
        if step == 3:
            x_relay(qbuf, k_q)

    k_y = ids(3)
    for m in range(3):
        for way, frm in enumerate((zl, zr)):
            arrived(rsr.at[way, 3, m], rs_id(4, m, way), frm)
        total = gbuf[z, m] + rsr[0, 3, m].astype(F32) + rsr[1, 3, m].astype(F32)
        gbuf[z, m] = total
        ys[m] = total.astype(BF16)
        send(ys.at[m], yr.at[m], k_y + m, ypeer)
    x_last(qbuf, k_q)
    own_rows = pl.ds(pl.multiple_of(z * ROWS, 16), ROWS)
    k_n = ids(24)
    new_sums = []
    for m in range(3):
        arrived(yr.at[m], k_y + m, ypeer)
        old_w = wcur[own_rows, m * U:(m + 1) * U].astype(F32)
        nw[z, m] = (old_w - (gbuf[z, m] + yr[m].astype(F32))).astype(BF16)
        ring_send(nw, k_n, 1, m)
        new_sums.append(square_sums(nw[z, m]))
    for step in range(2, 6):
        for m in range(3):
            ring_arrived(nw, k_n, step - 1, m)
            if step < 5:
                ring_send(nw, k_n, step, m)
                for sign in (-1, 1):
                    new_sums[m] = new_sums[m] + square_sums(nw[zpos(sign * (step - 1)), m])
            else:
                new_sums[m] = new_sums[m] + square_sums(nw[zpos(4), m])
    for m in range(3):
        sms[3 + m:4 + m, :] = new_sums[m]
    sms[6:8, :] = jnp.zeros((2, U), F32)
    k_s = ids(1)
    send(sms, smr, k_s, peer)

    k_qp = ids(4)

    def q_copy(b):
        return copy(qs.at[b], qr.at[b], k_qp + b, peer)

    @pl.loop(0, 4)
    def _(b):
        for m in range(2):
            qs[b, :, m * U:(m + 1) * U] = dot(qbuf[b], nw[:, m].reshape(DC, U))
        q_copy(b).start()

    arrived(smr, k_s, peer)
    sums = sms[...] + smr[...]
    r1, r3, r2 = [jnp.sqrt((sums[m:m + 1] + EPS) / (sums[3 + m:4 + m] + EPS)) for m in range(3)]

    k_x = ids(4)
    for b in range(4):
        q_copy(b).wait_recv()

        @pl.loop(0, TOK // 16)
        def _(t):
            r = pl.ds(pl.multiple_of(t * 16, 16), 16)
            qg = (qs[b, r, 0:U] + qr[b, r, 0:U]) * r1
            qu = (qs[b, r, U:2 * U] + qr[b, r, U:2 * U]) * r3
            qh[b, r, :] = (qg * jax.nn.sigmoid(qg) * qu * r2).astype(BF16)

        part_out = dot_nt(qh[b], nw[:, 2].reshape(DC, U))
        if b == OPP:
            ob[OPP] = part_out.astype(BF16)
            send(ob.at[OPP, 0:HALF], obr.at[0:HALF], k_x, xr)
            send(ob.at[OPP, HALF:TOK], obr.at[HALF:TOK], k_x + 1, xl)
        elif b == LEFT:
            ob[LEFT, 0:HALF] = part_out[0:HALF].astype(BF16)
            arrived(obr.at[HALF:TOK], k_x + 1, xr)
            ob[LEFT, HALF:TOK] = (part_out[HALF:TOK] + obr[HALF:TOK].astype(F32)).astype(BF16)
            send(ob.at[LEFT], fin.at[1], k_x + 2, xl)
        elif b == RIGHT:
            ob[RIGHT, HALF:TOK] = part_out[HALF:TOK].astype(BF16)
            arrived(obr.at[0:HALF], k_x, xl)
            ob[RIGHT, 0:HALF] = (part_out[0:HALF] + obr[0:HALF].astype(F32)).astype(BF16)
            send(ob.at[RIGHT], fin.at[0], k_x + 3, xr)
        else:
            arrived(fin.at[1], k_x + 2, xr)
            arrived(fin.at[0], k_x + 3, xl)
            out_ref[...] = (part_out + fin[0].astype(F32) + fin[1].astype(F32)).astype(BF16)

    for cp in sends:
        cp.wait_send()
    for is_self, cp in w_copies:
        pl.when(jnp.logical_not(is_self))(cp.wait_send)

    @pl.loop(0, 4)
    def _(b):
        p_copy(b).wait_send()
        q_copy(b).wait_send()


N_SEM = 4 + 12 + 24 + 4 + 24 + 3 + 24 + 1 + 4 + 4


def body(keys, values, queries, step_size, gate_weight, up_weight, down_weight):
    vmem = pl.BlockSpec(memory_space=pltpu.VMEM)
    return pl.pallas_call(
        kernel,
        out_shape=jax.ShapeDtypeStruct((TOK, DC), BF16),
        in_specs=[vmem] * 7,
        out_specs=vmem,
        scratch_shapes=[
            pltpu.VMEM((2, PADDED, 3 * U), BF16),
            pltpu.VMEM((4, PADDED, 3 * U), BF16),
            pltpu.VMEM((NZ, 3, ROWS, U), BF16),
            pltpu.VMEM((DC, DC), BF16),
            pltpu.VMEM((DC, 3 * U), BF16),
            pltpu.VMEM((4, TOK, DC), BF16),
            pltpu.VMEM((4, TOK, DC), BF16),
            pltpu.VMEM((4, TOK, DC), BF16),
            pltpu.VMEM((DC, 4 * TOK), BF16),
            pltpu.VMEM((DC, 4 * TOK), BF16),
            pltpu.VMEM((4, TOK, 3 * U), F32),
            pltpu.VMEM((4, TOK, 3 * U), F32),
            pltpu.VMEM((4 * TOK, 2 * U), BF16),
            pltpu.VMEM((4 * TOK, U), BF16),
            pltpu.VMEM((NZ, 3, ROWS, U), F32),
            pltpu.VMEM((2, 4, 3, ROWS, U), BF16),
            pltpu.VMEM((2, 4, 3, ROWS, U), BF16),
            pltpu.VMEM((3, ROWS, U), BF16),
            pltpu.VMEM((3, ROWS, U), BF16),
            pltpu.VMEM((NZ, 3, ROWS, U), BF16),
            pltpu.VMEM((8, U), F32),
            pltpu.VMEM((8, U), F32),
            pltpu.VMEM((4, TOK, 2 * U), F32),
            pltpu.VMEM((4, TOK, 2 * U), F32),
            pltpu.VMEM((4, TOK, U), BF16),
            pltpu.VMEM((4, TOK, DC), BF16),
            pltpu.VMEM((TOK, DC), BF16),
            pltpu.VMEM((2, TOK, DC), BF16),
            pltpu.SemaphoreType.DMA((N_SEM,)),
            pltpu.SemaphoreType.DMA((N_SEM,)),
            pltpu.SemaphoreType.DMA((2,)),
        ],
        compiler_params=pltpu.CompilerParams(
            collective_id=0, has_side_effects=True, vmem_limit_bytes=60 << 20
        ),
        name="ttt_layer",
    )(keys, values, queries, step_size, gate_weight, up_weight, down_weight)


def solution(mesh):
    finer = Mesh(mesh.devices.reshape(2, 2, 4, 2, 8), ("yh", "core", "x", "yl", "z"))
    seq, head = ("x", "yl", "z"), ("yh", "core")
    placed = (
        P(seq, head), P(seq, head), P(seq, head), P(seq, None),
        P(seq, head), P(seq, head), P(seq, head),
    )
    return jax.shard_map(body, mesh=finer, in_specs=placed, out_specs=P(seq, head), check_vma=False)
```

```python
import jax
import jax.numpy as jnp
from jax import lax
from jax.experimental import pallas as pl
from jax.experimental.pallas import tpu as pltpu
from jax.sharding import Mesh
from jax.sharding import PartitionSpec as P

EPS = 1e-06
MESH = pl.DeviceIdType.MESH
F32 = jnp.float32
BF16 = jnp.bfloat16

NX, NZ = 4, 8
TOK = 192
DC = 640
U = 384
ROWS = 80
PIECE = 20
PADDED = 32
HALF = TOK // 2
CUT = ((0, 48), (48, ROWS))
CHUNKS = ((0, 0), (0, 1), (1, 0), (1, 1))
OPP, LEFT, RIGHT, OWN = 0, 1, 2, 3
STEP = 32


def dot(a, b):
    return jnp.dot(a, b, preferred_element_type=F32)


def dot_nt(a, b):
    return lax.dot_general(a, b, (((1,), (1,)), ((), ())), preferred_element_type=F32)


def square_sums(v):
    f = v.astype(F32)
    return jnp.sum(f * f, axis=0, keepdims=True)


def far_way(kind, h):
    return h if kind == 0 else 1 - h


def kernel(
    k_hbm, v_hbm, q_hbm, s_hbm, w1_hbm, w3_hbm, w2_hbm, out_ref,
    win, vin, sin, wsend, warr, wg, perm, wcur, kbuf, obuf, qbuf, kt, ot, ps, pr, gg, hid,
    ga, gb, ysf, ysend, yrecv, rss, rsr, ybs, ybr, nw, sms, smr, qs, qr, qh, ob, op, obr, fin,
    send_sem, recv_sem, loc_sem,
):
    yh = lax.axis_index("yh")
    c = lax.axis_index("core")
    x = lax.axis_index("x")
    y = lax.axis_index("yl")
    z = lax.axis_index("z")
    xr, xl = {"x": lax.rem(x + 1, NX)}, {"x": lax.rem(x + NX - 1, NX)}
    zr, zl = {"z": lax.rem(z + 1, NZ)}, {"z": lax.rem(z + NZ - 1, NZ)}
    peer, ypeer = {"core": 1 - c}, {"yl": 1 - y}
    xhalf = x // 2
    xlow = lax.rem(x, 2)
    own_w = xhalf == c

    def wtarget(j, dy):
        return {"x": 2 * c + j, "core": xhalf, "yl": y if dy == 0 else 1 - y}

    counter = [0]
    sends = []

    def ids(n):
        first = counter[0]
        counter[0] += n
        return first

    def copy(src, dst, k, to):
        return pltpu.make_async_remote_copy(
            src_ref=src, dst_ref=dst, send_sem=send_sem.at[k], recv_sem=recv_sem.at[k],
            device_id=to, device_id_type=MESH,
        )

    def send(src, dst, k, to):
        cp = copy(src, dst, k, to)
        cp.start()
        sends.append(cp)

    def arrived(ref, k, frm):
        copy(ref, ref, k, frm).wait_recv()

    barrier = pltpu.get_barrier_semaphore()
    for to in (peer, xr, xl, zr, zl, ypeer, wtarget(0, 1), wtarget(1, 1)):
        pl.semaphore_signal(barrier, inc=1, device_id=to, device_id_type=MESH)
    for j in range(2):
        @pl.when(jnp.logical_not(jnp.logical_and(own_w, xlow == j)))
        def _():
            pl.semaphore_signal(barrier, inc=1, device_id=wtarget(j, 0), device_id_type=MESH)

    loads = [
        pltpu.make_async_copy(w1_hbm, win.at[0], loc_sem.at[0]),
        pltpu.make_async_copy(w3_hbm, win.at[1], loc_sem.at[1]),
        pltpu.make_async_copy(w2_hbm, win.at[2], loc_sem.at[2]),
        pltpu.make_async_copy(k_hbm, kbuf.at[OWN], loc_sem.at[3]),
        pltpu.make_async_copy(v_hbm, vin, loc_sem.at[4]),
        pltpu.make_async_copy(s_hbm, sin, loc_sem.at[5]),
        pltpu.make_async_copy(q_hbm, qbuf.at[OWN], loc_sem.at[6]),
    ]
    for ld in loads:
        ld.start()

    wsend[...] = jnp.zeros_like(wsend)
    for m in range(3):
        loads[m].wait()
    for j in range(2):
        for t in range(2):
            wsend[j, t, 0:PIECE, 0:U] = win[t, :, j * U:(j + 1) * U]
            wsend[j, t, 0:PIECE, U:2 * U] = win[2, :, j * U:(j + 1) * U]
    loads[3].wait()
    pl.semaphore_wait(barrier, 10 - jnp.where(own_w, 1, 0))

    k_w = ids(4)
    slot = 2 * xlow + y
    w_copies = []
    for j in range(2):
        for dy in (1, 0):
            block = wsend.at[j, y if dy == 0 else 1 - y]
            cp = pltpu.make_async_remote_copy(
                src_ref=block, dst_ref=warr.at[slot],
                send_sem=send_sem.at[k_w + 2 * j + dy], recv_sem=recv_sem.at[k_w + slot],
                device_id=wtarget(j, dy), device_id_type=MESH,
            )
            if dy == 1:
                cp.start()
                sends.append(cp)
            else:
                is_self = jnp.logical_and(own_w, xlow == j)
                w_copies.append((is_self, cp))
                lc = pltpu.make_async_copy(block, warr.at[slot], loc_sem.at[7 + j])
                pl.when(jnp.logical_not(is_self))(cp.start)

                @pl.when(is_self)
                def _():
                    lc.start()
                    lc.wait()

    def x_out(buf, k):
        send(buf.at[OWN], buf.at[LEFT], k, xr)
        send(buf.at[OWN], buf.at[RIGHT], k + 1, xl)

    def x_relay(buf, k):
        arrived(buf.at[LEFT], k, xl)
        send(buf.at[LEFT, 0:HALF], buf.at[OPP, 0:HALF], k + 2, xr)
        arrived(buf.at[RIGHT], k + 1, xr)
        send(buf.at[RIGHT, HALF:TOK], buf.at[OPP, HALF:TOK], k + 3, xl)

    def x_last(buf, k):
        arrived(buf.at[OPP, 0:HALF], k + 2, xl)
        arrived(buf.at[OPP, HALF:TOK], k + 3, xr)

    k_k, k_o, k_q = ids(4), ids(4), ids(4)
    x_out(kbuf, k_k)
    loads[4].wait()
    loads[5].wait()
    diag = lax.broadcasted_iota(jnp.int32, (TOK, TOK), 0) == lax.broadcasted_iota(jnp.int32, (TOK, TOK), 1)
    rate_row = jnp.where(yh == 0, sin[0:1, :], sin[1:2, :])
    rates = jnp.sum(jnp.where(diag, rate_row, 0.0), axis=1, keepdims=True)
    obuf[OWN] = (-(rates * vin[...].astype(F32))).astype(BF16)
    x_out(obuf, k_o)

    row = lax.broadcasted_iota(jnp.int32, (DC, DC), 0)
    col = lax.broadcasted_iota(jnp.int32, (DC, DC), 1)
    group = (row >= 160).astype(jnp.int32) + (row >= 320).astype(jnp.int32) + (row >= 480).astype(jnp.int32)
    rem = row - 160 * group
    step20 = jnp.zeros_like(rem)
    for t in range(1, NZ):
        step20 = step20 + (rem >= PIECE * t).astype(jnp.int32)
    wanted = ROWS * step20 + PIECE * group + rem - PIECE * step20
    perm[...] = jnp.where(col == wanted, 1.0, 0.0).astype(BF16)

    for s in range(4):
        from_x, from_y = s // 2, s % 2
        here = jnp.logical_and(jnp.logical_and(own_w, xlow == from_x), y == from_y)

        @pl.when(jnp.logical_not(here))
        def _():
            copy(warr.at[s], warr.at[s], k_w + s, ypeer).wait_recv()

    prow = lax.broadcasted_iota(jnp.int32, (ROWS, 4 * PADDED), 0)
    pcol = lax.broadcasted_iota(jnp.int32, (ROWS, 4 * PADDED), 1)
    pgroup = (prow >= 20).astype(jnp.int32) + (prow >= 40).astype(jnp.int32) + (prow >= 60).astype(jnp.int32)
    pack = jnp.where(pcol == prow + (PADDED - PIECE) * pgroup, 1.0, 0.0).astype(BF16)
    packed = dot(pack, warr[...].reshape(4 * PADDED, 2 * U)).astype(BF16)
    wg[z, y] = packed[:, 0:U]
    wg[z, 2] = packed[:, U:2 * U]

    def zpos(off):
        return lax.rem(z + off + 2 * NZ, NZ)

    def chunk(buf, at, kind, h):
        return buf.at[at, y if kind == 0 else 2, CUT[h][0]:CUT[h][1]]

    def ways(step, kind, h):
        return (0, 1) if step < 4 else (far_way(kind, h),)

    def ring_id(k, step, kind, h, way):
        return k + (step - 1) * 8 + 4 * kind + 2 * h + way

    def ring_send(buf, k, step, kind, h):
        for way in ways(step, kind, h):
            ref = chunk(buf, zpos((1 - step) if way == 0 else (step - 1)), kind, h)
            send(ref, ref, ring_id(k, step, kind, h, way), zr if way == 0 else zl)

    def ring_arrived(buf, k, step, kind, h):
        for way in ways(step, kind, h):
            ref = chunk(buf, zpos(-step if way == 0 else step), kind, h)
            arrived(ref, ring_id(k, step, kind, h, way), zl if way == 0 else zr)

    def offsets(step):
        return ((0,), (-1, 1), (-2, 2), (-3, 3), (4,))[step]

    def pair_send(buf, k, step):
        for i, off in enumerate(offsets(step)):
            at = zpos(off)
            send(buf.at[at, y], buf.at[at, y], k + 2 * step + i, ypeer)

    def pair_arrived(buf, k, step):
        for i, off in enumerate(offsets(step)):
            arrived(buf.at[zpos(off), 1 - y], k + 2 * step + i, ypeer)

    def gather(buf, k, k_pair, step):
        for kind, h in CHUNKS:
            if step > 1:
                ring_arrived(buf, k, step - 1, kind, h)
            ring_send(buf, k, step, kind, h)
            if (kind, h) == (0, 1):
                pair_send(buf, k_pair, step - 1)

    k_g, k_gp = ids(32), ids(10)
    gather(wg, k_g, k_gp, 1)
    gather(wg, k_g, k_gp, 2)
    x_relay(kbuf, k_k)
    gather(wg, k_g, k_gp, 3)
    gather(wg, k_g, k_gp, 4)
    x_relay(obuf, k_o)
    loads[6].wait()
    x_out(qbuf, k_q)
    for h in range(2):
        ring_arrived(wg, k_g, 4, 0, h)
    pair_send(wg, k_gp, 4)
    for h in range(2):
        ring_arrived(wg, k_g, 4, 1, h)
    x_last(kbuf, k_k)
    for h in range(2):
        kt[:, h * U:(h + 1) * U] = kbuf[2 * h:2 * h + 2].reshape(2 * TOK, DC).T
    wcur[:, 2 * U:3 * U] = dot(perm[...], wg[:, 2].reshape(DC, U)).astype(BF16)
    for step in range(5):
        pair_arrived(wg, k_gp, step)
    for m in range(2):
        wcur[:, m * U:(m + 1) * U] = dot(perm[...], wg[:, m].reshape(DC, U)).astype(BF16)

    k_p = ids(4)

    def p_copy(b):
        return copy(ps.at[b], pr.at[b], k_p + b, peer)

    @pl.loop(0, 4)
    def _(i):
        b = 3 - i
        pl.when(i == 3)(lambda: x_last(obuf, k_o))
        ps[b, :, 0:2 * U] = dot(kbuf[b], wcur[:, 0:2 * U])
        ps[b, :, 2 * U:3 * U] = dot(obuf[b], wcur[:, 2 * U:3 * U])
        p_copy(b).start()

    for h in range(2):
        ot[:, h * U:(h + 1) * U] = obuf[2 * h:2 * h + 2].reshape(2 * TOK, DC).T

    @pl.loop(0, 4)
    def _(i):
        b = 3 - i
        p_copy(b).wait_recv()

        @pl.loop(0, TOK // STEP)
        def _(t):
            r = pl.ds(pl.multiple_of(t * STEP, STEP), STEP)
            o = pl.ds(pl.multiple_of(b * TOK + t * STEP, STEP), STEP)
            gate = ps[b, r, 0:U] + pr[b, r, 0:U]
            up = ps[b, r, U:2 * U] + pr[b, r, U:2 * U]
            hg = ps[b, r, 2 * U:3 * U] + pr[b, r, 2 * U:3 * U]
            sg = jax.nn.sigmoid(gate)
            silu = gate * sg
            hid[o, :] = (silu * up).astype(BF16)
            gg[0, o, :] = (hg * up * (sg * (1.0 + gate * (1.0 - sg)))).astype(BF16)
            gg[1, o, :] = (hg * silu).astype(BF16)

    k_ya = ids(10)
    k_r = ids(32)
    far = pl.ds(pl.multiple_of(zpos(4) * ROWS, 16), ROWS)
    ysf[...] = dot(kt[far, :], gg[1 - y]).astype(BF16)
    send(ysf, yrecv.at[zpos(4)], k_ya + 8, ypeer)
    ysend[...] = dot(kt[...], gg[1 - y]).astype(BF16).reshape(NZ, ROWS, U)
    for step in (3, 2, 1, 0):
        for i, off in enumerate(offsets(step)):
            at = zpos(off)
            send(ysend.at[at], yrecv.at[at], k_ya + 2 * step + i, ypeer)
    gb[...] = dot(ot[...], hid[...]).reshape(NZ, ROWS, U)

    def rs_send(step, kind, h, way):
        lo, hi = CUT[h]
        at = zpos((5 - step) if way == 0 else (step - 5))
        v = (ga if kind == 0 else gb)[at, lo:hi]
        if kind == 0:
            v = v + yrecv[at, lo:hi].astype(F32)
        if step > 2 or (step == 2 and far_way(kind, h) == way):
            arrived(rsr.at[way, step - 2, kind, lo:hi], ring_id(k_r, step - 1, kind, h, way), zl if way == 0 else zr)
            v = v + rsr[way, step - 2, kind, lo:hi].astype(F32)
        rss[way, step - 1, kind, lo:hi] = v.astype(BF16)
        send(
            rss.at[way, step - 1, kind, lo:hi], rsr.at[way, step - 1, kind, lo:hi],
            ring_id(k_r, step, kind, h, way), zr if way == 0 else zl,
        )

    for h in range(2):
        rs_send(1, 1, h, far_way(1, h))
    ga[...] = dot(kt[...], gg[y]).reshape(NZ, ROWS, U)
    arrived(yrecv.at[zpos(4)], k_ya + 8, ypeer)
    for h in range(2):
        rs_send(1, 0, h, far_way(0, h))

    for step in range(2, 5):
        for way in range(2):
            for h in range(2):
                rs_send(step, 1, h, way)
        for way, off in enumerate((5 - step, step - 5)):
            arrived(yrecv.at[zpos(off)], k_ya + 2 * (5 - step) + (1 - way), ypeer)
            for h in range(2):
                rs_send(step, 0, h, way)
        if step == 2:
            for m in range(3):
                sms[m:m + 1, :] = square_sums(wcur[:, m * U:(m + 1) * U])
        if step == 3:
            x_relay(qbuf, k_q)

    def total(kind):
        for way in range(2):
            for h in range(2):
                lo, hi = CUT[h]
                arrived(rsr.at[way, 3, kind, lo:hi], ring_id(k_r, 4, kind, h, way), zl if way == 0 else zr)
        return (ga if kind == 0 else gb)[z] + rsr[0, 3, kind].astype(F32) + rsr[1, 3, kind].astype(F32)

    k_yb = ids(1)
    tb = total(1)
    gb[z] = tb
    ybs[...] = tb.astype(BF16)
    send(ybs, ybr, k_yb, ypeer)
    own_rows = pl.ds(pl.multiple_of(z * ROWS, 16), ROWS)
    arrived(yrecv.at[z], k_ya, ypeer)
    ta = total(0) + yrecv[z].astype(F32)
    old_a = jnp.where(y == 0, wcur[own_rows, 0:U].astype(F32), wcur[own_rows, U:2 * U].astype(F32))
    nw[z, y] = (old_a - ta).astype(BF16)
    k_n, k_np = ids(32), ids(10)
    for h in range(2):
        ring_send(nw, k_n, 1, 0, h)
    pair_send(nw, k_np, 0)
    arrived(ybr, k_yb, ypeer)
    nw[z, 2] = (wcur[own_rows, 2 * U:3 * U].astype(F32) - (gb[z] + ybr[...].astype(F32))).astype(BF16)
    for h in range(2):
        ring_send(nw, k_n, 1, 1, h)
    x_last(qbuf, k_q)
    for step in range(2, 5):
        gather(nw, k_n, k_np, step)
    for h in range(2):
        ring_arrived(nw, k_n, 4, 0, h)
    pair_send(nw, k_np, 4)
    for h in range(2):
        ring_arrived(nw, k_n, 4, 1, h)
    sms[5:6, :] = square_sums(nw[:, 2].reshape(DC, U))
    for step in range(5):
        pair_arrived(nw, k_np, step)

    k_qp = ids(4)
    k_s = ids(1)

    def q_copy(b):
        return copy(qs.at[b], qr.at[b], k_qp + b, peer)

    def q_part(b):
        for m in range(2):
            qs[b, :, m * U:(m + 1) * U] = dot(qbuf[b], nw[:, m].reshape(DC, U))
        cp = q_copy(b)
        cp.start()
        sends.append(cp)

    q_part(OPP)
    for m in range(2):
        sms[3 + m:4 + m, :] = square_sums(nw[:, m].reshape(DC, U))
    sms[6:8, :] = jnp.zeros((2, U), F32)
    send(sms, smr, k_s, peer)
    q_part(LEFT)
    arrived(smr, k_s, peer)
    sums = sms[...] + smr[...]
    r1, r3, r2 = [jnp.sqrt((sums[m:m + 1] + EPS) / (sums[3 + m:4 + m] + EPS)) for m in range(3)]

    def out_part(b):
        q_copy(b).wait_recv()

        @pl.loop(0, TOK // STEP)
        def _(t):
            r = pl.ds(pl.multiple_of(t * STEP, STEP), STEP)
            qg = (qs[b, r, 0:U] + qr[b, r, 0:U]) * r1
            qu = (qs[b, r, U:2 * U] + qr[b, r, U:2 * U]) * r3
            qh[b, r, :] = (qg * jax.nn.sigmoid(qg) * qu * r2).astype(BF16)

        return dot_nt(qh[b], nw[:, 2].reshape(DC, U))

    k_x = ids(6)
    part = out_part(OPP)
    ob[OPP] = part.astype(BF16)
    send(ob.at[OPP, 0:HALF], obr.at[0:HALF], k_x, xr)
    send(ob.at[OPP, HALF:TOK], obr.at[HALF:TOK], k_x + 1, xl)
    q_part(RIGHT)
    part = out_part(LEFT)
    ob[LEFT, 0:HALF] = part[0:HALF].astype(BF16)
    send(ob.at[LEFT, 0:HALF], fin.at[1, 0:HALF], k_x + 2, xl)
    op[0] = part[HALF:TOK]
    q_part(OWN)
    part = out_part(RIGHT)
    ob[RIGHT, HALF:TOK] = part[HALF:TOK].astype(BF16)
    send(ob.at[RIGHT, HALF:TOK], fin.at[0, HALF:TOK], k_x + 4, xr)
    op[1] = part[0:HALF]
    arrived(obr.at[HALF:TOK], k_x + 1, xr)
    ob[LEFT, HALF:TOK] = (op[0] + obr[HALF:TOK].astype(F32)).astype(BF16)
    send(ob.at[LEFT, HALF:TOK], fin.at[1, HALF:TOK], k_x + 3, xl)
    arrived(obr.at[0:HALF], k_x, xl)
    ob[RIGHT, 0:HALF] = (op[1] + obr[0:HALF].astype(F32)).astype(BF16)
    send(ob.at[RIGHT, 0:HALF], fin.at[0, 0:HALF], k_x + 5, xr)
    part = out_part(OWN)
    arrived(fin.at[1, 0:HALF], k_x + 2, xr)
    arrived(fin.at[1, HALF:TOK], k_x + 3, xr)
    arrived(fin.at[0, HALF:TOK], k_x + 4, xl)
    arrived(fin.at[0, 0:HALF], k_x + 5, xl)
    out_ref[...] = (part + fin[0].astype(F32) + fin[1].astype(F32)).astype(BF16)

    for cp in sends:
        cp.wait_send()
    for is_self, cp in w_copies:
        pl.when(jnp.logical_not(is_self))(cp.wait_send)

    @pl.loop(0, 4)
    def _(b):
        p_copy(b).wait_send()


N_SEM = 4 + 12 + 42 + 4 + 42 + 1 + 42 + 5 + 6


def body(keys, values, queries, step_size, gate_weight, up_weight, down_weight):
    hbm = pl.BlockSpec(memory_space=pl.ANY)
    return pl.pallas_call(
        kernel,
        out_shape=jax.ShapeDtypeStruct((TOK, DC), BF16),
        in_specs=[hbm] * 7,
        out_specs=pl.BlockSpec(memory_space=pltpu.VMEM),
        scratch_shapes=[
            pltpu.VMEM((3, PIECE, 2 * U), BF16),
            pltpu.VMEM((TOK, DC), BF16),
            pltpu.VMEM((2, TOK), F32),
            pltpu.VMEM((2, 2, PADDED, 2 * U), BF16),
            pltpu.VMEM((4, PADDED, 2 * U), BF16),
            pltpu.VMEM((NZ, 3, ROWS, U), BF16),
            pltpu.VMEM((DC, DC), BF16),
            pltpu.VMEM((DC, 3 * U), BF16),
            pltpu.VMEM((4, TOK, DC), BF16),
            pltpu.VMEM((4, TOK, DC), BF16),
            pltpu.VMEM((4, TOK, DC), BF16),
            pltpu.VMEM((DC, 4 * TOK), BF16),
            pltpu.VMEM((DC, 4 * TOK), BF16),
            pltpu.VMEM((4, TOK, 3 * U), F32),
            pltpu.VMEM((4, TOK, 3 * U), F32),
            pltpu.VMEM((2, 4 * TOK, U), BF16),
            pltpu.VMEM((4 * TOK, U), BF16),
            pltpu.VMEM((NZ, ROWS, U), F32),
            pltpu.VMEM((NZ, ROWS, U), F32),
            pltpu.VMEM((ROWS, U), BF16),
            pltpu.VMEM((NZ, ROWS, U), BF16),
            pltpu.VMEM((NZ, ROWS, U), BF16),
            pltpu.VMEM((2, 4, 2, ROWS, U), BF16),
            pltpu.VMEM((2, 4, 2, ROWS, U), BF16),
            pltpu.VMEM((ROWS, U), BF16),
            pltpu.VMEM((ROWS, U), BF16),
            pltpu.VMEM((NZ, 3, ROWS, U), BF16),
            pltpu.VMEM((8, U), F32),
            pltpu.VMEM((8, U), F32),
            pltpu.VMEM((4, TOK, 2 * U), F32),
            pltpu.VMEM((4, TOK, 2 * U), F32),
            pltpu.VMEM((4, TOK, U), BF16),
            pltpu.VMEM((4, TOK, DC), BF16),
            pltpu.VMEM((2, HALF, DC), F32),
            pltpu.VMEM((TOK, DC), BF16),
            pltpu.VMEM((2, TOK, DC), BF16),
            pltpu.SemaphoreType.DMA((N_SEM,)),
            pltpu.SemaphoreType.DMA((N_SEM,)),
            pltpu.SemaphoreType.DMA((9,)),
        ],
        compiler_params=pltpu.CompilerParams(
            collective_id=0, has_side_effects=True, vmem_limit_bytes=60 << 20
        ),
        name="ttt_layer",
    )(keys, values, queries, step_size.T, gate_weight, up_weight, down_weight)


def solution(mesh):
    finer = Mesh(mesh.devices.reshape(2, 2, 4, 2, 8), ("yh", "core", "x", "yl", "z"))
    seq, head = ("x", "yl", "z"), ("yh", "core")
    placed = (
        P(seq, head), P(seq, head), P(seq, head), P(seq, None),
        P(seq, head), P(seq, head), P(seq, head),
    )
    return jax.shard_map(body, mesh=finer, in_specs=placed, out_specs=P(seq, head), check_vma=False)
```

```python
import jax
import jax.numpy as jnp
from jax import lax
from jax.experimental import pallas as pl
from jax.experimental.pallas import tpu as pltpu
from jax.sharding import Mesh
from jax.sharding import PartitionSpec as P

EPS = 1e-06
MESH = pl.DeviceIdType.MESH
F32 = jnp.float32
BF16 = jnp.bfloat16

NX, NZ = 4, 8
TOK = 192
DC = 640
U = 384
ROWS = 80
PIECE = 20
PADDED = 48
SECOND = 24
HALF = TOK // 2
CUT = ((0, 48), (48, ROWS))
CHUNKS = ((0, 0), (0, 1), (1, 0), (1, 1))
OPP, LEFT, RIGHT, OWN = 0, 1, 2, 3
STEP = 96


def dot(a, b):
    return jnp.dot(a, b, preferred_element_type=F32)


def dot_nt(a, b):
    return lax.dot_general(a, b, (((1,), (1,)), ((), ())), preferred_element_type=F32)


def square_sums(v):
    f = v.astype(F32)
    return jnp.sum(f * f, axis=0, keepdims=True)


def far_way(kind, h):
    return h if kind == 0 else 1 - h


def kernel(
    k_hbm, v_hbm, q_hbm, s_hbm, w1_hbm, w3_hbm, w2_hbm, out_ref,
    win, vin, sin, wsend, warr, wg, perm, wcur, kbuf, obuf, qbuf, kt, ot, ps, pr, gg, hid,
    ga, gb, ysf, ysend, yrecv, rss, rsr, ybs, ybr, nw, sms, smr, qs, qr, qh, ob, op, obr, fin,
    send_sem, recv_sem, loc_sem,
):
    yh = lax.axis_index("yh")
    c = lax.axis_index("core")
    x = lax.axis_index("x")
    y = lax.axis_index("yl")
    z = lax.axis_index("z")
    xr, xl = {"x": lax.rem(x + 1, NX)}, {"x": lax.rem(x + NX - 1, NX)}
    zr, zl = {"z": lax.rem(z + 1, NZ)}, {"z": lax.rem(z + NZ - 1, NZ)}
    peer, ypeer = {"core": 1 - c}, {"yl": 1 - y}
    xhalf = x // 2
    xlow = lax.rem(x, 2)
    own_w = xhalf == c

    def wtarget(j, dy):
        return {"x": 2 * c + j, "core": xhalf, "yl": y if dy == 0 else 1 - y}

    counter = [0]
    sends = []

    def ids(n):
        first = counter[0]
        counter[0] += n
        return first

    def copy(src, dst, k, to):
        return pltpu.make_async_remote_copy(
            src_ref=src, dst_ref=dst, send_sem=send_sem.at[k], recv_sem=recv_sem.at[k],
            device_id=to, device_id_type=MESH,
        )

    def send(src, dst, k, to):
        cp = copy(src, dst, k, to)
        cp.start()
        sends.append(cp)

    def arrived(ref, k, frm):
        copy(ref, ref, k, frm).wait_recv()

    barrier = pltpu.get_barrier_semaphore()
    for to in (peer, xr, xl, zr, zl, ypeer, wtarget(0, 1), wtarget(1, 1)):
        pl.semaphore_signal(barrier, inc=1, device_id=to, device_id_type=MESH)
    for j in range(2):
        @pl.when(jnp.logical_not(jnp.logical_and(own_w, xlow == j)))
        def _():
            pl.semaphore_signal(barrier, inc=1, device_id=wtarget(j, 0), device_id_type=MESH)

    loads = [
        pltpu.make_async_copy(w1_hbm, win.at[0], loc_sem.at[0]),
        pltpu.make_async_copy(w3_hbm, win.at[1], loc_sem.at[1]),
        pltpu.make_async_copy(w2_hbm, win.at[2], loc_sem.at[2]),
        pltpu.make_async_copy(k_hbm, kbuf.at[OWN], loc_sem.at[3]),
        pltpu.make_async_copy(v_hbm, vin, loc_sem.at[4]),
        pltpu.make_async_copy(s_hbm, sin, loc_sem.at[5]),
        pltpu.make_async_copy(q_hbm, qbuf.at[OWN], loc_sem.at[6]),
    ]
    for ld in loads:
        ld.start()

    wsend[...] = jnp.zeros_like(wsend)
    for m in range(3):
        loads[m].wait()
    for j in range(2):
        for t in range(2):
            wsend[j, t, 0:PIECE, :] = win[t, :, j * U:(j + 1) * U]
            wsend[j, t, SECOND:SECOND + PIECE, :] = win[2, :, j * U:(j + 1) * U]
    loads[3].wait()
    pl.semaphore_wait(barrier, 10 - jnp.where(own_w, 1, 0))

    k_w = ids(4)
    slot = 2 * xlow + y
    w_copies = []
    for j in range(2):
        for dy in (1, 0):
            block = wsend.at[j, y if dy == 0 else 1 - y]
            cp = pltpu.make_async_remote_copy(
                src_ref=block, dst_ref=warr.at[slot],
                send_sem=send_sem.at[k_w + 2 * j + dy], recv_sem=recv_sem.at[k_w + slot],
                device_id=wtarget(j, dy), device_id_type=MESH,
            )
            if dy == 1:
                cp.start()
                sends.append(cp)
            else:
                is_self = jnp.logical_and(own_w, xlow == j)
                w_copies.append((is_self, cp))
                lc = pltpu.make_async_copy(block, warr.at[slot], loc_sem.at[7 + j])
                pl.when(jnp.logical_not(is_self))(cp.start)

                @pl.when(is_self)
                def _():
                    lc.start()
                    lc.wait()

    def x_out(buf, k):
        send(buf.at[OWN], buf.at[LEFT], k, xr)
        send(buf.at[OWN], buf.at[RIGHT], k + 1, xl)

    def x_relay(buf, k):
        arrived(buf.at[LEFT], k, xl)
        send(buf.at[LEFT, 0:HALF], buf.at[OPP, 0:HALF], k + 2, xr)
        arrived(buf.at[RIGHT], k + 1, xr)
        send(buf.at[RIGHT, HALF:TOK], buf.at[OPP, HALF:TOK], k + 3, xl)

    def x_last(buf, k):
        arrived(buf.at[OPP, 0:HALF], k + 2, xl)
        arrived(buf.at[OPP, HALF:TOK], k + 3, xr)

    k_k, k_o, k_q = ids(4), ids(4), ids(4)
    x_out(kbuf, k_k)
    loads[4].wait()
    loads[5].wait()
    diag = lax.broadcasted_iota(jnp.int32, (TOK, TOK), 0) == lax.broadcasted_iota(jnp.int32, (TOK, TOK), 1)
    rate_row = jnp.where(yh == 0, sin[0:1, :], sin[1:2, :])
    rates = jnp.sum(jnp.where(diag, rate_row, 0.0), axis=1, keepdims=True)
    obuf[OWN] = (-(rates * vin[...].astype(F32))).astype(BF16)
    x_out(obuf, k_o)

    row = lax.broadcasted_iota(jnp.int32, (DC, DC), 0)
    col = lax.broadcasted_iota(jnp.int32, (DC, DC), 1)
    group = (row >= 160).astype(jnp.int32) + (row >= 320).astype(jnp.int32) + (row >= 480).astype(jnp.int32)
    rem = row - 160 * group
    step20 = jnp.zeros_like(rem)
    for t in range(1, NZ):
        step20 = step20 + (rem >= PIECE * t).astype(jnp.int32)
    wanted = ROWS * step20 + PIECE * group + rem - PIECE * step20
    perm[...] = jnp.where(col == wanted, 1.0, 0.0).astype(BF16)

    for s in range(4):
        from_x, from_y = s // 2, s % 2
        here = jnp.logical_and(jnp.logical_and(own_w, xlow == from_x), y == from_y)

        @pl.when(jnp.logical_not(here))
        def _():
            copy(warr.at[s], warr.at[s], k_w + s, ypeer).wait_recv()

    prow = lax.broadcasted_iota(jnp.int32, (ROWS, 4 * PADDED), 0)
    pcol = lax.broadcasted_iota(jnp.int32, (ROWS, 4 * PADDED), 1)
    pgroup = (prow >= 20).astype(jnp.int32) + (prow >= 40).astype(jnp.int32) + (prow >= 60).astype(jnp.int32)
    pfrom = prow + (PADDED - PIECE) * pgroup
    blocks = warr[...].reshape(4 * PADDED, U)
    wg[z, 0] = dot(jnp.where(pcol == pfrom, 1.0, 0.0).astype(BF16), blocks).astype(BF16)
    wg[z, 2] = dot(jnp.where(pcol == pfrom + SECOND, 1.0, 0.0).astype(BF16), blocks).astype(BF16)

    def zpos(off):
        return lax.rem(z + off + 2 * NZ, NZ)

    def chunk(buf, at, kind, h):
        return buf.at[at, 2 * kind, CUT[h][0]:CUT[h][1]]

    def ways(step, kind, h):
        return (0, 1) if step < 4 else (far_way(kind, h),)

    def ring_id(k, step, kind, h, way):
        return k + (step - 1) * 8 + 4 * kind + 2 * h + way

    def ring_send(buf, k, step, kind, h):
        for way in ways(step, kind, h):
            ref = chunk(buf, zpos((1 - step) if way == 0 else (step - 1)), kind, h)
            send(ref, ref, ring_id(k, step, kind, h, way), zr if way == 0 else zl)

    def ring_arrived(buf, k, step, kind, h):
        for way in ways(step, kind, h):
            ref = chunk(buf, zpos(-step if way == 0 else step), kind, h)
            arrived(ref, ring_id(k, step, kind, h, way), zl if way == 0 else zr)

    def offsets(step):
        return ((0,), (-1, 1), (-2, 2), (-3, 3), (4,))[step]

    def pair_send(buf, k, step):
        for i, off in enumerate(offsets(step)):
            at = zpos(off)
            send(buf.at[at, 0], buf.at[at, 1], k + 2 * step + i, ypeer)

    def pair_send_far(buf, k, k_ring):
        for h in range(2):
            ring_arrived(buf, k_ring, 4, 0, h)
            at, rows = zpos(4), pl.ds(CUT[h][0], CUT[h][1] - CUT[h][0])
            send(buf.at[at, 0, rows], buf.at[at, 1, rows], k + 8 + h, ypeer)

    def pair_arrived(buf, k):
        for step in range(4):
            for i, off in enumerate(offsets(step)):
                arrived(buf.at[zpos(off), 1], k + 2 * step + i, ypeer)
        for h in range(2):
            arrived(buf.at[zpos(4), 1, CUT[h][0]:CUT[h][1]], k + 8 + h, ypeer)

    def gather(buf, k, k_pair, step):
        for kind, h in CHUNKS:
            if step > 1:
                ring_arrived(buf, k, step - 1, kind, h)
            ring_send(buf, k, step, kind, h)
            if (kind, h) == (0, 1):
                pair_send(buf, k_pair, step - 1)

    k_g, k_gp = ids(32), ids(10)
    gather(wg, k_g, k_gp, 1)
    x_relay(kbuf, k_k)
    gather(wg, k_g, k_gp, 2)
    gather(wg, k_g, k_gp, 3)
    x_relay(obuf, k_o)
    gather(wg, k_g, k_gp, 4)
    loads[6].wait()
    x_out(qbuf, k_q)
    pair_send_far(wg, k_gp, k_g)

    def in_order(m):
        return dot(perm[...], wg[:, m].reshape(DC, U)).astype(BF16)

    for h in range(2):
        ring_arrived(wg, k_g, 4, 1, h)
    wcur[2] = in_order(2)
    wcur[0] = in_order(0)
    pair_arrived(wg, k_gp)
    wcur[1] = in_order(1)
    x_last(kbuf, k_k)

    k_p = ids(4)

    def p_copy(b):
        return copy(ps.at[b], pr.at[b], k_p + b, peer)

    @pl.loop(0, 4)
    def _(i):
        b = 3 - i
        pl.when(i == 3)(lambda: x_last(obuf, k_o))
        ps[b, 0] = dot(kbuf[b], wcur[0])
        ps[b, 1] = dot(kbuf[b], wcur[1])
        ps[b, 2] = dot(obuf[b], wcur[2])
        p_copy(b).start()

    for h in range(2):
        kt[:, h * U:(h + 1) * U] = kbuf[2 * h:2 * h + 2].reshape(2 * TOK, DC).T
        ot[:, h * U:(h + 1) * U] = obuf[2 * h:2 * h + 2].reshape(2 * TOK, DC).T

    @pl.loop(0, 4)
    def _(i):
        b = 3 - i
        p_copy(b).wait_recv()

        @pl.loop(0, TOK // STEP)
        def _(t):
            r = pl.ds(pl.multiple_of(t * STEP, STEP), STEP)
            o = pl.ds(pl.multiple_of(b * TOK + t * STEP, STEP), STEP)
            gate = ps[b, y, r, :] + pr[b, y, r, :]
            up = ps[b, 1 - y, r, :] + pr[b, 1 - y, r, :]
            hg = ps[b, 2, r, :] + pr[b, 2, r, :]
            sg = jax.nn.sigmoid(gate)
            silu = gate * sg
            hid[o, :] = (silu * up).astype(BF16)
            gg[0, o, :] = (hg * up * (sg * (1.0 + gate * (1.0 - sg)))).astype(BF16)
            gg[1, o, :] = (hg * silu).astype(BF16)

    k_ya = ids(10)
    k_r = ids(32)
    far = pl.ds(pl.multiple_of(zpos(4) * ROWS, 16), ROWS)
    ysf[...] = dot(kt[far, :], gg[1 - y]).astype(BF16)
    send(ysf, yrecv.at[zpos(4)], k_ya + 8, ypeer)

    def rs_send(step, kind, h, way):
        lo, hi = CUT[h]
        at = zpos((5 - step) if way == 0 else (step - 5))
        v = (ga if kind == 0 else gb)[at, lo:hi]
        if kind == 0:
            v = v + yrecv[at, lo:hi].astype(F32)
        if step > 2 or (step == 2 and far_way(kind, h) == way):
            arrived(rsr.at[way, step - 2, kind, lo:hi], ring_id(k_r, step - 1, kind, h, way), zl if way == 0 else zr)
            v = v + rsr[way, step - 2, kind, lo:hi].astype(F32)
        rss[way, step - 1, kind, lo:hi] = v.astype(BF16)
        send(
            rss.at[way, step - 1, kind, lo:hi], rsr.at[way, step - 1, kind, lo:hi],
            ring_id(k_r, step, kind, h, way), zr if way == 0 else zl,
        )

    gb[zpos(4)] = dot(ot[far, :], hid[...])
    for h in range(2):
        rs_send(1, 1, h, far_way(1, h))
    ysend[...] = dot(kt[...], gg[1 - y]).astype(BF16).reshape(NZ, ROWS, U)
    for step in (3, 2, 1, 0):
        for i, off in reversed(list(enumerate(offsets(step)))):
            at = zpos(off)
            send(ysend.at[at], yrecv.at[at], k_ya + 2 * step + i, ypeer)
    gb[...] = dot(ot[...], hid[...]).reshape(NZ, ROWS, U)
    ga[...] = dot(kt[...], gg[y]).reshape(NZ, ROWS, U)
    arrived(yrecv.at[zpos(4)], k_ya + 8, ypeer)
    for h in range(2):
        rs_send(1, 0, h, far_way(0, h))

    for step in range(2, 5):
        for way in range(2):
            for h in range(2):
                rs_send(step, 1, h, way)
        for way, off in enumerate((5 - step, step - 5)):
            arrived(yrecv.at[zpos(off)], k_ya + 2 * (5 - step) + (1 - way), ypeer)
            for h in range(2):
                rs_send(step, 0, h, way)
        if step == 2:
            for m in range(3):
                sms[m:m + 1, :] = square_sums(wcur[m])
        if step == 3:
            x_relay(qbuf, k_q)

    def total(kind):
        for way in range(2):
            for h in range(2):
                lo, hi = CUT[h]
                arrived(rsr.at[way, 3, kind, lo:hi], ring_id(k_r, 4, kind, h, way), zl if way == 0 else zr)
        return (ga if kind == 0 else gb)[z] + rsr[0, 3, kind].astype(F32) + rsr[1, 3, kind].astype(F32)

    k_yb = ids(1)
    tb = total(1)
    gb[z] = tb
    ybs[...] = tb.astype(BF16)
    send(ybs, ybr, k_yb, ypeer)
    own_rows = pl.ds(pl.multiple_of(z * ROWS, 16), ROWS)
    arrived(yrecv.at[z], k_ya, ypeer)
    ta = total(0) + yrecv[z].astype(F32)
    nw[z, 0] = (wcur[0, own_rows, :].astype(F32) - ta).astype(BF16)
    k_n, k_np = ids(32), ids(10)
    for h in range(2):
        ring_send(nw, k_n, 1, 0, h)
    pair_send(nw, k_np, 0)
    arrived(ybr, k_yb, ypeer)
    nw[z, 2] = (wcur[2, own_rows, :].astype(F32) - (gb[z] + ybr[...].astype(F32))).astype(BF16)
    for h in range(2):
        ring_send(nw, k_n, 1, 1, h)
    x_last(qbuf, k_q)
    for step in range(2, 5):
        gather(nw, k_n, k_np, step)
    pair_send_far(nw, k_np, k_n)

    k_qp = ids(8)
    k_s = ids(1)

    def q_copy(b, kind):
        return copy(qs.at[b, kind], qr.at[b, kind], k_qp + 2 * b + kind, peer)

    def q_part(b, kind):
        qs[b, kind] = dot(qbuf[b], nw[:, kind].reshape(DC, U))
        cp = q_copy(b, kind)
        cp.start()
        sends.append(cp)

    for b in range(4):
        q_part(b, 0)
    for h in range(2):
        ring_arrived(nw, k_n, 4, 1, h)
    sms[5:6, :] = square_sums(nw[:, 2].reshape(DC, U))
    pair_arrived(nw, k_np)
    q_part(OPP, 1)
    for m in range(2):
        sms[3 + m:4 + m, :] = square_sums(nw[:, m].reshape(DC, U))
    sms[6:8, :] = jnp.zeros((2, U), F32)
    send(sms, smr, k_s, peer)
    q_part(LEFT, 1)
    arrived(smr, k_s, peer)
    sums = sms[...] + smr[...]
    ra, rb, r2 = [jnp.sqrt((sums[m:m + 1] + EPS) / (sums[3 + m:4 + m] + EPS)) for m in range(3)]
    r1, r3 = jnp.where(y == 0, ra, rb), jnp.where(y == 0, rb, ra)

    def out_part(b):
        q_copy(b, 0).wait_recv()
        q_copy(b, 1).wait_recv()

        @pl.loop(0, TOK // STEP)
        def _(t):
            r = pl.ds(pl.multiple_of(t * STEP, STEP), STEP)
            qg = (qs[b, y, r, :] + qr[b, y, r, :]) * r1
            qu = (qs[b, 1 - y, r, :] + qr[b, 1 - y, r, :]) * r3
            qh[b, r, :] = (qg * jax.nn.sigmoid(qg) * qu * r2).astype(BF16)

        return dot_nt(qh[b], nw[:, 2].reshape(DC, U))

    k_x = ids(6)
    part = out_part(OPP)
    ob[OPP] = part.astype(BF16)
    send(ob.at[OPP, 0:HALF], obr.at[0:HALF], k_x, xr)
    send(ob.at[OPP, HALF:TOK], obr.at[HALF:TOK], k_x + 1, xl)
    q_part(RIGHT, 1)
    part = out_part(LEFT)
    ob[LEFT, 0:HALF] = part[0:HALF].astype(BF16)
    send(ob.at[LEFT, 0:HALF], fin.at[1, 0:HALF], k_x + 2, xl)
    op[0] = part[HALF:TOK]
    q_part(OWN, 1)
    part = out_part(RIGHT)
    ob[RIGHT, HALF:TOK] = part[HALF:TOK].astype(BF16)
    send(ob.at[RIGHT, HALF:TOK], fin.at[0, HALF:TOK], k_x + 4, xr)
    op[1] = part[0:HALF]
    arrived(obr.at[HALF:TOK], k_x + 1, xr)
    ob[LEFT, HALF:TOK] = (op[0] + obr[HALF:TOK].astype(F32)).astype(BF16)
    send(ob.at[LEFT, HALF:TOK], fin.at[1, HALF:TOK], k_x + 3, xl)
    arrived(obr.at[0:HALF], k_x, xl)
    ob[RIGHT, 0:HALF] = (op[1] + obr[0:HALF].astype(F32)).astype(BF16)
    send(ob.at[RIGHT, 0:HALF], fin.at[0, 0:HALF], k_x + 5, xr)
    part = out_part(OWN)
    arrived(fin.at[1, 0:HALF], k_x + 2, xr)
    arrived(fin.at[1, HALF:TOK], k_x + 3, xr)
    arrived(fin.at[0, HALF:TOK], k_x + 4, xl)
    arrived(fin.at[0, 0:HALF], k_x + 5, xl)
    out_ref[...] = (part + fin[0].astype(F32) + fin[1].astype(F32)).astype(BF16)

    for cp in sends:
        cp.wait_send()
    for is_self, cp in w_copies:
        pl.when(jnp.logical_not(is_self))(cp.wait_send)

    @pl.loop(0, 4)
    def _(b):
        p_copy(b).wait_send()


N_SEM = 4 + 12 + 42 + 4 + 42 + 1 + 42 + 9 + 6


def body(keys, values, queries, step_size, gate_weight, up_weight, down_weight):
    hbm = pl.BlockSpec(memory_space=pl.ANY)
    return pl.pallas_call(
        kernel,
        out_shape=jax.ShapeDtypeStruct((TOK, DC), BF16),
        in_specs=[hbm] * 7,
        out_specs=pl.BlockSpec(memory_space=pltpu.VMEM),
        scratch_shapes=[
            pltpu.VMEM((3, PIECE, 2 * U), BF16),
            pltpu.VMEM((TOK, DC), BF16),
            pltpu.VMEM((2, TOK), F32),
            pltpu.VMEM((2, 2, PADDED, U), BF16),
            pltpu.VMEM((4, PADDED, U), BF16),
            pltpu.VMEM((NZ, 3, ROWS, U), BF16),
            pltpu.VMEM((DC, DC), BF16),
            pltpu.VMEM((3, DC, U), BF16),
            pltpu.VMEM((4, TOK, DC), BF16),
            pltpu.VMEM((4, TOK, DC), BF16),
            pltpu.VMEM((4, TOK, DC), BF16),
            pltpu.VMEM((DC, 4 * TOK), BF16),
            pltpu.VMEM((DC, 4 * TOK), BF16),
            pltpu.VMEM((4, 3, TOK, U), F32),
            pltpu.VMEM((4, 3, TOK, U), F32),
            pltpu.VMEM((2, 4 * TOK, U), BF16),
            pltpu.VMEM((4 * TOK, U), BF16),
            pltpu.VMEM((NZ, ROWS, U), F32),
            pltpu.VMEM((NZ, ROWS, U), F32),
            pltpu.VMEM((ROWS, U), BF16),
            pltpu.VMEM((NZ, ROWS, U), BF16),
            pltpu.VMEM((NZ, ROWS, U), BF16),
            pltpu.VMEM((2, 4, 2, ROWS, U), BF16),
            pltpu.VMEM((2, 4, 2, ROWS, U), BF16),
            pltpu.VMEM((ROWS, U), BF16),
            pltpu.VMEM((ROWS, U), BF16),
            pltpu.VMEM((NZ, 3, ROWS, U), BF16),
            pltpu.VMEM((8, U), F32),
            pltpu.VMEM((8, U), F32),
            pltpu.VMEM((4, 2, TOK, U), F32),
            pltpu.VMEM((4, 2, TOK, U), F32),
            pltpu.VMEM((4, TOK, U), BF16),
            pltpu.VMEM((4, TOK, DC), BF16),
            pltpu.VMEM((2, HALF, DC), F32),
            pltpu.VMEM((TOK, DC), BF16),
            pltpu.VMEM((2, TOK, DC), BF16),
            pltpu.SemaphoreType.DMA((N_SEM,)),
            pltpu.SemaphoreType.DMA((N_SEM,)),
            pltpu.SemaphoreType.DMA((9,)),
        ],
        compiler_params=pltpu.CompilerParams(
            collective_id=0, has_side_effects=True, vmem_limit_bytes=60 << 20
        ),
        name="ttt_layer",
    )(keys, values, queries, step_size.T, gate_weight, up_weight, down_weight)


def solution(mesh):
    finer = Mesh(mesh.devices.reshape(2, 2, 4, 2, 8), ("yh", "core", "x", "yl", "z"))
    seq, head = ("x", "yl", "z"), ("yh", "core")
    placed = (
        P(seq, head), P(seq, head), P(seq, head), P(seq, None),
        P(seq, head), P(seq, head), P(seq, head),
    )
    return jax.shard_map(body, mesh=finer, in_specs=placed, out_specs=P(seq, head), check_vma=False)
```

```python
import jax
import jax.numpy as jnp
from jax import lax
from jax.experimental import pallas as pl
from jax.experimental.pallas import tpu as pltpu
from jax.sharding import Mesh
from jax.sharding import PartitionSpec as P

EPS = 1e-06
MESH = pl.DeviceIdType.MESH
F32 = jnp.float32
BF16 = jnp.bfloat16

NX, NZ = 4, 8
TOK = 192
DC = 640
U = 384
ROWS = 80
PIECE = 20
PADDED = 48
SECOND = 24
HALF = TOK // 2
CUT = ((0, 48), (48, ROWS))
CHUNKS = ((0, 0), (0, 1), (1, 0), (1, 1))
OPP, LEFT, RIGHT, OWN = 0, 1, 2, 3
STEP = 96


def dot(a, b):
    return jnp.dot(a, b, preferred_element_type=F32)


def dot_nt(a, b):
    return lax.dot_general(a, b, (((1,), (1,)), ((), ())), preferred_element_type=F32)


def square_sums(v):
    f = v.astype(F32)
    return jnp.sum(f * f, axis=0, keepdims=True)


def far_way(kind, h):
    return h if kind == 0 else 1 - h


def kernel(
    k_hbm, v_hbm, q_hbm, s_hbm, w1_hbm, w3_hbm, w2_hbm, out_ref,
    win, kin, vin, qin, sin, wsend, warr, wg, perm, wout, kbuf, obuf, qbuf, kt, ot, ps, pb, pr, gg, hid,
    ga, gb, ysf, ysend, yrecv, rss, rsr, ybs, ybr, nw, sms, smr, qs, qb, qr, qh, ob, op, obr, fin,
    send_sem, recv_sem, loc_sem,
):
    yh = lax.axis_index("yh")
    c = lax.axis_index("core")
    x = lax.axis_index("x")
    y = lax.axis_index("yl")
    z = lax.axis_index("z")
    xr, xl = {"x": lax.rem(x + 1, NX)}, {"x": lax.rem(x + NX - 1, NX)}
    zr, zl = {"z": lax.rem(z + 1, NZ)}, {"z": lax.rem(z + NZ - 1, NZ)}
    peer, ypeer = {"core": 1 - c}, {"yl": 1 - y}
    xhalf = x // 2
    xlow = lax.rem(x, 2)
    own_w = xhalf == c

    def wtarget(j, dy):
        return {"x": 2 * c + j, "core": xhalf, "yl": y if dy == 0 else 1 - y}

    counter = [0]
    sends = []

    def ids(n):
        first = counter[0]
        counter[0] += n
        return first

    def copy(src, dst, k, to):
        return pltpu.make_async_remote_copy(
            src_ref=src, dst_ref=dst, send_sem=send_sem.at[k], recv_sem=recv_sem.at[k],
            device_id=to, device_id_type=MESH,
        )

    def send(src, dst, k, to):
        cp = copy(src, dst, k, to)
        cp.start()
        sends.append(cp)

    def arrived(ref, k, frm):
        copy(ref, ref, k, frm).wait_recv()

    barrier = pltpu.get_barrier_semaphore()
    for to in (peer, xr, xl, zr, zl, ypeer, wtarget(0, 1), wtarget(1, 1)):
        pl.semaphore_signal(barrier, inc=1, device_id=to, device_id_type=MESH)
    for j in range(2):
        @pl.when(jnp.logical_not(jnp.logical_and(own_w, xlow == j)))
        def _():
            pl.semaphore_signal(barrier, inc=1, device_id=wtarget(j, 0), device_id_type=MESH)

    loads = [
        pltpu.make_async_copy(w1_hbm, win.at[0], loc_sem.at[0]),
        pltpu.make_async_copy(w3_hbm, win.at[1], loc_sem.at[1]),
        pltpu.make_async_copy(w2_hbm, win.at[2], loc_sem.at[2]),
        pltpu.make_async_copy(k_hbm, kin, loc_sem.at[3]),
        pltpu.make_async_copy(v_hbm, vin, loc_sem.at[4]),
        pltpu.make_async_copy(s_hbm, sin, loc_sem.at[5]),
        pltpu.make_async_copy(q_hbm, qin, loc_sem.at[6]),
    ]
    for ld in loads:
        ld.start()

    wsend[...] = jnp.zeros_like(wsend)
    for m in range(3):
        loads[m].wait()
    for j in range(2):
        for t in range(2):
            wsend[j, t, 0:PIECE, :] = win[t, :, j * U:(j + 1) * U]
            wsend[j, t, SECOND:SECOND + PIECE, :] = win[2, :, j * U:(j + 1) * U]
    row = lax.broadcasted_iota(jnp.int32, (DC, DC), 0)
    col = lax.broadcasted_iota(jnp.int32, (DC, DC), 1)
    group = (row >= 160).astype(jnp.int32) + (row >= 320).astype(jnp.int32) + (row >= 480).astype(jnp.int32)
    rem = row - 160 * group
    step20 = jnp.zeros_like(rem)
    for t in range(1, NZ):
        step20 = step20 + (rem >= PIECE * t).astype(jnp.int32)
    wanted = ROWS * step20 + PIECE * group + rem - PIECE * step20
    perm[...] = jnp.where(col == wanted, 1.0, 0.0).astype(BF16)

    def gathered_order(v):
        return dot(v, perm[...]).astype(BF16)

    loads[3].wait()
    kbuf[OWN] = gathered_order(kin[...])
    pl.semaphore_wait(barrier, 10 - jnp.where(own_w, 1, 0))

    k_w = ids(4)
    slot = 2 * xlow + y
    w_copies = []
    for j in range(2):
        for dy in (1, 0):
            block = wsend.at[j, y if dy == 0 else 1 - y]
            cp = pltpu.make_async_remote_copy(
                src_ref=block, dst_ref=warr.at[slot],
                send_sem=send_sem.at[k_w + 2 * j + dy], recv_sem=recv_sem.at[k_w + slot],
                device_id=wtarget(j, dy), device_id_type=MESH,
            )
            if dy == 1:
                cp.start()
                sends.append(cp)
            else:
                is_self = jnp.logical_and(own_w, xlow == j)
                w_copies.append((is_self, cp))
                lc = pltpu.make_async_copy(block, warr.at[slot], loc_sem.at[7 + j])
                pl.when(jnp.logical_not(is_self))(cp.start)

                @pl.when(is_self)
                def _():
                    lc.start()
                    lc.wait()

    def x_out(buf, k):
        send(buf.at[OWN], buf.at[LEFT], k, xr)
        send(buf.at[OWN], buf.at[RIGHT], k + 1, xl)

    def x_relay(buf, k):
        arrived(buf.at[LEFT], k, xl)
        send(buf.at[LEFT, 0:HALF], buf.at[OPP, 0:HALF], k + 2, xr)
        arrived(buf.at[RIGHT], k + 1, xr)
        send(buf.at[RIGHT, HALF:TOK], buf.at[OPP, HALF:TOK], k + 3, xl)

    def x_last(buf, k):
        arrived(buf.at[OPP, 0:HALF], k + 2, xl)
        arrived(buf.at[OPP, HALF:TOK], k + 3, xr)

    k_k, k_o, k_q = ids(4), ids(4), ids(4)
    x_out(kbuf, k_k)
    loads[4].wait()
    loads[5].wait()
    diag = lax.broadcasted_iota(jnp.int32, (TOK, TOK), 0) == lax.broadcasted_iota(jnp.int32, (TOK, TOK), 1)
    rate_row = jnp.where(yh == 0, sin[0:1, :], sin[1:2, :])
    rates = jnp.sum(jnp.where(diag, rate_row, 0.0), axis=1, keepdims=True)
    obuf[OWN] = gathered_order((-(rates * vin[...].astype(F32))).astype(BF16))
    x_out(obuf, k_o)
    loads[6].wait()
    qbuf[OWN] = gathered_order(qin[...])

    for s in range(4):
        from_x, from_y = s // 2, s % 2
        here = jnp.logical_and(jnp.logical_and(own_w, xlow == from_x), y == from_y)

        @pl.when(jnp.logical_not(here))
        def _():
            copy(warr.at[s], warr.at[s], k_w + s, ypeer).wait_recv()

    prow = lax.broadcasted_iota(jnp.int32, (ROWS, 4 * PADDED), 0)
    pcol = lax.broadcasted_iota(jnp.int32, (ROWS, 4 * PADDED), 1)
    pgroup = (prow >= 20).astype(jnp.int32) + (prow >= 40).astype(jnp.int32) + (prow >= 60).astype(jnp.int32)
    pfrom = prow + (PADDED - PIECE) * pgroup
    blocks = warr[...].reshape(4 * PADDED, U)
    wg[z, 0] = dot(jnp.where(pcol == pfrom, 1.0, 0.0).astype(BF16), blocks).astype(BF16)
    wg[z, 2] = dot(jnp.where(pcol == pfrom + SECOND, 1.0, 0.0).astype(BF16), blocks).astype(BF16)

    def zpos(off):
        return lax.rem(z + off + 2 * NZ, NZ)

    def chunk(buf, at, kind, h):
        return buf.at[at, 2 * kind, CUT[h][0]:CUT[h][1]]

    def ways(step, kind, h):
        return (0, 1) if step < 4 else (far_way(kind, h),)

    def ring_id(k, step, kind, h, way):
        return k + (step - 1) * 8 + 4 * kind + 2 * h + way

    def ring_send(buf, k, step, kind, h):
        for way in ways(step, kind, h):
            ref = chunk(buf, zpos((1 - step) if way == 0 else (step - 1)), kind, h)
            send(ref, ref, ring_id(k, step, kind, h, way), zr if way == 0 else zl)

    def ring_arrived(buf, k, step, kind, h):
        for way in ways(step, kind, h):
            ref = chunk(buf, zpos(-step if way == 0 else step), kind, h)
            arrived(ref, ring_id(k, step, kind, h, way), zl if way == 0 else zr)

    def offsets(step):
        return ((0,), (-1, 1), (-2, 2), (-3, 3), (4,))[step]

    def pair_send(buf, k, step):
        for i, off in enumerate(offsets(step)):
            at = zpos(off)
            send(buf.at[at, 0], buf.at[at, 1], k + 2 * step + i, ypeer)

    def pair_send_far(buf, k, k_ring):
        for h in range(2):
            ring_arrived(buf, k_ring, 4, 0, h)
            at, rows = zpos(4), pl.ds(CUT[h][0], CUT[h][1] - CUT[h][0])
            send(buf.at[at, 0, rows], buf.at[at, 1, rows], k + 8 + h, ypeer)

    def pair_arrived(buf, k):
        for step in range(4):
            for i, off in enumerate(offsets(step)):
                arrived(buf.at[zpos(off), 1], k + 2 * step + i, ypeer)
        for h in range(2):
            arrived(buf.at[zpos(4), 1, CUT[h][0]:CUT[h][1]], k + 8 + h, ypeer)

    def gather(buf, k, k_pair, step):
        for kind, h in CHUNKS:
            if step > 1:
                ring_arrived(buf, k, step - 1, kind, h)
            ring_send(buf, k, step, kind, h)
            if (kind, h) == (0, 1):
                pair_send(buf, k_pair, step - 1)

    k_g, k_gp = ids(32), ids(10)
    gather(wg, k_g, k_gp, 1)
    gather(wg, k_g, k_gp, 2)
    gather(wg, k_g, k_gp, 3)
    x_relay(kbuf, k_k)
    gather(wg, k_g, k_gp, 4)
    x_relay(obuf, k_o)
    x_out(qbuf, k_q)
    pair_send_far(wg, k_gp, k_g)

    for h in range(2):
        ring_arrived(wg, k_g, 4, 1, h)
    k_p = ids(12)

    def p_part(b, kind):
        v = dot((obuf if kind == 2 else kbuf)[b], wg[:, kind].reshape(DC, U))
        ps[b, kind] = v
        pb[b, kind] = v.astype(BF16)
        send(pb.at[b, kind], pr.at[b, kind], k_p + 3 * b + kind, peer)

    for b in (OWN, RIGHT, LEFT):
        p_part(b, 0)
        p_part(b, 2)
    x_last(kbuf, k_k)
    p_part(OPP, 0)
    x_last(obuf, k_o)
    p_part(OPP, 2)
    pair_arrived(wg, k_gp)
    for b in (OWN, RIGHT, LEFT, OPP):
        p_part(b, 1)

    for h in range(2):
        kt[:, h * U:(h + 1) * U] = kbuf[2 * h:2 * h + 2].reshape(2 * TOK, DC).T
        ot[:, h * U:(h + 1) * U] = obuf[2 * h:2 * h + 2].reshape(2 * TOK, DC).T

    for b in (OWN, RIGHT, LEFT, OPP):
        for kind in range(3):
            arrived(pr.at[b, kind], k_p + 3 * b + kind, peer)

        @pl.loop(0, TOK // STEP)
        def _(t):
            r = pl.ds(pl.multiple_of(t * STEP, STEP), STEP)
            o = pl.ds(pl.multiple_of(b * TOK + t * STEP, STEP), STEP)
            gate = ps[b, y, r, :] + pr[b, y, r, :].astype(F32)
            up = ps[b, 1 - y, r, :] + pr[b, 1 - y, r, :].astype(F32)
            hg = ps[b, 2, r, :] + pr[b, 2, r, :].astype(F32)
            sg = jax.nn.sigmoid(gate)
            silu = gate * sg
            hid[o, :] = (silu * up).astype(BF16)
            gg[0, o, :] = (hg * up * (sg * (1.0 + gate * (1.0 - sg)))).astype(BF16)
            gg[1, o, :] = (hg * silu).astype(BF16)

    k_ya = ids(10)
    k_r = ids(32)
    far = pl.ds(pl.multiple_of(zpos(4) * ROWS, 16), ROWS)
    ysf[...] = dot(kt[far, :], gg[1 - y]).astype(BF16)
    send(ysf, yrecv.at[zpos(4)], k_ya + 8, ypeer)

    def rs_send(step, kind, h, way):
        lo, hi = CUT[h]
        at = zpos((5 - step) if way == 0 else (step - 5))
        v = (ga if kind == 0 else gb)[at, lo:hi]
        if kind == 0:
            v = v + yrecv[at, lo:hi].astype(F32)
        if step > 2 or (step == 2 and far_way(kind, h) == way):
            arrived(rsr.at[way, step - 2, kind, lo:hi], ring_id(k_r, step - 1, kind, h, way), zl if way == 0 else zr)
            v = v + rsr[way, step - 2, kind, lo:hi].astype(F32)
        rss[way, step - 1, kind, lo:hi] = v.astype(BF16)
        send(
            rss.at[way, step - 1, kind, lo:hi], rsr.at[way, step - 1, kind, lo:hi],
            ring_id(k_r, step, kind, h, way), zr if way == 0 else zl,
        )

    gb[zpos(4)] = dot(ot[far, :], hid[...])
    for h in range(2):
        rs_send(1, 1, h, far_way(1, h))
    ysend[...] = dot(kt[...], gg[1 - y]).astype(BF16).reshape(NZ, ROWS, U)
    for step in (3, 2, 1, 0):
        for i, off in reversed(list(enumerate(offsets(step)))):
            at = zpos(off)
            send(ysend.at[at], yrecv.at[at], k_ya + 2 * step + i, ypeer)
    gb[...] = dot(ot[...], hid[...]).reshape(NZ, ROWS, U)
    ga[...] = dot(kt[...], gg[y]).reshape(NZ, ROWS, U)
    arrived(yrecv.at[zpos(4)], k_ya + 8, ypeer)
    for h in range(2):
        rs_send(1, 0, h, far_way(0, h))

    for step in range(2, 5):
        for way in range(2):
            for h in range(2):
                rs_send(step, 1, h, way)
        for way, off in enumerate((5 - step, step - 5)):
            arrived(yrecv.at[zpos(off)], k_ya + 2 * (5 - step) + (1 - way), ypeer)
            for h in range(2):
                rs_send(step, 0, h, way)
        if step == 2:
            for m in range(3):
                sms[m:m + 1, :] = square_sums(wg[:, m].reshape(DC, U))
        if step == 3:
            x_relay(qbuf, k_q)

    def total(kind):
        for way in range(2):
            for h in range(2):
                lo, hi = CUT[h]
                arrived(rsr.at[way, 3, kind, lo:hi], ring_id(k_r, 4, kind, h, way), zl if way == 0 else zr)
        return (ga if kind == 0 else gb)[z] + rsr[0, 3, kind].astype(F32) + rsr[1, 3, kind].astype(F32)

    k_yb = ids(1)
    tb = total(1)
    gb[z] = tb
    ybs[...] = tb.astype(BF16)
    send(ybs, ybr, k_yb, ypeer)
    arrived(yrecv.at[z], k_ya, ypeer)
    ta = total(0) + yrecv[z].astype(F32)
    nw[z, 0] = (wg[z, 0].astype(F32) - ta).astype(BF16)
    k_n, k_np = ids(32), ids(10)
    for h in range(2):
        ring_send(nw, k_n, 1, 0, h)
    pair_send(nw, k_np, 0)
    arrived(ybr, k_yb, ypeer)
    nw[z, 2] = (wg[z, 2].astype(F32) - (gb[z] + ybr[...].astype(F32))).astype(BF16)
    for h in range(2):
        ring_send(nw, k_n, 1, 1, h)
    x_last(qbuf, k_q)
    for step in range(2, 5):
        gather(nw, k_n, k_np, step)
    pair_send_far(nw, k_np, k_n)

    k_qp = ids(8)
    k_s = ids(1)

    def q_part(b, kind):
        v = dot(qbuf[b], nw[:, kind].reshape(DC, U))
        qs[b, kind] = v
        qb[b, kind] = v.astype(BF16)
        send(qb.at[b, kind], qr.at[b, kind], k_qp + 2 * b + kind, peer)

    for b in range(4):
        q_part(b, 0)
    for h in range(2):
        ring_arrived(nw, k_n, 4, 1, h)
    sms[5:6, :] = square_sums(nw[:, 2].reshape(DC, U))
    wout[...] = dot(perm[...], nw[:, 2].reshape(DC, U)).astype(BF16)
    pair_arrived(nw, k_np)
    q_part(OPP, 1)
    for m in range(2):
        sms[3 + m:4 + m, :] = square_sums(nw[:, m].reshape(DC, U))
    sms[6:8, :] = jnp.zeros((2, U), F32)
    send(sms, smr, k_s, peer)
    q_part(LEFT, 1)
    arrived(smr, k_s, peer)
    sums = sms[...] + smr[...]
    ra, rb, r2 = [jnp.sqrt((sums[m:m + 1] + EPS) / (sums[3 + m:4 + m] + EPS)) for m in range(3)]
    r1, r3 = jnp.where(y == 0, ra, rb), jnp.where(y == 0, rb, ra)

    def out_part(b):
        for kind in range(2):
            arrived(qr.at[b, kind], k_qp + 2 * b + kind, peer)

        @pl.loop(0, TOK // STEP)
        def _(t):
            r = pl.ds(pl.multiple_of(t * STEP, STEP), STEP)
            qg = (qs[b, y, r, :] + qr[b, y, r, :].astype(F32)) * r1
            qu = (qs[b, 1 - y, r, :] + qr[b, 1 - y, r, :].astype(F32)) * r3
            qh[b, r, :] = (qg * jax.nn.sigmoid(qg) * qu * r2).astype(BF16)

        return dot_nt(qh[b], wout[...])

    k_x = ids(6)
    part = out_part(OPP)
    ob[OPP] = part.astype(BF16)
    send(ob.at[OPP, 0:HALF], obr.at[0:HALF], k_x, xr)
    send(ob.at[OPP, HALF:TOK], obr.at[HALF:TOK], k_x + 1, xl)
    q_part(RIGHT, 1)
    part = out_part(LEFT)
    ob[LEFT, 0:HALF] = part[0:HALF].astype(BF16)
    send(ob.at[LEFT, 0:HALF], fin.at[1, 0:HALF], k_x + 2, xl)
    op[0] = part[HALF:TOK]
    q_part(OWN, 1)
    part = out_part(RIGHT)
    ob[RIGHT, HALF:TOK] = part[HALF:TOK].astype(BF16)
    send(ob.at[RIGHT, HALF:TOK], fin.at[0, HALF:TOK], k_x + 4, xr)
    op[1] = part[0:HALF]
    arrived(obr.at[HALF:TOK], k_x + 1, xr)
    ob[LEFT, HALF:TOK] = (op[0] + obr[HALF:TOK].astype(F32)).astype(BF16)
    send(ob.at[LEFT, HALF:TOK], fin.at[1, HALF:TOK], k_x + 3, xl)
    arrived(obr.at[0:HALF], k_x, xl)
    ob[RIGHT, 0:HALF] = (op[1] + obr[0:HALF].astype(F32)).astype(BF16)
    send(ob.at[RIGHT, 0:HALF], fin.at[0, 0:HALF], k_x + 5, xr)
    part = out_part(OWN)
    arrived(fin.at[1, 0:HALF], k_x + 2, xr)
    arrived(fin.at[1, HALF:TOK], k_x + 3, xr)
    arrived(fin.at[0, HALF:TOK], k_x + 4, xl)
    arrived(fin.at[0, 0:HALF], k_x + 5, xl)
    out_ref[...] = (part + fin[0].astype(F32) + fin[1].astype(F32)).astype(BF16)

    for cp in sends:
        cp.wait_send()
    for is_self, cp in w_copies:
        pl.when(jnp.logical_not(is_self))(cp.wait_send)


N_SEM = 4 + 12 + 42 + 12 + 42 + 1 + 42 + 9 + 6


def body(keys, values, queries, step_size, gate_weight, up_weight, down_weight):
    hbm = pl.BlockSpec(memory_space=pl.ANY)
    return pl.pallas_call(
        kernel,
        out_shape=jax.ShapeDtypeStruct((TOK, DC), BF16),
        in_specs=[hbm] * 7,
        out_specs=pl.BlockSpec(memory_space=pltpu.VMEM),
        scratch_shapes=[
            pltpu.VMEM((3, PIECE, 2 * U), BF16),
            pltpu.VMEM((TOK, DC), BF16),
            pltpu.VMEM((TOK, DC), BF16),
            pltpu.VMEM((TOK, DC), BF16),
            pltpu.VMEM((2, TOK), F32),
            pltpu.VMEM((2, 2, PADDED, U), BF16),
            pltpu.VMEM((4, PADDED, U), BF16),
            pltpu.VMEM((NZ, 3, ROWS, U), BF16),
            pltpu.VMEM((DC, DC), BF16),
            pltpu.VMEM((DC, U), BF16),
            pltpu.VMEM((4, TOK, DC), BF16),
            pltpu.VMEM((4, TOK, DC), BF16),
            pltpu.VMEM((4, TOK, DC), BF16),
            pltpu.VMEM((DC, 4 * TOK), BF16),
            pltpu.VMEM((DC, 4 * TOK), BF16),
            pltpu.VMEM((4, 3, TOK, U), F32),
            pltpu.VMEM((4, 3, TOK, U), BF16),
            pltpu.VMEM((4, 3, TOK, U), BF16),
            pltpu.VMEM((2, 4 * TOK, U), BF16),
            pltpu.VMEM((4 * TOK, U), BF16),
            pltpu.VMEM((NZ, ROWS, U), F32),
            pltpu.VMEM((NZ, ROWS, U), F32),
            pltpu.VMEM((ROWS, U), BF16),
            pltpu.VMEM((NZ, ROWS, U), BF16),
            pltpu.VMEM((NZ, ROWS, U), BF16),
            pltpu.VMEM((2, 4, 2, ROWS, U), BF16),
            pltpu.VMEM((2, 4, 2, ROWS, U), BF16),
            pltpu.VMEM((ROWS, U), BF16),
            pltpu.VMEM((ROWS, U), BF16),
            pltpu.VMEM((NZ, 3, ROWS, U), BF16),
            pltpu.VMEM((8, U), F32),
            pltpu.VMEM((8, U), F32),
            pltpu.VMEM((4, 2, TOK, U), F32),
            pltpu.VMEM((4, 2, TOK, U), BF16),
            pltpu.VMEM((4, 2, TOK, U), BF16),
            pltpu.VMEM((4, TOK, U), BF16),
            pltpu.VMEM((4, TOK, DC), BF16),
            pltpu.VMEM((2, HALF, DC), F32),
            pltpu.VMEM((TOK, DC), BF16),
            pltpu.VMEM((2, TOK, DC), BF16),
            pltpu.SemaphoreType.DMA((N_SEM,)),
            pltpu.SemaphoreType.DMA((N_SEM,)),
            pltpu.SemaphoreType.DMA((9,)),
        ],
        compiler_params=pltpu.CompilerParams(
            collective_id=0, has_side_effects=True, vmem_limit_bytes=60 << 20
        ),
        name="ttt_layer",
    )(keys, values, queries, step_size.T, gate_weight, up_weight, down_weight)


def solution(mesh):
    finer = Mesh(mesh.devices.reshape(2, 2, 4, 2, 8), ("yh", "core", "x", "yl", "z"))
    seq, head = ("x", "yl", "z"), ("yh", "core")
    placed = (
        P(seq, head), P(seq, head), P(seq, head), P(seq, None),
        P(seq, head), P(seq, head), P(seq, head),
    )
    return jax.shard_map(body, mesh=finer, in_specs=placed, out_specs=P(seq, head), check_vma=False)
```

```python
import jax
import jax.numpy as jnp
from jax import lax
from jax.experimental import pallas as pl
from jax.experimental.pallas import tpu as pltpu
from jax.sharding import Mesh
from jax.sharding import PartitionSpec as P

EPS = 1e-06
MESH = pl.DeviceIdType.MESH
F32 = jnp.float32
BF16 = jnp.bfloat16

NX, NZ = 4, 8
TOK = 192
DC = 640
U = 384
ROWS = 80
PIECE = 20
PADDED = 48
SECOND = 24
HALF = TOK // 2
CUT = ((0, 48), (48, ROWS))
CHUNKS = ((0, 0), (0, 1), (1, 0), (1, 1))
OPP, LEFT, RIGHT, OWN = 0, 1, 2, 3
STEP = 96


def dot(a, b):
    return jnp.dot(a, b, preferred_element_type=F32)


def dot_nt(a, b):
    return lax.dot_general(a, b, (((1,), (1,)), ((), ())), preferred_element_type=F32)


def square_sums(v):
    f = v.astype(F32)
    return jnp.sum(f * f, axis=0, keepdims=True)


def far_way(kind, h):
    return h if kind == 0 else 1 - h


def kernel(
    k_hbm, v_hbm, q_hbm, s_hbm, w1_hbm, w3_hbm, w2_hbm, out_ref,
    win, kin, vin, qin, sin, wsend, warr, wg, perm, wout, kbuf, obuf, qbuf, kt, ot, ps, pb, pr, gg, hid,
    ga, gb, yfar, ysend, yrecv, rss, rsr, ybs, ybr, nw, sms, smr, qs, qr, qh, ob, op, obr, fin,
    send_sem, recv_sem, loc_sem,
):
    yh = lax.axis_index("yh")
    c = lax.axis_index("core")
    x = lax.axis_index("x")
    y = lax.axis_index("yl")
    z = lax.axis_index("z")
    xr, xl = {"x": lax.rem(x + 1, NX)}, {"x": lax.rem(x + NX - 1, NX)}
    zr, zl = {"z": lax.rem(z + 1, NZ)}, {"z": lax.rem(z + NZ - 1, NZ)}
    dr, dl = {"yl": 1 - y, **zr}, {"yl": 1 - y, **zl}
    peer, ypeer = {"core": 1 - c}, {"yl": 1 - y}
    xhalf = x // 2
    xlow = lax.rem(x, 2)
    own_w = xhalf == c

    def wtarget(j, dy):
        return {"x": 2 * c + j, "core": xhalf, "yl": y if dy == 0 else 1 - y}

    counter = [0]
    sends = []

    def ids(n):
        first = counter[0]
        counter[0] += n
        return first

    def copy(src, dst, k, to):
        return pltpu.make_async_remote_copy(
            src_ref=src, dst_ref=dst, send_sem=send_sem.at[k], recv_sem=recv_sem.at[k],
            device_id=to, device_id_type=MESH,
        )

    def send(src, dst, k, to):
        cp = copy(src, dst, k, to)
        cp.start()
        sends.append(cp)

    def arrived(ref, k, frm):
        copy(ref, ref, k, frm).wait_recv()

    barrier = pltpu.get_barrier_semaphore()
    for to in (peer, xr, xl, zr, zl, dr, dl, ypeer, wtarget(0, 1), wtarget(1, 1)):
        pl.semaphore_signal(barrier, inc=1, device_id=to, device_id_type=MESH)
    for j in range(2):
        @pl.when(jnp.logical_not(jnp.logical_and(own_w, xlow == j)))
        def _():
            pl.semaphore_signal(barrier, inc=1, device_id=wtarget(j, 0), device_id_type=MESH)

    loads = [
        pltpu.make_async_copy(w1_hbm, win.at[0], loc_sem.at[0]),
        pltpu.make_async_copy(w3_hbm, win.at[1], loc_sem.at[1]),
        pltpu.make_async_copy(w2_hbm, win.at[2], loc_sem.at[2]),
        pltpu.make_async_copy(k_hbm, kin, loc_sem.at[3]),
        pltpu.make_async_copy(v_hbm, vin, loc_sem.at[4]),
        pltpu.make_async_copy(s_hbm, sin, loc_sem.at[5]),
        pltpu.make_async_copy(q_hbm, qin, loc_sem.at[6]),
    ]
    for ld in loads:
        ld.start()

    wsend[...] = jnp.zeros_like(wsend)
    for m in range(3):
        loads[m].wait()
    for j in range(2):
        for t in range(2):
            wsend[j, t, 0:PIECE, :] = win[t, :, j * U:(j + 1) * U]
            wsend[j, t, SECOND:SECOND + PIECE, :] = win[2, :, j * U:(j + 1) * U]
    row = lax.broadcasted_iota(jnp.int32, (DC, DC), 0)
    col = lax.broadcasted_iota(jnp.int32, (DC, DC), 1)
    group = (row >= 160).astype(jnp.int32) + (row >= 320).astype(jnp.int32) + (row >= 480).astype(jnp.int32)
    rem = row - 160 * group
    step20 = jnp.zeros_like(rem)
    for t in range(1, NZ):
        step20 = step20 + (rem >= PIECE * t).astype(jnp.int32)
    wanted = ROWS * step20 + PIECE * group + rem - PIECE * step20
    perm[...] = jnp.where(col == wanted, 1.0, 0.0).astype(BF16)

    def gathered_order(v):
        return dot(v, perm[...]).astype(BF16)

    loads[3].wait()
    kbuf[OWN] = gathered_order(kin[...])
    pl.semaphore_wait(barrier, 12 - jnp.where(own_w, 1, 0))

    k_w = ids(4)
    slot = 2 * xlow + y
    w_copies = []
    for j in range(2):
        for dy in (1, 0):
            block = wsend.at[j, y if dy == 0 else 1 - y]
            cp = pltpu.make_async_remote_copy(
                src_ref=block, dst_ref=warr.at[slot],
                send_sem=send_sem.at[k_w + 2 * j + dy], recv_sem=recv_sem.at[k_w + slot],
                device_id=wtarget(j, dy), device_id_type=MESH,
            )
            if dy == 1:
                cp.start()
                sends.append(cp)
            else:
                is_self = jnp.logical_and(own_w, xlow == j)
                w_copies.append((is_self, cp))
                lc = pltpu.make_async_copy(block, warr.at[slot], loc_sem.at[7 + j])
                pl.when(jnp.logical_not(is_self))(cp.start)

                @pl.when(is_self)
                def _():
                    lc.start()
                    lc.wait()

    def x_out(buf, k):
        send(buf.at[OWN], buf.at[LEFT], k, xr)
        send(buf.at[OWN], buf.at[RIGHT], k + 1, xl)

    def x_relay(buf, k):
        arrived(buf.at[LEFT], k, xl)
        send(buf.at[LEFT, 0:HALF], buf.at[OPP, 0:HALF], k + 2, xr)
        arrived(buf.at[RIGHT], k + 1, xr)
        send(buf.at[RIGHT, HALF:TOK], buf.at[OPP, HALF:TOK], k + 3, xl)

    def x_last(buf, k):
        arrived(buf.at[OPP, 0:HALF], k + 2, xl)
        arrived(buf.at[OPP, HALF:TOK], k + 3, xr)

    k_k, k_o, k_q = ids(4), ids(4), ids(4)
    x_out(kbuf, k_k)
    loads[4].wait()
    loads[5].wait()
    diag = lax.broadcasted_iota(jnp.int32, (TOK, TOK), 0) == lax.broadcasted_iota(jnp.int32, (TOK, TOK), 1)
    rate_row = jnp.where(yh == 0, sin[0:1, :], sin[1:2, :])
    rates = jnp.sum(jnp.where(diag, rate_row, 0.0), axis=1, keepdims=True)
    obuf[OWN] = gathered_order((-(rates * vin[...].astype(F32))).astype(BF16))
    x_out(obuf, k_o)
    loads[6].wait()
    qbuf[OWN] = gathered_order(qin[...])

    for s in range(4):
        from_x, from_y = s // 2, s % 2
        here = jnp.logical_and(jnp.logical_and(own_w, xlow == from_x), y == from_y)

        @pl.when(jnp.logical_not(here))
        def _():
            copy(warr.at[s], warr.at[s], k_w + s, ypeer).wait_recv()

    prow = lax.broadcasted_iota(jnp.int32, (ROWS, 4 * PADDED), 0)
    pcol = lax.broadcasted_iota(jnp.int32, (ROWS, 4 * PADDED), 1)
    pgroup = (prow >= 20).astype(jnp.int32) + (prow >= 40).astype(jnp.int32) + (prow >= 60).astype(jnp.int32)
    pfrom = prow + (PADDED - PIECE) * pgroup
    blocks = warr[...].reshape(4 * PADDED, U)
    wg[z, 0] = dot(jnp.where(pcol == pfrom, 1.0, 0.0).astype(BF16), blocks).astype(BF16)
    wg[z, 2] = dot(jnp.where(pcol == pfrom + SECOND, 1.0, 0.0).astype(BF16), blocks).astype(BF16)

    def zpos(off):
        return lax.rem(z + off + 2 * NZ, NZ)

    def chunk(buf, at, kind, h):
        return buf.at[at, 2 * kind, CUT[h][0]:CUT[h][1]]

    def ways(step, kind, h):
        return (0, 1) if step < 4 else (far_way(kind, h),)

    def ring_id(k, step, kind, h, way):
        return k + (step - 1) * 8 + 4 * kind + 2 * h + way

    def ring_send(buf, k, step, kind, h):
        for way in ways(step, kind, h):
            ref = chunk(buf, zpos((1 - step) if way == 0 else (step - 1)), kind, h)
            send(ref, ref, ring_id(k, step, kind, h, way), zr if way == 0 else zl)

    def ring_arrived(buf, k, step, kind, h):
        for way in ways(step, kind, h):
            ref = chunk(buf, zpos(-step if way == 0 else step), kind, h)
            arrived(ref, ring_id(k, step, kind, h, way), zl if way == 0 else zr)

    def offsets(step):
        return ((0,), (-1, 1), (-2, 2), (-3, 3), (4,))[step]

    def pair_send(buf, k, step):
        for i, off in enumerate(offsets(step)):
            at = zpos(off)
            send(buf.at[at, 0], buf.at[at, 1], k + 2 * step + i, ypeer)

    def far_send(buf, k, h):
        at, rows = zpos(-3 if h == 0 else 3), pl.ds(CUT[h][0], CUT[h][1] - CUT[h][0])
        send(buf.at[at, 0, rows], buf.at[at, 1, rows], k + 8 + h, dr if h == 0 else dl)

    def far_arrived(buf, k):
        for h in range(2):
            ring_arrived(buf, k, 4, 0, h)

    def pair_arrived(buf, k):
        for step in range(4):
            for i, off in enumerate(offsets(step)):
                arrived(buf.at[zpos(off), 1], k + 2 * step + i, ypeer)
        for h in range(2):
            arrived(buf.at[zpos(4), 1, CUT[h][0]:CUT[h][1]], k + 8 + h, ypeer)

    def gather(buf, k, k_pair, step):
        for kind, h in CHUNKS:
            if step > 1:
                ring_arrived(buf, k, step - 1, kind, h)
            ring_send(buf, k, step, kind, h)
            if step == 4 and kind == 0:
                far_send(buf, k_pair, h)
            if (kind, h) == (0, 1):
                pair_send(buf, k_pair, step - 1)

    k_g, k_gp = ids(32), ids(10)
    gather(wg, k_g, k_gp, 1)
    gather(wg, k_g, k_gp, 2)
    gather(wg, k_g, k_gp, 3)
    x_relay(kbuf, k_k)
    gather(wg, k_g, k_gp, 4)
    x_relay(obuf, k_o)
    x_out(qbuf, k_q)
    far_arrived(wg, k_g)

    for h in range(2):
        ring_arrived(wg, k_g, 4, 1, h)
    k_p = ids(12)

    def p_part(b, kind):
        v = dot((obuf if kind == 2 else kbuf)[b], wg[:, kind].reshape(DC, U))
        ps[b, kind] = v
        pb[b, kind] = v.astype(BF16)
        send(pb.at[b, kind], pr.at[b, kind], k_p + 3 * b + kind, peer)

    for b in (OWN, RIGHT, LEFT):
        p_part(b, 0)
        p_part(b, 2)
    x_last(kbuf, k_k)
    p_part(OPP, 0)
    x_last(obuf, k_o)
    p_part(OPP, 2)
    pair_arrived(wg, k_gp)
    for b in (OWN, RIGHT, LEFT, OPP):
        p_part(b, 1)

    for h in range(2):
        kt[:, h * U:(h + 1) * U] = kbuf[2 * h:2 * h + 2].reshape(2 * TOK, DC).T
        ot[:, h * U:(h + 1) * U] = obuf[2 * h:2 * h + 2].reshape(2 * TOK, DC).T

    for b in (OWN, RIGHT, LEFT, OPP):
        for kind in range(3):
            arrived(pr.at[b, kind], k_p + 3 * b + kind, peer)

        @pl.loop(0, TOK // STEP)
        def _(t):
            r = pl.ds(pl.multiple_of(t * STEP, STEP), STEP)
            o = pl.ds(pl.multiple_of(b * TOK + t * STEP, STEP), STEP)
            gate = ps[b, y, r, :] + pr[b, y, r, :].astype(F32)
            up = ps[b, 1 - y, r, :] + pr[b, 1 - y, r, :].astype(F32)
            hg = ps[b, 2, r, :] + pr[b, 2, r, :].astype(F32)
            sg = jax.nn.sigmoid(gate)
            silu = gate * sg
            hid[o, :] = (silu * up).astype(BF16)
            gg[0, o, :] = (hg * up * (sg * (1.0 + gate * (1.0 - sg)))).astype(BF16)
            gg[1, o, :] = (hg * silu).astype(BF16)

    k_ya = ids(10)
    k_r = ids(32)
    far = pl.ds(pl.multiple_of(zpos(4) * ROWS, 16), ROWS)
    def rs_send(step, kind, h, way):
        lo, hi = CUT[h]
        at = zpos((5 - step) if way == 0 else (step - 5))
        v = (ga if kind == 0 else gb)[at, lo:hi]
        if kind == 0 and step > 1:
            v = v + yrecv[at, lo:hi].astype(F32)
        if kind == 0 and step == 2 and h == way:
            arrived(yfar.at[lo:hi], k_ya + 8 + h, dl if way == 0 else dr)
            v = v + yfar[lo:hi].astype(F32)
        if step > 2 or (step == 2 and far_way(kind, h) == way):
            arrived(rsr.at[way, step - 2, kind, lo:hi], ring_id(k_r, step - 1, kind, h, way), zl if way == 0 else zr)
            v = v + rsr[way, step - 2, kind, lo:hi].astype(F32)
        rss[way, step - 1, kind, lo:hi] = v.astype(BF16)
        send(
            rss.at[way, step - 1, kind, lo:hi], rsr.at[way, step - 1, kind, lo:hi],
            ring_id(k_r, step, kind, h, way), zr if way == 0 else zl,
        )

    gb[zpos(4)] = dot(ot[far, :], hid[...])
    for h in range(2):
        rs_send(1, 1, h, far_way(1, h))
    ysend[...] = dot(kt[...], gg[1 - y]).astype(BF16).reshape(NZ, ROWS, U)
    for h in range(2):
        lo, hi = CUT[h]
        send(ysend.at[zpos(4), lo:hi], yfar.at[lo:hi], k_ya + 8 + h, dr if h == 0 else dl)
    for step in (3, 2, 1, 0):
        for i, off in reversed(list(enumerate(offsets(step)))):
            at = zpos(off)
            send(ysend.at[at], yrecv.at[at], k_ya + 2 * step + i, ypeer)
    ga[zpos(4)] = dot(kt[far, :], gg[y])
    for h in range(2):
        rs_send(1, 0, h, far_way(0, h))
    gb[...] = dot(ot[...], hid[...]).reshape(NZ, ROWS, U)
    ga[...] = dot(kt[...], gg[y]).reshape(NZ, ROWS, U)

    for step in range(2, 5):
        for way in range(2):
            for h in range(2):
                rs_send(step, 1, h, way)
        for way, off in enumerate((5 - step, step - 5)):
            arrived(yrecv.at[zpos(off)], k_ya + 2 * (5 - step) + (1 - way), ypeer)
            for h in range(2):
                rs_send(step, 0, h, way)
        if step == 2:
            for m in range(3):
                sms[m:m + 1, :] = square_sums(wg[:, m].reshape(DC, U))
        if step == 3:
            x_relay(qbuf, k_q)

    def total(kind):
        for way in range(2):
            for h in range(2):
                lo, hi = CUT[h]
                arrived(rsr.at[way, 3, kind, lo:hi], ring_id(k_r, 4, kind, h, way), zl if way == 0 else zr)
        return (ga if kind == 0 else gb)[z] + rsr[0, 3, kind].astype(F32) + rsr[1, 3, kind].astype(F32)

    k_yb = ids(1)
    tb = total(1)
    gb[z] = tb
    ybs[...] = tb.astype(BF16)
    send(ybs, ybr, k_yb, ypeer)
    arrived(yrecv.at[z], k_ya, ypeer)
    ta = total(0) + yrecv[z].astype(F32)
    nw[z, 0] = (wg[z, 0].astype(F32) - ta).astype(BF16)
    k_n, k_np = ids(32), ids(10)
    for h in range(2):
        ring_send(nw, k_n, 1, 0, h)
    pair_send(nw, k_np, 0)
    arrived(ybr, k_yb, ypeer)
    nw[z, 2] = (wg[z, 2].astype(F32) - (gb[z] + ybr[...].astype(F32))).astype(BF16)
    for h in range(2):
        ring_send(nw, k_n, 1, 1, h)
    x_last(qbuf, k_q)
    for step in range(2, 5):
        gather(nw, k_n, k_np, step)
    far_arrived(nw, k_n)

    k_qp = ids(8)
    k_s = ids(1)

    def q_part(b, kind):
        qs[b, kind] = dot(qbuf[b], nw[:, kind].reshape(DC, U))
        send(qs.at[b, kind], qr.at[b, kind], k_qp + 2 * b + kind, peer)

    for b in range(4):
        q_part(b, 0)
    for h in range(2):
        ring_arrived(nw, k_n, 4, 1, h)
    sms[5:6, :] = square_sums(nw[:, 2].reshape(DC, U))
    wout[...] = dot(perm[...], nw[:, 2].reshape(DC, U)).astype(BF16)
    pair_arrived(nw, k_np)
    q_part(OPP, 1)
    for m in range(2):
        sms[3 + m:4 + m, :] = square_sums(nw[:, m].reshape(DC, U))
    sms[6:8, :] = jnp.zeros((2, U), F32)
    send(sms, smr, k_s, peer)
    q_part(LEFT, 1)
    arrived(smr, k_s, peer)
    sums = sms[...] + smr[...]
    ra, rb, r2 = [jnp.sqrt((sums[m:m + 1] + EPS) / (sums[3 + m:4 + m] + EPS)) for m in range(3)]
    r1, r3 = jnp.where(y == 0, ra, rb), jnp.where(y == 0, rb, ra)

    def out_part(b):
        for kind in range(2):
            arrived(qr.at[b, kind], k_qp + 2 * b + kind, peer)

        @pl.loop(0, TOK // STEP)
        def _(t):
            r = pl.ds(pl.multiple_of(t * STEP, STEP), STEP)
            qg = (qs[b, y, r, :] + qr[b, y, r, :]) * r1
            qu = (qs[b, 1 - y, r, :] + qr[b, 1 - y, r, :]) * r3
            qh[b, r, :] = (qg * jax.nn.sigmoid(qg) * qu * r2).astype(BF16)

        return dot_nt(qh[b], wout[...])

    k_x = ids(6)
    part = out_part(OPP)
    ob[OPP] = part.astype(BF16)
    send(ob.at[OPP, 0:HALF], obr.at[0:HALF], k_x, xr)
    send(ob.at[OPP, HALF:TOK], obr.at[HALF:TOK], k_x + 1, xl)
    q_part(RIGHT, 1)
    part = out_part(LEFT)
    ob[LEFT, 0:HALF] = part[0:HALF].astype(BF16)
    send(ob.at[LEFT, 0:HALF], fin.at[1, 0:HALF], k_x + 2, xl)
    op[0] = part[HALF:TOK]
    q_part(OWN, 1)
    part = out_part(RIGHT)
    ob[RIGHT, HALF:TOK] = part[HALF:TOK].astype(BF16)
    send(ob.at[RIGHT, HALF:TOK], fin.at[0, HALF:TOK], k_x + 4, xr)
    op[1] = part[0:HALF]
    arrived(obr.at[HALF:TOK], k_x + 1, xr)
    ob[LEFT, HALF:TOK] = (op[0] + obr[HALF:TOK].astype(F32)).astype(BF16)
    send(ob.at[LEFT, HALF:TOK], fin.at[1, HALF:TOK], k_x + 3, xl)
    arrived(obr.at[0:HALF], k_x, xl)
    ob[RIGHT, 0:HALF] = (op[1] + obr[0:HALF].astype(F32)).astype(BF16)
    send(ob.at[RIGHT, 0:HALF], fin.at[0, 0:HALF], k_x + 5, xr)
    part = out_part(OWN)
    arrived(fin.at[1, 0:HALF], k_x + 2, xr)
    arrived(fin.at[1, HALF:TOK], k_x + 3, xr)
    arrived(fin.at[0, HALF:TOK], k_x + 4, xl)
    arrived(fin.at[0, 0:HALF], k_x + 5, xl)
    out_ref[...] = (part + fin[0].astype(F32) + fin[1].astype(F32)).astype(BF16)

    for cp in sends:
        cp.wait_send()
    for is_self, cp in w_copies:
        pl.when(jnp.logical_not(is_self))(cp.wait_send)


N_SEM = 4 + 12 + 42 + 12 + 42 + 1 + 42 + 9 + 6


def body(keys, values, queries, step_size, gate_weight, up_weight, down_weight):
    hbm = pl.BlockSpec(memory_space=pl.ANY)
    return pl.pallas_call(
        kernel,
        out_shape=jax.ShapeDtypeStruct((TOK, DC), BF16),
        in_specs=[hbm] * 7,
        out_specs=pl.BlockSpec(memory_space=pltpu.VMEM),
        scratch_shapes=[
            pltpu.VMEM((3, PIECE, 2 * U), BF16),
            pltpu.VMEM((TOK, DC), BF16),
            pltpu.VMEM((TOK, DC), BF16),
            pltpu.VMEM((TOK, DC), BF16),
            pltpu.VMEM((2, TOK), F32),
            pltpu.VMEM((2, 2, PADDED, U), BF16),
            pltpu.VMEM((4, PADDED, U), BF16),
            pltpu.VMEM((NZ, 3, ROWS, U), BF16),
            pltpu.VMEM((DC, DC), BF16),
            pltpu.VMEM((DC, U), BF16),
            pltpu.VMEM((4, TOK, DC), BF16),
            pltpu.VMEM((4, TOK, DC), BF16),
            pltpu.VMEM((4, TOK, DC), BF16),
            pltpu.VMEM((DC, 4 * TOK), BF16),
            pltpu.VMEM((DC, 4 * TOK), BF16),
            pltpu.VMEM((4, 3, TOK, U), F32),
            pltpu.VMEM((4, 3, TOK, U), BF16),
            pltpu.VMEM((4, 3, TOK, U), BF16),
            pltpu.VMEM((2, 4 * TOK, U), BF16),
            pltpu.VMEM((4 * TOK, U), BF16),
            pltpu.VMEM((NZ, ROWS, U), F32),
            pltpu.VMEM((NZ, ROWS, U), F32),
            pltpu.VMEM((ROWS, U), BF16),
            pltpu.VMEM((NZ, ROWS, U), BF16),
            pltpu.VMEM((NZ, ROWS, U), BF16),
            pltpu.VMEM((2, 4, 2, ROWS, U), BF16),
            pltpu.VMEM((2, 4, 2, ROWS, U), BF16),
            pltpu.VMEM((ROWS, U), BF16),
            pltpu.VMEM((ROWS, U), BF16),
            pltpu.VMEM((NZ, 3, ROWS, U), BF16),
            pltpu.VMEM((8, U), F32),
            pltpu.VMEM((8, U), F32),
            pltpu.VMEM((4, 2, TOK, U), F32),
            pltpu.VMEM((4, 2, TOK, U), F32),
            pltpu.VMEM((4, TOK, U), BF16),
            pltpu.VMEM((4, TOK, DC), BF16),
            pltpu.VMEM((2, HALF, DC), F32),
            pltpu.VMEM((TOK, DC), BF16),
            pltpu.VMEM((2, TOK, DC), BF16),
            pltpu.SemaphoreType.DMA((N_SEM,)),
            pltpu.SemaphoreType.DMA((N_SEM,)),
            pltpu.SemaphoreType.DMA((9,)),
        ],
        compiler_params=pltpu.CompilerParams(
            collective_id=0, has_side_effects=True, vmem_limit_bytes=60 << 20
        ),
        name="ttt_layer",
    )(keys, values, queries, step_size.T, gate_weight, up_weight, down_weight)


def solution(mesh):
    finer = Mesh(mesh.devices.reshape(2, 2, 4, 2, 8), ("yh", "core", "x", "yl", "z"))
    seq, head = ("x", "yl", "z"), ("yh", "core")
    placed = (
        P(seq, head), P(seq, head), P(seq, head), P(seq, None),
        P(seq, head), P(seq, head), P(seq, head),
    )
    return jax.shard_map(body, mesh=finer, in_specs=placed, out_specs=P(seq, head), check_vma=False)
```

```python
import jax
import jax.numpy as jnp
from jax import lax
from jax.experimental import pallas as pl
from jax.experimental.pallas import tpu as pltpu
from jax.sharding import Mesh
from jax.sharding import PartitionSpec as P

EPS = 1e-06
MESH = pl.DeviceIdType.MESH
F32 = jnp.float32
BF16 = jnp.bfloat16

NX, NZ = 4, 8
TOK = 192
DC = 640
U = 384
ROWS = 80
PIECE = 20
PADDED = 48
SECOND = 24
HALF = TOK // 2
CUT = ((0, 48), (48, ROWS))
CHUNKS = ((0, 0), (0, 1), (1, 0), (1, 1))
OPP, LEFT, RIGHT, OWN = 0, 1, 2, 3
STEP = 96


def dot(a, b):
    return jnp.dot(a, b, preferred_element_type=F32)


def dot_nt(a, b):
    return lax.dot_general(a, b, (((1,), (1,)), ((), ())), preferred_element_type=F32)


def square_sums(v):
    f = v.astype(F32)
    return jnp.sum(f * f, axis=0, keepdims=True)


def far_way(kind, h):
    return h if kind == 0 else 1 - h


def kernel(
    k_hbm, v_hbm, q_hbm, s_hbm, w1_hbm, w3_hbm, w2_hbm, out_ref,
    win, kin, vin, qin, sin, wsend, warr, wg, perm, wout, kbuf, obuf, qbuf, kt, ot, ps, pb, pr, gg, hid,
    ga, gb, yfar, ysend, yrecv, rss, rsr, ybs, ybr, nw, sms, smr, qs, qr, qh, ob, op, obr, fin,
    send_sem, recv_sem, loc_sem,
):
    yh = lax.axis_index("yh")
    c = lax.axis_index("core")
    x = lax.axis_index("x")
    y = lax.axis_index("yl")
    z = lax.axis_index("z")
    xr, xl = {"x": lax.rem(x + 1, NX)}, {"x": lax.rem(x + NX - 1, NX)}
    zr, zl = {"z": lax.rem(z + 1, NZ)}, {"z": lax.rem(z + NZ - 1, NZ)}
    dr, dl = {"yl": 1 - y, **zr}, {"yl": 1 - y, **zl}
    peer, ypeer = {"core": 1 - c}, {"yl": 1 - y}
    xhalf = x // 2
    xlow = lax.rem(x, 2)
    own_w = xhalf == c

    def wtarget(j, dy):
        return {"x": 2 * c + j, "core": xhalf, "yl": y if dy == 0 else 1 - y}

    counter = [0]
    sends = []

    def ids(n):
        first = counter[0]
        counter[0] += n
        return first

    def copy(src, dst, k, to):
        return pltpu.make_async_remote_copy(
            src_ref=src, dst_ref=dst, send_sem=send_sem.at[k], recv_sem=recv_sem.at[k],
            device_id=to, device_id_type=MESH,
        )

    def send(src, dst, k, to):
        cp = copy(src, dst, k, to)
        cp.start()
        sends.append(cp)

    def arrived(ref, k, frm):
        copy(ref, ref, k, frm).wait_recv()

    barrier = pltpu.get_barrier_semaphore()
    for to in (peer, xr, xl, zr, zl, dr, dl, ypeer, wtarget(0, 1), wtarget(1, 1)):
        pl.semaphore_signal(barrier, inc=1, device_id=to, device_id_type=MESH)
    for j in range(2):
        @pl.when(jnp.logical_not(jnp.logical_and(own_w, xlow == j)))
        def _():
            pl.semaphore_signal(barrier, inc=1, device_id=wtarget(j, 0), device_id_type=MESH)

    loads = [
        pltpu.make_async_copy(w1_hbm, win.at[0], loc_sem.at[0]),
        pltpu.make_async_copy(w3_hbm, win.at[1], loc_sem.at[1]),
        pltpu.make_async_copy(w2_hbm, win.at[2], loc_sem.at[2]),
        pltpu.make_async_copy(k_hbm, kin, loc_sem.at[3]),
        pltpu.make_async_copy(v_hbm, vin, loc_sem.at[4]),
        pltpu.make_async_copy(s_hbm, sin, loc_sem.at[5]),
        pltpu.make_async_copy(q_hbm, qin, loc_sem.at[6]),
    ]
    for ld in loads:
        ld.start()

    wsend[...] = jnp.zeros_like(wsend)
    for m in range(3):
        loads[m].wait()
    for j in range(2):
        for t in range(2):
            wsend[j, t, 0:PIECE, :] = win[t, :, j * U:(j + 1) * U]
            wsend[j, t, SECOND:SECOND + PIECE, :] = win[2, :, j * U:(j + 1) * U]
    row = lax.broadcasted_iota(jnp.int32, (DC, DC), 0)
    col = lax.broadcasted_iota(jnp.int32, (DC, DC), 1)
    group = (row >= 160).astype(jnp.int32) + (row >= 320).astype(jnp.int32) + (row >= 480).astype(jnp.int32)
    rem = row - 160 * group
    step20 = jnp.zeros_like(rem)
    for t in range(1, NZ):
        step20 = step20 + (rem >= PIECE * t).astype(jnp.int32)
    wanted = ROWS * step20 + PIECE * group + rem - PIECE * step20
    perm[...] = jnp.where(col == wanted, 1.0, 0.0).astype(BF16)

    def gathered_order(v):
        return dot(v, perm[...]).astype(BF16)

    loads[3].wait()
    kbuf[OWN] = gathered_order(kin[...])
    pl.semaphore_wait(barrier, 12 - jnp.where(own_w, 1, 0))

    k_w = ids(4)
    slot = 2 * xlow + y
    w_copies = []
    for j in range(2):
        for dy in (1, 0):
            block = wsend.at[j, y if dy == 0 else 1 - y]
            cp = pltpu.make_async_remote_copy(
                src_ref=block, dst_ref=warr.at[slot],
                send_sem=send_sem.at[k_w + 2 * j + dy], recv_sem=recv_sem.at[k_w + slot],
                device_id=wtarget(j, dy), device_id_type=MESH,
            )
            if dy == 1:
                cp.start()
                sends.append(cp)
            else:
                is_self = jnp.logical_and(own_w, xlow == j)
                w_copies.append((is_self, cp))
                lc = pltpu.make_async_copy(block, warr.at[slot], loc_sem.at[7 + j])
                pl.when(jnp.logical_not(is_self))(cp.start)

                @pl.when(is_self)
                def _():
                    lc.start()
                    lc.wait()

    def x_out(buf, k):
        send(buf.at[OWN], buf.at[LEFT], k, xr)
        send(buf.at[OWN], buf.at[RIGHT], k + 1, xl)

    def x_relay(buf, k):
        arrived(buf.at[LEFT], k, xl)
        send(buf.at[LEFT, 0:HALF], buf.at[OPP, 0:HALF], k + 2, xr)
        arrived(buf.at[RIGHT], k + 1, xr)
        send(buf.at[RIGHT, HALF:TOK], buf.at[OPP, HALF:TOK], k + 3, xl)

    def x_last(buf, k):
        arrived(buf.at[OPP, 0:HALF], k + 2, xl)
        arrived(buf.at[OPP, HALF:TOK], k + 3, xr)

    k_k, k_o, k_q = ids(4), ids(4), ids(4)
    x_out(kbuf, k_k)
    loads[4].wait()
    loads[5].wait()
    diag = lax.broadcasted_iota(jnp.int32, (TOK, TOK), 0) == lax.broadcasted_iota(jnp.int32, (TOK, TOK), 1)
    rate_row = jnp.where(yh == 0, sin[0:1, :], sin[1:2, :])
    rates = jnp.sum(jnp.where(diag, rate_row, 0.0), axis=1, keepdims=True)
    obuf[OWN] = gathered_order((-(rates * vin[...].astype(F32))).astype(BF16))
    x_out(obuf, k_o)
    loads[6].wait()
    qbuf[OWN] = gathered_order(qin[...])

    for s in range(4):
        from_x, from_y = s // 2, s % 2
        here = jnp.logical_and(jnp.logical_and(own_w, xlow == from_x), y == from_y)

        @pl.when(jnp.logical_not(here))
        def _():
            copy(warr.at[s], warr.at[s], k_w + s, ypeer).wait_recv()

    prow = lax.broadcasted_iota(jnp.int32, (ROWS, 4 * PADDED), 0)
    pcol = lax.broadcasted_iota(jnp.int32, (ROWS, 4 * PADDED), 1)
    pgroup = (prow >= 20).astype(jnp.int32) + (prow >= 40).astype(jnp.int32) + (prow >= 60).astype(jnp.int32)
    pfrom = prow + (PADDED - PIECE) * pgroup
    blocks = warr[...].reshape(4 * PADDED, U)
    wg[z, 0] = dot(jnp.where(pcol == pfrom, 1.0, 0.0).astype(BF16), blocks).astype(BF16)
    wg[z, 2] = dot(jnp.where(pcol == pfrom + SECOND, 1.0, 0.0).astype(BF16), blocks).astype(BF16)

    def zpos(off):
        return lax.rem(z + off + 2 * NZ, NZ)

    def chunk(buf, at, kind, h):
        return buf.at[at, 2 * kind, CUT[h][0]:CUT[h][1]]

    def ways(step, kind, h):
        return (0, 1) if step < 4 else (far_way(kind, h),)

    def ring_id(k, step, kind, h, way):
        return k + (step - 1) * 8 + 4 * kind + 2 * h + way

    def ring_send(buf, k, step, kind, h):
        for way in ways(step, kind, h):
            ref = chunk(buf, zpos((1 - step) if way == 0 else (step - 1)), kind, h)
            send(ref, ref, ring_id(k, step, kind, h, way), zr if way == 0 else zl)

    def ring_arrived(buf, k, step, kind, h):
        for way in ways(step, kind, h):
            ref = chunk(buf, zpos(-step if way == 0 else step), kind, h)
            arrived(ref, ring_id(k, step, kind, h, way), zl if way == 0 else zr)

    def offsets(step):
        return ((0,), (-1, 1), (-2, 2), (-3, 3), (4,))[step]

    def pair_send(buf, k, step):
        for i, off in enumerate(offsets(step)):
            at = zpos(off)
            send(buf.at[at, 0], buf.at[at, 1], k + 2 * step + i, ypeer)

    def far_send(buf, k, h):
        at, rows = zpos(-3 if h == 0 else 3), pl.ds(CUT[h][0], CUT[h][1] - CUT[h][0])
        send(buf.at[at, 0, rows], buf.at[at, 1, rows], k + 8 + h, dr if h == 0 else dl)

    def far_arrived(buf, k):
        for h in range(2):
            ring_arrived(buf, k, 4, 0, h)

    def pair_arrived(buf, k):
        for step in range(4):
            for i, off in enumerate(offsets(step)):
                arrived(buf.at[zpos(off), 1], k + 2 * step + i, ypeer)
        for h in range(2):
            arrived(buf.at[zpos(4), 1, CUT[h][0]:CUT[h][1]], k + 8 + h, ypeer)

    def gather(buf, k, k_pair, step):
        for kind, h in CHUNKS:
            if step > 1:
                ring_arrived(buf, k, step - 1, kind, h)
            ring_send(buf, k, step, kind, h)
            if step == 4 and kind == 0:
                far_send(buf, k_pair, h)
            if (kind, h) == (0, 1):
                pair_send(buf, k_pair, step - 1)

    k_g, k_gp = ids(32), ids(10)
    gather(wg, k_g, k_gp, 1)
    gather(wg, k_g, k_gp, 2)
    x_relay(kbuf, k_k)
    gather(wg, k_g, k_gp, 3)
    x_relay(obuf, k_o)
    gather(wg, k_g, k_gp, 4)
    x_out(qbuf, k_q)

    def transposes(h):
        kt[:, h * U:(h + 1) * U] = kbuf[2 * h:2 * h + 2].reshape(2 * TOK, DC).T
        ot[:, h * U:(h + 1) * U] = obuf[2 * h:2 * h + 2].reshape(2 * TOK, DC).T

    transposes(1)
    far_arrived(wg, k_g)

    for h in range(2):
        ring_arrived(wg, k_g, 4, 1, h)
    k_p = ids(12)

    def p_part(b, kind):
        v = dot((obuf if kind == 2 else kbuf)[b], wg[:, kind].reshape(DC, U))
        ps[b, kind] = v
        pb[b, kind] = v.astype(BF16)
        send(pb.at[b, kind], pr.at[b, kind], k_p + 3 * b + kind, peer)

    for b in (OWN, RIGHT, LEFT):
        p_part(b, 0)
        p_part(b, 2)
    x_last(kbuf, k_k)
    p_part(OPP, 0)
    x_last(obuf, k_o)
    p_part(OPP, 2)
    pair_arrived(wg, k_gp)
    for b in (OWN, RIGHT, LEFT, OPP):
        p_part(b, 1)

    transposes(0)

    for b in (OWN, RIGHT, LEFT, OPP):
        for kind in range(3):
            arrived(pr.at[b, kind], k_p + 3 * b + kind, peer)

        @pl.loop(0, TOK // STEP)
        def _(t):
            r = pl.ds(pl.multiple_of(t * STEP, STEP), STEP)
            o = pl.ds(pl.multiple_of(b * TOK + t * STEP, STEP), STEP)
            gate = ps[b, y, r, :] + pr[b, y, r, :].astype(F32)
            up = ps[b, 1 - y, r, :] + pr[b, 1 - y, r, :].astype(F32)
            hg = ps[b, 2, r, :] + pr[b, 2, r, :].astype(F32)
            sg = jax.nn.sigmoid(gate)
            silu = gate * sg
            hid[o, :] = (silu * up).astype(BF16)
            gg[0, o, :] = (hg * up * (sg * (1.0 + gate * (1.0 - sg)))).astype(BF16)
            gg[1, o, :] = (hg * silu).astype(BF16)

    k_ya = ids(10)
    k_r = ids(32)
    far = pl.ds(pl.multiple_of(zpos(4) * ROWS, 16), ROWS)
    def rs_send(step, kind, h, way):
        lo, hi = CUT[h]
        at = zpos((5 - step) if way == 0 else (step - 5))
        v = (ga if kind == 0 else gb)[at, lo:hi]
        if kind == 0 and step > 1:
            v = v + yrecv[at, lo:hi].astype(F32)
        if kind == 0 and step == 2 and h == way:
            arrived(yfar.at[lo:hi], k_ya + 8 + h, dl if way == 0 else dr)
            v = v + yfar[lo:hi].astype(F32)
        if step > 2 or (step == 2 and far_way(kind, h) == way):
            arrived(rsr.at[way, step - 2, kind, lo:hi], ring_id(k_r, step - 1, kind, h, way), zl if way == 0 else zr)
            v = v + rsr[way, step - 2, kind, lo:hi].astype(F32)
        rss[way, step - 1, kind, lo:hi] = v.astype(BF16)
        send(
            rss.at[way, step - 1, kind, lo:hi], rsr.at[way, step - 1, kind, lo:hi],
            ring_id(k_r, step, kind, h, way), zr if way == 0 else zl,
        )

    gb[zpos(4)] = dot(ot[far, :], hid[...])
    for h in range(2):
        rs_send(1, 1, h, far_way(1, h))
    ysend[...] = dot(kt[...], gg[1 - y]).astype(BF16).reshape(NZ, ROWS, U)
    for h in range(2):
        lo, hi = CUT[h]
        send(ysend.at[zpos(4), lo:hi], yfar.at[lo:hi], k_ya + 8 + h, dr if h == 0 else dl)
    for step in (3, 2, 1, 0):
        for i, off in reversed(list(enumerate(offsets(step)))):
            at = zpos(off)
            send(ysend.at[at], yrecv.at[at], k_ya + 2 * step + i, ypeer)
    ga[zpos(4)] = dot(kt[far, :], gg[y])
    for h in range(2):
        rs_send(1, 0, h, far_way(0, h))
    gb[...] = dot(ot[...], hid[...]).reshape(NZ, ROWS, U)
    ga[...] = dot(kt[...], gg[y]).reshape(NZ, ROWS, U)

    for step in range(2, 5):
        for way in range(2):
            for h in range(2):
                rs_send(step, 1, h, way)
        for way, off in enumerate((5 - step, step - 5)):
            arrived(yrecv.at[zpos(off)], k_ya + 2 * (5 - step) + (1 - way), ypeer)
            for h in range(2):
                rs_send(step, 0, h, way)
        if step == 2:
            for m in range(3):
                sms[m:m + 1, :] = square_sums(wg[:, m].reshape(DC, U))
        if step == 3:
            x_relay(qbuf, k_q)

    def total(kind):
        for way in range(2):
            for h in range(2):
                lo, hi = CUT[h]
                arrived(rsr.at[way, 3, kind, lo:hi], ring_id(k_r, 4, kind, h, way), zl if way == 0 else zr)
        return (ga if kind == 0 else gb)[z] + rsr[0, 3, kind].astype(F32) + rsr[1, 3, kind].astype(F32)

    k_yb = ids(1)
    tb = total(1)
    gb[z] = tb
    ybs[...] = tb.astype(BF16)
    send(ybs, ybr, k_yb, ypeer)
    arrived(yrecv.at[z], k_ya, ypeer)
    ta = total(0) + yrecv[z].astype(F32)
    nw[z, 0] = (wg[z, 0].astype(F32) - ta).astype(BF16)
    k_n, k_np = ids(32), ids(10)
    for h in range(2):
        ring_send(nw, k_n, 1, 0, h)
    pair_send(nw, k_np, 0)
    arrived(ybr, k_yb, ypeer)
    nw[z, 2] = (wg[z, 2].astype(F32) - (gb[z] + ybr[...].astype(F32))).astype(BF16)
    for h in range(2):
        ring_send(nw, k_n, 1, 1, h)
    x_last(qbuf, k_q)
    for step in range(2, 5):
        gather(nw, k_n, k_np, step)
    far_arrived(nw, k_n)

    k_qp = ids(8)
    k_s = ids(1)

    def q_part(b, kind):
        qs[b, kind] = dot(qbuf[b], nw[:, kind].reshape(DC, U))
        send(qs.at[b, kind], qr.at[b, kind], k_qp + 2 * b + kind, peer)

    for b in range(4):
        q_part(b, 0)
    for h in range(2):
        ring_arrived(nw, k_n, 4, 1, h)
    sms[3:4, :] = square_sums(nw[:, 0].reshape(DC, U))
    sms[5:6, :] = square_sums(nw[:, 2].reshape(DC, U))
    sms[6:8, :] = jnp.zeros((2, U), F32)
    wout[...] = dot(perm[...], nw[:, 2].reshape(DC, U)).astype(BF16)
    pair_arrived(nw, k_np)
    q_part(OPP, 1)
    sms[4:5, :] = square_sums(nw[:, 1].reshape(DC, U))
    send(sms, smr, k_s, peer)
    q_part(LEFT, 1)
    arrived(smr, k_s, peer)
    sums = sms[...] + smr[...]
    ra, rb, r2 = [jnp.sqrt((sums[m:m + 1] + EPS) / (sums[3 + m:4 + m] + EPS)) for m in range(3)]
    r1, r3 = jnp.where(y == 0, ra, rb), jnp.where(y == 0, rb, ra)

    def out_part(b):
        for kind in range(2):
            arrived(qr.at[b, kind], k_qp + 2 * b + kind, peer)

        @pl.loop(0, TOK // STEP)
        def _(t):
            r = pl.ds(pl.multiple_of(t * STEP, STEP), STEP)
            qg = (qs[b, y, r, :] + qr[b, y, r, :]) * r1
            qu = (qs[b, 1 - y, r, :] + qr[b, 1 - y, r, :]) * r3
            qh[b, r, :] = (qg * jax.nn.sigmoid(qg) * qu * r2).astype(BF16)

        return dot_nt(qh[b], wout[...])

    k_x = ids(6)
    part = out_part(OPP)
    ob[OPP] = part.astype(BF16)
    send(ob.at[OPP, 0:HALF], obr.at[0:HALF], k_x, xr)
    send(ob.at[OPP, HALF:TOK], obr.at[HALF:TOK], k_x + 1, xl)
    q_part(RIGHT, 1)
    part = out_part(LEFT)
    ob[LEFT, 0:HALF] = part[0:HALF].astype(BF16)
    send(ob.at[LEFT, 0:HALF], fin.at[1, 0:HALF], k_x + 2, xl)
    op[0] = part[HALF:TOK]
    q_part(OWN, 1)
    part = out_part(RIGHT)
    ob[RIGHT, HALF:TOK] = part[HALF:TOK].astype(BF16)
    send(ob.at[RIGHT, HALF:TOK], fin.at[0, HALF:TOK], k_x + 4, xr)
    op[1] = part[0:HALF]
    arrived(obr.at[HALF:TOK], k_x + 1, xr)
    ob[LEFT, HALF:TOK] = (op[0] + obr[HALF:TOK].astype(F32)).astype(BF16)
    send(ob.at[LEFT, HALF:TOK], fin.at[1, HALF:TOK], k_x + 3, xl)
    arrived(obr.at[0:HALF], k_x, xl)
    ob[RIGHT, 0:HALF] = (op[1] + obr[0:HALF].astype(F32)).astype(BF16)
    send(ob.at[RIGHT, 0:HALF], fin.at[0, 0:HALF], k_x + 5, xr)
    part = out_part(OWN)
    arrived(fin.at[1, 0:HALF], k_x + 2, xr)
    arrived(fin.at[1, HALF:TOK], k_x + 3, xr)
    arrived(fin.at[0, HALF:TOK], k_x + 4, xl)
    arrived(fin.at[0, 0:HALF], k_x + 5, xl)
    out_ref[...] = (part + fin[0].astype(F32) + fin[1].astype(F32)).astype(BF16)

    for cp in sends:
        cp.wait_send()
    for is_self, cp in w_copies:
        pl.when(jnp.logical_not(is_self))(cp.wait_send)


N_SEM = 4 + 12 + 42 + 12 + 42 + 1 + 42 + 9 + 6


def body(keys, values, queries, step_size, gate_weight, up_weight, down_weight):
    hbm = pl.BlockSpec(memory_space=pl.ANY)
    return pl.pallas_call(
        kernel,
        out_shape=jax.ShapeDtypeStruct((TOK, DC), BF16),
        in_specs=[hbm] * 7,
        out_specs=pl.BlockSpec(memory_space=pltpu.VMEM),
        scratch_shapes=[
            pltpu.VMEM((3, PIECE, 2 * U), BF16),
            pltpu.VMEM((TOK, DC), BF16),
            pltpu.VMEM((TOK, DC), BF16),
            pltpu.VMEM((TOK, DC), BF16),
            pltpu.VMEM((2, TOK), F32),
            pltpu.VMEM((2, 2, PADDED, U), BF16),
            pltpu.VMEM((4, PADDED, U), BF16),
            pltpu.VMEM((NZ, 3, ROWS, U), BF16),
            pltpu.VMEM((DC, DC), BF16),
            pltpu.VMEM((DC, U), BF16),
            pltpu.VMEM((4, TOK, DC), BF16),
            pltpu.VMEM((4, TOK, DC), BF16),
            pltpu.VMEM((4, TOK, DC), BF16),
            pltpu.VMEM((DC, 4 * TOK), BF16),
            pltpu.VMEM((DC, 4 * TOK), BF16),
            pltpu.VMEM((4, 3, TOK, U), F32),
            pltpu.VMEM((4, 3, TOK, U), BF16),
            pltpu.VMEM((4, 3, TOK, U), BF16),
            pltpu.VMEM((2, 4 * TOK, U), BF16),
            pltpu.VMEM((4 * TOK, U), BF16),
            pltpu.VMEM((NZ, ROWS, U), F32),
            pltpu.VMEM((NZ, ROWS, U), F32),
            pltpu.VMEM((ROWS, U), BF16),
            pltpu.VMEM((NZ, ROWS, U), BF16),
            pltpu.VMEM((NZ, ROWS, U), BF16),
            pltpu.VMEM((2, 4, 2, ROWS, U), BF16),
            pltpu.VMEM((2, 4, 2, ROWS, U), BF16),
            pltpu.VMEM((ROWS, U), BF16),
            pltpu.VMEM((ROWS, U), BF16),
            pltpu.VMEM((NZ, 3, ROWS, U), BF16),
            pltpu.VMEM((8, U), F32),
            pltpu.VMEM((8, U), F32),
            pltpu.VMEM((4, 2, TOK, U), F32),
            pltpu.VMEM((4, 2, TOK, U), F32),
            pltpu.VMEM((4, TOK, U), BF16),
            pltpu.VMEM((4, TOK, DC), BF16),
            pltpu.VMEM((2, HALF, DC), F32),
            pltpu.VMEM((TOK, DC), BF16),
            pltpu.VMEM((2, TOK, DC), BF16),
            pltpu.SemaphoreType.DMA((N_SEM,)),
            pltpu.SemaphoreType.DMA((N_SEM,)),
            pltpu.SemaphoreType.DMA((9,)),
        ],
        compiler_params=pltpu.CompilerParams(
            collective_id=0, has_side_effects=True, vmem_limit_bytes=60 << 20
        ),
        name="ttt_layer",
    )(keys, values, queries, step_size.T, gate_weight, up_weight, down_weight)


def solution(mesh):
    finer = Mesh(mesh.devices.reshape(2, 2, 4, 2, 8), ("yh", "core", "x", "yl", "z"))
    seq, head = ("x", "yl", "z"), ("yh", "core")
    placed = (
        P(seq, head), P(seq, head), P(seq, head), P(seq, None),
        P(seq, head), P(seq, head), P(seq, head),
    )
    return jax.shard_map(body, mesh=finer, in_specs=placed, out_specs=P(seq, head), check_vma=False)
```

```python
import jax
import jax.numpy as jnp
from jax import lax
from jax.experimental import pallas as pl
from jax.experimental.pallas import tpu as pltpu
from jax.sharding import Mesh
from jax.sharding import PartitionSpec as P

EPS = 1e-06
MESH = pl.DeviceIdType.MESH
F32 = jnp.float32
BF16 = jnp.bfloat16

NX, NZ = 4, 8
TOK = 192
DC = 640
U = 384
ROWS = 80
PIECE = 20
PADDED = 48
SECOND = 24
HALF = TOK // 2
CUT = ((0, 48), (48, ROWS))
CHUNKS = ((0, 0), (0, 1), (1, 0), (1, 1))
OPP, LEFT, RIGHT, OWN = 0, 1, 2, 3
STEP = 96


def dot(a, b):
    return jnp.dot(a, b, preferred_element_type=F32)


def dot_nt(a, b):
    return lax.dot_general(a, b, (((1,), (1,)), ((), ())), preferred_element_type=F32)


def square_sums(v):
    f = v.astype(F32)
    return jnp.sum(f * f, axis=0, keepdims=True)


def far_way(kind, h):
    return h if kind == 0 else 1 - h


def kernel(
    k_hbm, v_hbm, q_hbm, s_hbm, w1_hbm, w3_hbm, w2_hbm, out_ref,
    win, kin, vin, qin, sin, wsend, warr, wg, perm, wout, kbuf, obuf, qbuf, kt, ot, ps, pb, pr, gg, hid,
    ga, gb, yfar, ysend, yrecv, rss, rsr, ybs, ybr, nw, sms, smr, qs, qr, qh, ob, op, obr, fin,
    send_sem, recv_sem, loc_sem,
):
    yh = lax.axis_index("yh")
    c = lax.axis_index("core")
    x = lax.axis_index("x")
    y = lax.axis_index("yl")
    z = lax.axis_index("z")
    xr, xl = {"x": lax.rem(x + 1, NX)}, {"x": lax.rem(x + NX - 1, NX)}
    zr, zl = {"z": lax.rem(z + 1, NZ)}, {"z": lax.rem(z + NZ - 1, NZ)}
    dr, dl = {"yl": 1 - y, **zr}, {"yl": 1 - y, **zl}
    peer, ypeer = {"core": 1 - c}, {"yl": 1 - y}
    xhalf = x // 2
    xlow = lax.rem(x, 2)
    own_w = xhalf == c

    def wtarget(j, dy):
        return {"x": 2 * c + j, "core": xhalf, "yl": y if dy == 0 else 1 - y}

    counter = [0]
    sends = []

    def ids(n):
        first = counter[0]
        counter[0] += n
        return first

    def copy(src, dst, k, to):
        return pltpu.make_async_remote_copy(
            src_ref=src, dst_ref=dst, send_sem=send_sem.at[k], recv_sem=recv_sem.at[k],
            device_id=to, device_id_type=MESH,
        )

    def send(src, dst, k, to):
        cp = copy(src, dst, k, to)
        cp.start()
        sends.append(cp)

    def arrived(ref, k, frm):
        copy(ref, ref, k, frm).wait_recv()

    barrier = pltpu.get_barrier_semaphore()
    for to in (peer, xr, xl, zr, zl, dr, dl, ypeer, wtarget(0, 1), wtarget(1, 1)):
        pl.semaphore_signal(barrier, inc=1, device_id=to, device_id_type=MESH)
    for j in range(2):
        @pl.when(jnp.logical_not(jnp.logical_and(own_w, xlow == j)))
        def _():
            pl.semaphore_signal(barrier, inc=1, device_id=wtarget(j, 0), device_id_type=MESH)

    loads = [
        pltpu.make_async_copy(w1_hbm, win.at[0], loc_sem.at[0]),
        pltpu.make_async_copy(w3_hbm, win.at[1], loc_sem.at[1]),
        pltpu.make_async_copy(w2_hbm, win.at[2], loc_sem.at[2]),
        pltpu.make_async_copy(k_hbm, kin, loc_sem.at[3]),
        pltpu.make_async_copy(v_hbm, vin, loc_sem.at[4]),
        pltpu.make_async_copy(s_hbm, sin, loc_sem.at[5]),
        pltpu.make_async_copy(q_hbm, qin, loc_sem.at[6]),
    ]
    for ld in loads:
        ld.start()

    wsend[...] = jnp.zeros_like(wsend)
    for m in range(3):
        loads[m].wait()
    for j in range(2):
        for t in range(2):
            wsend[j, t, 0:PIECE, :] = win[t, :, j * U:(j + 1) * U]
            wsend[j, t, SECOND:SECOND + PIECE, :] = win[2, :, j * U:(j + 1) * U]
    pl.semaphore_wait(barrier, 12 - jnp.where(own_w, 1, 0))

    k_w = ids(4)
    slot = 2 * xlow + y
    w_copies = []
    for j in range(2):
        for dy in (1, 0):
            block = wsend.at[j, y if dy == 0 else 1 - y]
            cp = pltpu.make_async_remote_copy(
                src_ref=block, dst_ref=warr.at[slot],
                send_sem=send_sem.at[k_w + 2 * j + dy], recv_sem=recv_sem.at[k_w + slot],
                device_id=wtarget(j, dy), device_id_type=MESH,
            )
            if dy == 1:
                cp.start()
                sends.append(cp)
            else:
                is_self = jnp.logical_and(own_w, xlow == j)
                w_copies.append((is_self, cp))
                lc = pltpu.make_async_copy(block, warr.at[slot], loc_sem.at[7 + j])
                pl.when(jnp.logical_not(is_self))(cp.start)

                @pl.when(is_self)
                def _():
                    lc.start()
                    lc.wait()

    row = lax.broadcasted_iota(jnp.int32, (DC, DC), 0)
    col = lax.broadcasted_iota(jnp.int32, (DC, DC), 1)
    group = (row >= 160).astype(jnp.int32) + (row >= 320).astype(jnp.int32) + (row >= 480).astype(jnp.int32)
    rem = row - 160 * group
    step20 = jnp.zeros_like(rem)
    for t in range(1, NZ):
        step20 = step20 + (rem >= PIECE * t).astype(jnp.int32)
    wanted = ROWS * step20 + PIECE * group + rem - PIECE * step20
    perm[...] = jnp.where(col == wanted, 1.0, 0.0).astype(BF16)

    def gathered_order(v):
        return dot(v, perm[...]).astype(BF16)

    loads[3].wait()
    kbuf[OWN] = gathered_order(kin[...])

    def x_out(buf, k):
        send(buf.at[OWN], buf.at[LEFT], k, xr)
        send(buf.at[OWN], buf.at[RIGHT], k + 1, xl)

    def x_relay(buf, k):
        arrived(buf.at[LEFT], k, xl)
        send(buf.at[LEFT, 0:HALF], buf.at[OPP, 0:HALF], k + 2, xr)
        arrived(buf.at[RIGHT], k + 1, xr)
        send(buf.at[RIGHT, HALF:TOK], buf.at[OPP, HALF:TOK], k + 3, xl)

    def x_last(buf, k):
        arrived(buf.at[OPP, 0:HALF], k + 2, xl)
        arrived(buf.at[OPP, HALF:TOK], k + 3, xr)

    k_k, k_o, k_q = ids(4), ids(4), ids(4)
    x_out(kbuf, k_k)
    loads[4].wait()
    loads[5].wait()
    diag = lax.broadcasted_iota(jnp.int32, (TOK, TOK), 0) == lax.broadcasted_iota(jnp.int32, (TOK, TOK), 1)
    rate_row = jnp.where(yh == 0, sin[0:1, :], sin[1:2, :])
    rates = jnp.sum(jnp.where(diag, rate_row, 0.0), axis=1, keepdims=True)
    obuf[OWN] = gathered_order((-(rates * vin[...].astype(F32))).astype(BF16))
    x_out(obuf, k_o)
    loads[6].wait()
    qbuf[OWN] = gathered_order(qin[...])

    for s in range(4):
        from_x, from_y = s // 2, s % 2
        here = jnp.logical_and(jnp.logical_and(own_w, xlow == from_x), y == from_y)

        @pl.when(jnp.logical_not(here))
        def _():
            copy(warr.at[s], warr.at[s], k_w + s, ypeer).wait_recv()

    prow = lax.broadcasted_iota(jnp.int32, (ROWS, 4 * PADDED), 0)
    pcol = lax.broadcasted_iota(jnp.int32, (ROWS, 4 * PADDED), 1)
    pgroup = (prow >= 20).astype(jnp.int32) + (prow >= 40).astype(jnp.int32) + (prow >= 60).astype(jnp.int32)
    pfrom = prow + (PADDED - PIECE) * pgroup
    blocks = warr[...].reshape(4 * PADDED, U)
    wg[z, 0] = dot(jnp.where(pcol == pfrom, 1.0, 0.0).astype(BF16), blocks).astype(BF16)
    wg[z, 2] = dot(jnp.where(pcol == pfrom + SECOND, 1.0, 0.0).astype(BF16), blocks).astype(BF16)

    def zpos(off):
        return lax.rem(z + off + 2 * NZ, NZ)

    def chunk(buf, at, kind, h):
        return buf.at[at, 2 * kind, CUT[h][0]:CUT[h][1]]

    def ways(step, kind, h):
        return (0, 1) if step < 4 else (far_way(kind, h),)

    def ring_id(k, step, kind, h, way):
        return k + (step - 1) * 8 + 4 * kind + 2 * h + way

    def ring_send(buf, k, step, kind, h):
        for way in ways(step, kind, h):
            ref = chunk(buf, zpos((1 - step) if way == 0 else (step - 1)), kind, h)
            send(ref, ref, ring_id(k, step, kind, h, way), zr if way == 0 else zl)

    def ring_arrived(buf, k, step, kind, h):
        for way in ways(step, kind, h):
            ref = chunk(buf, zpos(-step if way == 0 else step), kind, h)
            arrived(ref, ring_id(k, step, kind, h, way), zl if way == 0 else zr)

    def offsets(step):
        return ((0,), (-1, 1), (-2, 2), (-3, 3), (4,))[step]

    def pair_send(buf, k, step):
        for i, off in enumerate(offsets(step)):
            at = zpos(off)
            send(buf.at[at, 0], buf.at[at, 1], k + 2 * step + i, ypeer)

    def far_send(buf, k, h):
        at, rows = zpos(-3 if h == 0 else 3), pl.ds(CUT[h][0], CUT[h][1] - CUT[h][0])
        send(buf.at[at, 0, rows], buf.at[at, 1, rows], k + 8 + h, dr if h == 0 else dl)

    def far_arrived(buf, k):
        for h in range(2):
            ring_arrived(buf, k, 4, 0, h)

    def pair_arrived(buf, k):
        for step in range(4):
            for i, off in enumerate(offsets(step)):
                arrived(buf.at[zpos(off), 1], k + 2 * step + i, ypeer)
        for h in range(2):
            arrived(buf.at[zpos(4), 1, CUT[h][0]:CUT[h][1]], k + 8 + h, ypeer)

    def gather(buf, k, k_pair, step):
        for kind, h in CHUNKS:
            if step > 1:
                ring_arrived(buf, k, step - 1, kind, h)
            ring_send(buf, k, step, kind, h)
            if step == 4 and kind == 0:
                far_send(buf, k_pair, h)
            if (kind, h) == (0, 1):
                pair_send(buf, k_pair, step - 1)

    k_g, k_gp = ids(32), ids(10)
    gather(wg, k_g, k_gp, 1)
    gather(wg, k_g, k_gp, 2)
    x_relay(kbuf, k_k)
    gather(wg, k_g, k_gp, 3)
    x_relay(obuf, k_o)
    gather(wg, k_g, k_gp, 4)
    x_out(qbuf, k_q)

    def transposes(h):
        kt[:, h * U:(h + 1) * U] = kbuf[2 * h:2 * h + 2].reshape(2 * TOK, DC).T
        ot[:, h * U:(h + 1) * U] = obuf[2 * h:2 * h + 2].reshape(2 * TOK, DC).T

    transposes(1)
    far_arrived(wg, k_g)

    for h in range(2):
        ring_arrived(wg, k_g, 4, 1, h)
    k_p = ids(12)

    def p_part(b, kind):
        v = dot((obuf if kind == 2 else kbuf)[b], wg[:, kind].reshape(DC, U))
        ps[b, kind] = v
        pb[b, kind] = v.astype(BF16)
        send(pb.at[b, kind], pr.at[b, kind], k_p + 3 * b + kind, peer)

    for b in (OWN, RIGHT, LEFT):
        p_part(b, 0)
        p_part(b, 2)
    x_last(kbuf, k_k)
    p_part(OPP, 0)
    x_last(obuf, k_o)
    p_part(OPP, 2)
    pair_arrived(wg, k_gp)
    for b in (OWN, RIGHT, LEFT, OPP):
        p_part(b, 1)

    transposes(0)

    for b in (OWN, RIGHT, LEFT, OPP):
        for kind in range(3):
            arrived(pr.at[b, kind], k_p + 3 * b + kind, peer)

        @pl.loop(0, TOK // STEP)
        def _(t):
            r = pl.ds(pl.multiple_of(t * STEP, STEP), STEP)
            o = pl.ds(pl.multiple_of(b * TOK + t * STEP, STEP), STEP)
            gate = ps[b, y, r, :] + pr[b, y, r, :].astype(F32)
            up = ps[b, 1 - y, r, :] + pr[b, 1 - y, r, :].astype(F32)
            hg = ps[b, 2, r, :] + pr[b, 2, r, :].astype(F32)
            sg = jax.nn.sigmoid(gate)
            silu = gate * sg
            hid[o, :] = (silu * up).astype(BF16)
            gg[0, o, :] = (hg * up * (sg * (1.0 + gate * (1.0 - sg)))).astype(BF16)
            gg[1, o, :] = (hg * silu).astype(BF16)

    k_ya = ids(10)
    k_r = ids(32)
    far = pl.ds(pl.multiple_of(zpos(4) * ROWS, 16), ROWS)
    def rs_send(step, kind, h, way):
        lo, hi = CUT[h]
        at = zpos((5 - step) if way == 0 else (step - 5))
        v = (ga if kind == 0 else gb)[at, lo:hi]
        if kind == 0 and step > 1:
            v = v + yrecv[at, lo:hi].astype(F32)
        if kind == 0 and step == 2 and h == way:
            arrived(yfar.at[lo:hi], k_ya + 8 + h, dl if way == 0 else dr)
            v = v + yfar[lo:hi].astype(F32)
        if step > 2 or (step == 2 and far_way(kind, h) == way):
            arrived(rsr.at[way, step - 2, kind, lo:hi], ring_id(k_r, step - 1, kind, h, way), zl if way == 0 else zr)
            v = v + rsr[way, step - 2, kind, lo:hi].astype(F32)
        rss[way, step - 1, kind, lo:hi] = v.astype(BF16)
        send(
            rss.at[way, step - 1, kind, lo:hi], rsr.at[way, step - 1, kind, lo:hi],
            ring_id(k_r, step, kind, h, way), zr if way == 0 else zl,
        )

    gb[zpos(4)] = dot(ot[far, :], hid[...])
    for h in range(2):
        rs_send(1, 1, h, far_way(1, h))
    ysend[...] = dot(kt[...], gg[1 - y]).astype(BF16).reshape(NZ, ROWS, U)
    for h in range(2):
        lo, hi = CUT[h]
        send(ysend.at[zpos(4), lo:hi], yfar.at[lo:hi], k_ya + 8 + h, dr if h == 0 else dl)
    for step in (3, 2, 1, 0):
        for i, off in reversed(list(enumerate(offsets(step)))):
            at = zpos(off)
            send(ysend.at[at], yrecv.at[at], k_ya + 2 * step + i, ypeer)
    ga[zpos(4)] = dot(kt[far, :], gg[y])
    for h in range(2):
        rs_send(1, 0, h, far_way(0, h))
    gb[...] = dot(ot[...], hid[...]).reshape(NZ, ROWS, U)
    ga[...] = dot(kt[...], gg[y]).reshape(NZ, ROWS, U)

    for step in range(2, 5):
        for way in range(2):
            for h in range(2):
                rs_send(step, 1, h, way)
        for way, off in enumerate((5 - step, step - 5)):
            arrived(yrecv.at[zpos(off)], k_ya + 2 * (5 - step) + (1 - way), ypeer)
            for h in range(2):
                rs_send(step, 0, h, way)
        if step == 2:
            for m in range(3):
                sms[m:m + 1, :] = square_sums(wg[:, m].reshape(DC, U))
        if step == 3:
            x_relay(qbuf, k_q)

    def total(kind):
        for way in range(2):
            for h in range(2):
                lo, hi = CUT[h]
                arrived(rsr.at[way, 3, kind, lo:hi], ring_id(k_r, 4, kind, h, way), zl if way == 0 else zr)
        return (ga if kind == 0 else gb)[z] + rsr[0, 3, kind].astype(F32) + rsr[1, 3, kind].astype(F32)

    k_yb = ids(1)
    tb = total(1)
    gb[z] = tb
    ybs[...] = tb.astype(BF16)
    send(ybs, ybr, k_yb, ypeer)
    arrived(yrecv.at[z], k_ya, ypeer)
    ta = total(0) + yrecv[z].astype(F32)
    nw[z, 0] = (wg[z, 0].astype(F32) - ta).astype(BF16)
    k_n, k_np = ids(32), ids(10)
    for h in range(2):
        ring_send(nw, k_n, 1, 0, h)
    pair_send(nw, k_np, 0)
    arrived(ybr, k_yb, ypeer)
    nw[z, 2] = (wg[z, 2].astype(F32) - (gb[z] + ybr[...].astype(F32))).astype(BF16)
    for h in range(2):
        ring_send(nw, k_n, 1, 1, h)
    x_last(qbuf, k_q)
    for step in range(2, 5):
        gather(nw, k_n, k_np, step)
    far_arrived(nw, k_n)

    k_qp = ids(8)
    k_s = ids(1)

    def q_part(b, kind):
        qs[b, kind] = dot(qbuf[b], nw[:, kind].reshape(DC, U))
        send(qs.at[b, kind], qr.at[b, kind], k_qp + 2 * b + kind, peer)

    for b in range(4):
        q_part(b, 0)
    for h in range(2):
        ring_arrived(nw, k_n, 4, 1, h)
    sms[3:4, :] = square_sums(nw[:, 0].reshape(DC, U))
    sms[5:6, :] = square_sums(nw[:, 2].reshape(DC, U))
    sms[6:8, :] = jnp.zeros((2, U), F32)
    wout[...] = dot(perm[...], nw[:, 2].reshape(DC, U)).astype(BF16)
    pair_arrived(nw, k_np)
    q_part(OPP, 1)
    sms[4:5, :] = square_sums(nw[:, 1].reshape(DC, U))
    send(sms, smr, k_s, peer)
    q_part(LEFT, 1)
    arrived(smr, k_s, peer)
    sums = sms[...] + smr[...]
    ra, rb, r2 = [jnp.sqrt((sums[m:m + 1] + EPS) / (sums[3 + m:4 + m] + EPS)) for m in range(3)]
    r1, r3 = jnp.where(y == 0, ra, rb), jnp.where(y == 0, rb, ra)

    def out_part(b):
        for kind in range(2):
            arrived(qr.at[b, kind], k_qp + 2 * b + kind, peer)

        @pl.loop(0, TOK // STEP)
        def _(t):
            r = pl.ds(pl.multiple_of(t * STEP, STEP), STEP)
            qg = (qs[b, y, r, :] + qr[b, y, r, :]) * r1
            qu = (qs[b, 1 - y, r, :] + qr[b, 1 - y, r, :]) * r3
            qh[b, r, :] = (qg * jax.nn.sigmoid(qg) * qu * r2).astype(BF16)

        return dot_nt(qh[b], wout[...])

    k_x = ids(6)
    part = out_part(OPP)
    ob[OPP] = part.astype(BF16)
    send(ob.at[OPP, 0:HALF], obr.at[0:HALF], k_x, xr)
    send(ob.at[OPP, HALF:TOK], obr.at[HALF:TOK], k_x + 1, xl)
    q_part(RIGHT, 1)
    part = out_part(LEFT)
    ob[LEFT, 0:HALF] = part[0:HALF].astype(BF16)
    send(ob.at[LEFT, 0:HALF], fin.at[1, 0:HALF], k_x + 2, xl)
    op[0] = part[HALF:TOK]
    q_part(OWN, 1)
    part = out_part(RIGHT)
    ob[RIGHT, HALF:TOK] = part[HALF:TOK].astype(BF16)
    send(ob.at[RIGHT, HALF:TOK], fin.at[0, HALF:TOK], k_x + 4, xr)
    op[1] = part[0:HALF]
    arrived(obr.at[HALF:TOK], k_x + 1, xr)
    ob[LEFT, HALF:TOK] = (op[0] + obr[HALF:TOK].astype(F32)).astype(BF16)
    send(ob.at[LEFT, HALF:TOK], fin.at[1, HALF:TOK], k_x + 3, xl)
    arrived(obr.at[0:HALF], k_x, xl)
    ob[RIGHT, 0:HALF] = (op[1] + obr[0:HALF].astype(F32)).astype(BF16)
    send(ob.at[RIGHT, 0:HALF], fin.at[0, 0:HALF], k_x + 5, xr)
    part = out_part(OWN)
    arrived(fin.at[1, 0:HALF], k_x + 2, xr)
    arrived(fin.at[1, HALF:TOK], k_x + 3, xr)
    arrived(fin.at[0, HALF:TOK], k_x + 4, xl)
    arrived(fin.at[0, 0:HALF], k_x + 5, xl)
    out_ref[...] = (part + fin[0].astype(F32) + fin[1].astype(F32)).astype(BF16)

    for cp in sends:
        cp.wait_send()
    for is_self, cp in w_copies:
        pl.when(jnp.logical_not(is_self))(cp.wait_send)


N_SEM = 4 + 12 + 42 + 12 + 42 + 1 + 42 + 9 + 6


def body(keys, values, queries, step_size, gate_weight, up_weight, down_weight):
    hbm = pl.BlockSpec(memory_space=pl.ANY)
    return pl.pallas_call(
        kernel,
        out_shape=jax.ShapeDtypeStruct((TOK, DC), BF16),
        in_specs=[hbm] * 7,
        out_specs=pl.BlockSpec(memory_space=pltpu.VMEM),
        scratch_shapes=[
            pltpu.VMEM((3, PIECE, 2 * U), BF16),
            pltpu.VMEM((TOK, DC), BF16),
            pltpu.VMEM((TOK, DC), BF16),
            pltpu.VMEM((TOK, DC), BF16),
            pltpu.VMEM((2, TOK), F32),
            pltpu.VMEM((2, 2, PADDED, U), BF16),
            pltpu.VMEM((4, PADDED, U), BF16),
            pltpu.VMEM((NZ, 3, ROWS, U), BF16),
            pltpu.VMEM((DC, DC), BF16),
            pltpu.VMEM((DC, U), BF16),
            pltpu.VMEM((4, TOK, DC), BF16),
            pltpu.VMEM((4, TOK, DC), BF16),
            pltpu.VMEM((4, TOK, DC), BF16),
            pltpu.VMEM((DC, 4 * TOK), BF16),
            pltpu.VMEM((DC, 4 * TOK), BF16),
            pltpu.VMEM((4, 3, TOK, U), F32),
            pltpu.VMEM((4, 3, TOK, U), BF16),
            pltpu.VMEM((4, 3, TOK, U), BF16),
            pltpu.VMEM((2, 4 * TOK, U), BF16),
            pltpu.VMEM((4 * TOK, U), BF16),
            pltpu.VMEM((NZ, ROWS, U), F32),
            pltpu.VMEM((NZ, ROWS, U), F32),
            pltpu.VMEM((ROWS, U), BF16),
            pltpu.VMEM((NZ, ROWS, U), BF16),
            pltpu.VMEM((NZ, ROWS, U), BF16),
            pltpu.VMEM((2, 4, 2, ROWS, U), BF16),
            pltpu.VMEM((2, 4, 2, ROWS, U), BF16),
            pltpu.VMEM((ROWS, U), BF16),
            pltpu.VMEM((ROWS, U), BF16),
            pltpu.VMEM((NZ, 3, ROWS, U), BF16),
            pltpu.VMEM((8, U), F32),
            pltpu.VMEM((8, U), F32),
            pltpu.VMEM((4, 2, TOK, U), F32),
            pltpu.VMEM((4, 2, TOK, U), F32),
            pltpu.VMEM((4, TOK, U), BF16),
            pltpu.VMEM((4, TOK, DC), BF16),
            pltpu.VMEM((2, HALF, DC), F32),
            pltpu.VMEM((TOK, DC), BF16),
            pltpu.VMEM((2, TOK, DC), BF16),
            pltpu.SemaphoreType.DMA((N_SEM,)),
            pltpu.SemaphoreType.DMA((N_SEM,)),
            pltpu.SemaphoreType.DMA((9,)),
        ],
        compiler_params=pltpu.CompilerParams(
            collective_id=0, has_side_effects=True, vmem_limit_bytes=60 << 20
        ),
        name="ttt_layer",
    )(keys, values, queries, step_size.T, gate_weight, up_weight, down_weight)


def solution(mesh):
    finer = Mesh(mesh.devices.reshape(2, 2, 4, 2, 8), ("yh", "core", "x", "yl", "z"))
    seq, head = ("x", "yl", "z"), ("yh", "core")
    placed = (
        P(seq, head), P(seq, head), P(seq, head), P(seq, None),
        P(seq, head), P(seq, head), P(seq, head),
    )
    return jax.shard_map(body, mesh=finer, in_specs=placed, out_specs=P(seq, head), check_vma=False)
```

```python
import jax
import jax.numpy as jnp
from jax import lax
from jax.experimental import pallas as pl
from jax.experimental.pallas import tpu as pltpu
from jax.sharding import Mesh
from jax.sharding import PartitionSpec as P

EPS = 1e-06
MESH = pl.DeviceIdType.MESH
F32 = jnp.float32
BF16 = jnp.bfloat16

NX, NZ = 4, 8
TOK = 192
DC = 640
U = 384
ROWS = 80
PIECE = 20
PADDED = 48
SECOND = 24
HALF = TOK // 2
CUT = ((0, 48), (48, ROWS))
CHUNKS = ((0, 0), (0, 1), (1, 0), (1, 1))
OPP, LEFT, RIGHT, OWN = 0, 1, 2, 3
STEP = 96


def dot(a, b):
    return jnp.dot(a, b, preferred_element_type=F32)


def dot_nt(a, b):
    return lax.dot_general(a, b, (((1,), (1,)), ((), ())), preferred_element_type=F32)


def square_sums(v):
    f = v.astype(F32)
    return jnp.sum(f * f, axis=0, keepdims=True)


def far_way(kind, h):
    return h if kind == 0 else 1 - h


def kernel(
    k_hbm, v_hbm, q_hbm, s_hbm, w1_hbm, w3_hbm, w2_hbm, out_ref,
    win, kin, vin, qin, sin, wsend, warr, wg, perm, wout, kbuf, obuf, qbuf, kt, ot, ps, pb, pr, gg, hid,
    ga, gb, yfar, ysend, yrecv, rss, rsr, ybs, ybr, nw, sms, smr, qs, qr, qh, ob, op, obr, fin,
    send_sem, recv_sem, loc_sem,
):
    yh = lax.axis_index("yh")
    c = lax.axis_index("core")
    x = lax.axis_index("x")
    y = lax.axis_index("yl")
    z = lax.axis_index("z")
    xr, xl = {"x": lax.rem(x + 1, NX)}, {"x": lax.rem(x + NX - 1, NX)}
    zr, zl = {"z": lax.rem(z + 1, NZ)}, {"z": lax.rem(z + NZ - 1, NZ)}
    dr, dl = {"yl": 1 - y, **zr}, {"yl": 1 - y, **zl}
    peer, ypeer = {"core": 1 - c}, {"yl": 1 - y}
    xhalf = x // 2
    xlow = lax.rem(x, 2)
    own_w = xhalf == c

    def wtarget(j, dy):
        return {"x": 2 * c + j, "core": xhalf, "yl": y if dy == 0 else 1 - y}

    counter = [0]
    sends = []

    def ids(n):
        first = counter[0]
        counter[0] += n
        return first

    def copy(src, dst, k, to):
        return pltpu.make_async_remote_copy(
            src_ref=src, dst_ref=dst, send_sem=send_sem.at[k], recv_sem=recv_sem.at[k],
            device_id=to, device_id_type=MESH,
        )

    def send(src, dst, k, to):
        cp = copy(src, dst, k, to)
        cp.start()
        sends.append(cp)

    def arrived(ref, k, frm):
        copy(ref, ref, k, frm).wait_recv()

    barrier = pltpu.get_barrier_semaphore()
    for to in (peer, xr, xl, zr, zl, dr, dl, ypeer, wtarget(0, 1), wtarget(1, 1)):
        pl.semaphore_signal(barrier, inc=1, device_id=to, device_id_type=MESH)
    for j in range(2):
        @pl.when(jnp.logical_not(jnp.logical_and(own_w, xlow == j)))
        def _():
            pl.semaphore_signal(barrier, inc=1, device_id=wtarget(j, 0), device_id_type=MESH)

    loads = [
        pltpu.make_async_copy(w1_hbm, win.at[0], loc_sem.at[0]),
        pltpu.make_async_copy(w3_hbm, win.at[1], loc_sem.at[1]),
        pltpu.make_async_copy(w2_hbm, win.at[2], loc_sem.at[2]),
        pltpu.make_async_copy(k_hbm, kin, loc_sem.at[3]),
        pltpu.make_async_copy(v_hbm, vin, loc_sem.at[4]),
        pltpu.make_async_copy(s_hbm, sin, loc_sem.at[5]),
        pltpu.make_async_copy(q_hbm, qin, loc_sem.at[6]),
    ]
    for ld in loads:
        ld.start()

    wsend[...] = jnp.zeros_like(wsend)
    for m in range(3):
        loads[m].wait()
    for j in range(2):
        for t in range(2):
            wsend[j, t, 0:PIECE, :] = win[t, :, j * U:(j + 1) * U]
            wsend[j, t, SECOND:SECOND + PIECE, :] = win[2, :, j * U:(j + 1) * U]
    row = lax.broadcasted_iota(jnp.int32, (DC, DC), 0)
    col = lax.broadcasted_iota(jnp.int32, (DC, DC), 1)
    group = (row >= 160).astype(jnp.int32) + (row >= 320).astype(jnp.int32) + (row >= 480).astype(jnp.int32)
    rem = row - 160 * group
    step20 = jnp.zeros_like(rem)
    for t in range(1, NZ):
        step20 = step20 + (rem >= PIECE * t).astype(jnp.int32)
    wanted = ROWS * step20 + PIECE * group + rem - PIECE * step20
    perm[...] = jnp.where(col == wanted, 1.0, 0.0).astype(BF16)

    def gathered_order(v):
        return dot(v, perm[...]).astype(BF16)

    loads[3].wait()
    kbuf[OWN] = gathered_order(kin[...])
    pl.semaphore_wait(barrier, 12 - jnp.where(own_w, 1, 0))

    k_w = ids(4)
    slot = 2 * xlow + y
    w_copies = []
    for j in range(2):
        for dy in (1, 0):
            block = wsend.at[j, y if dy == 0 else 1 - y]
            cp = pltpu.make_async_remote_copy(
                src_ref=block, dst_ref=warr.at[slot],
                send_sem=send_sem.at[k_w + 2 * j + dy], recv_sem=recv_sem.at[k_w + slot],
                device_id=wtarget(j, dy), device_id_type=MESH,
            )
            if dy == 1:
                cp.start()
                sends.append(cp)
            else:
                is_self = jnp.logical_and(own_w, xlow == j)
                w_copies.append((is_self, cp))
                lc = pltpu.make_async_copy(block, warr.at[slot], loc_sem.at[7 + j])
                pl.when(jnp.logical_not(is_self))(cp.start)

                @pl.when(is_self)
                def _():
                    lc.start()
                    lc.wait()

    def x_out(buf, k):
        send(buf.at[OWN], buf.at[LEFT], k, xr)
        send(buf.at[OWN], buf.at[RIGHT], k + 1, xl)

    def x_relay(buf, k):
        arrived(buf.at[LEFT], k, xl)
        send(buf.at[LEFT, 0:HALF], buf.at[OPP, 0:HALF], k + 2, xr)
        arrived(buf.at[RIGHT], k + 1, xr)
        send(buf.at[RIGHT, HALF:TOK], buf.at[OPP, HALF:TOK], k + 3, xl)

    def x_last(buf, k):
        arrived(buf.at[OPP, 0:HALF], k + 2, xl)
        arrived(buf.at[OPP, HALF:TOK], k + 3, xr)

    k_k, k_o, k_q = ids(4), ids(4), ids(4)
    x_out(kbuf, k_k)
    loads[4].wait()
    loads[5].wait()
    diag = lax.broadcasted_iota(jnp.int32, (TOK, TOK), 0) == lax.broadcasted_iota(jnp.int32, (TOK, TOK), 1)
    rate_row = jnp.where(yh == 0, sin[0:1, :], sin[1:2, :])
    rates = jnp.sum(jnp.where(diag, rate_row, 0.0), axis=1, keepdims=True)
    obuf[OWN] = gathered_order((-(rates * vin[...].astype(F32))).astype(BF16))
    x_out(obuf, k_o)
    loads[6].wait()
    qbuf[OWN] = gathered_order(qin[...])

    for s in range(4):
        from_x, from_y = s // 2, s % 2
        here = jnp.logical_and(jnp.logical_and(own_w, xlow == from_x), y == from_y)

        @pl.when(jnp.logical_not(here))
        def _():
            copy(warr.at[s], warr.at[s], k_w + s, ypeer).wait_recv()

    prow = lax.broadcasted_iota(jnp.int32, (ROWS, 4 * PADDED), 0)
    pcol = lax.broadcasted_iota(jnp.int32, (ROWS, 4 * PADDED), 1)
    pgroup = (prow >= 20).astype(jnp.int32) + (prow >= 40).astype(jnp.int32) + (prow >= 60).astype(jnp.int32)
    pfrom = prow + (PADDED - PIECE) * pgroup
    blocks = warr[...].reshape(4 * PADDED, U)
    wg[z, 0] = dot(jnp.where(pcol == pfrom, 1.0, 0.0).astype(BF16), blocks).astype(BF16)
    wg[z, 2] = dot(jnp.where(pcol == pfrom + SECOND, 1.0, 0.0).astype(BF16), blocks).astype(BF16)

    def zpos(off):
        return lax.rem(z + off + 2 * NZ, NZ)

    def chunk(buf, at, kind, h):
        return buf.at[at, 2 * kind, CUT[h][0]:CUT[h][1]]

    def ways(step, kind, h):
        return (0, 1) if step < 4 else (far_way(kind, h),)

    def ring_id(k, step, kind, h, way):
        return k + (step - 1) * 8 + 4 * kind + 2 * h + way

    def ring_send(buf, k, step, kind, h):
        for way in ways(step, kind, h):
            ref = chunk(buf, zpos((1 - step) if way == 0 else (step - 1)), kind, h)
            send(ref, ref, ring_id(k, step, kind, h, way), zr if way == 0 else zl)

    def ring_arrived(buf, k, step, kind, h):
        for way in ways(step, kind, h):
            ref = chunk(buf, zpos(-step if way == 0 else step), kind, h)
            arrived(ref, ring_id(k, step, kind, h, way), zl if way == 0 else zr)

    def offsets(step):
        return ((0,), (-1, 1), (-2, 2), (-3, 3), (4,))[step]

    def pair_send(buf, k, step):
        for i, off in enumerate(offsets(step)):
            at = zpos(off)
            send(buf.at[at, 0], buf.at[at, 1], k + 2 * step + i, ypeer)

    def far_send(buf, k, h):
        at, rows = zpos(-3 if h == 0 else 3), pl.ds(CUT[h][0], CUT[h][1] - CUT[h][0])
        send(buf.at[at, 0, rows], buf.at[at, 1, rows], k + 8 + h, dr if h == 0 else dl)

    def far_arrived(buf, k):
        for h in range(2):
            ring_arrived(buf, k, 4, 0, h)

    def pair_arrived(buf, k):
        for step in range(4):
            for i, off in enumerate(offsets(step)):
                arrived(buf.at[zpos(off), 1], k + 2 * step + i, ypeer)
        for h in range(2):
            arrived(buf.at[zpos(4), 1, CUT[h][0]:CUT[h][1]], k + 8 + h, ypeer)

    def gather(buf, k, k_pair, step):
        for kind, h in CHUNKS:
            if step > 1:
                ring_arrived(buf, k, step - 1, kind, h)
            ring_send(buf, k, step, kind, h)
            if step == 4 and kind == 0:
                far_send(buf, k_pair, h)
            if (kind, h) == (0, 1):
                pair_send(buf, k_pair, step - 1)

    k_g, k_gp = ids(32), ids(10)
    gather(wg, k_g, k_gp, 1)
    gather(wg, k_g, k_gp, 2)
    x_relay(kbuf, k_k)
    gather(wg, k_g, k_gp, 3)
    x_relay(obuf, k_o)
    gather(wg, k_g, k_gp, 4)
    x_out(qbuf, k_q)

    def transposes(h):
        kt[:, h * U:(h + 1) * U] = kbuf[2 * h:2 * h + 2].reshape(2 * TOK, DC).T
        ot[:, h * U:(h + 1) * U] = obuf[2 * h:2 * h + 2].reshape(2 * TOK, DC).T

    transposes(1)
    far_arrived(wg, k_g)

    for h in range(2):
        ring_arrived(wg, k_g, 4, 1, h)
    k_p = ids(12)

    def p_part(b, kind):
        v = dot((obuf if kind == 2 else kbuf)[b], wg[:, kind].reshape(DC, U))
        ps[b, kind] = v
        pb[b, kind] = v.astype(BF16)
        send(pb.at[b, kind], pr.at[b, kind], k_p + 3 * b + kind, peer)

    for b in (OWN, RIGHT, LEFT):
        p_part(b, 0)
        p_part(b, 2)
    x_last(kbuf, k_k)
    p_part(OPP, 0)
    x_last(obuf, k_o)
    p_part(OPP, 2)
    pair_arrived(wg, k_gp)
    for b in (OWN, RIGHT, LEFT, OPP):
        p_part(b, 1)

    transposes(0)

    for b in (OWN, RIGHT, LEFT, OPP):
        for kind in range(3):
            arrived(pr.at[b, kind], k_p + 3 * b + kind, peer)

        @pl.loop(0, TOK // STEP)
        def _(t):
            r = pl.ds(pl.multiple_of(t * STEP, STEP), STEP)
            o = pl.ds(pl.multiple_of(b * TOK + t * STEP, STEP), STEP)
            gate = ps[b, y, r, :] + pr[b, y, r, :].astype(F32)
            up = ps[b, 1 - y, r, :] + pr[b, 1 - y, r, :].astype(F32)
            hg = ps[b, 2, r, :] + pr[b, 2, r, :].astype(F32)
            sg = jax.nn.sigmoid(gate)
            silu = gate * sg
            hid[o, :] = (silu * up).astype(BF16)
            gg[0, o, :] = (hg * up * (sg * (1.0 + gate * (1.0 - sg)))).astype(BF16)
            gg[1, o, :] = (hg * silu).astype(BF16)

    k_ya = ids(10)
    k_r = ids(32)
    far = pl.ds(pl.multiple_of(zpos(4) * ROWS, 16), ROWS)
    def rs_send(step, kind, h, way):
        lo, hi = CUT[h]
        at = zpos((5 - step) if way == 0 else (step - 5))
        v = (ga if kind == 0 else gb)[at, lo:hi]
        if kind == 0 and step > 1:
            v = v + yrecv[at, lo:hi].astype(F32)
        if kind == 0 and step == 2 and h == way:
            arrived(yfar.at[lo:hi], k_ya + 8 + h, dl if way == 0 else dr)
            v = v + yfar[lo:hi].astype(F32)
        if step > 2 or (step == 2 and far_way(kind, h) == way):
            arrived(rsr.at[way, step - 2, kind, lo:hi], ring_id(k_r, step - 1, kind, h, way), zl if way == 0 else zr)
            v = v + rsr[way, step - 2, kind, lo:hi].astype(F32)
        rss[way, step - 1, kind, lo:hi] = v.astype(BF16)
        send(
            rss.at[way, step - 1, kind, lo:hi], rsr.at[way, step - 1, kind, lo:hi],
            ring_id(k_r, step, kind, h, way), zr if way == 0 else zl,
        )

    gb[zpos(4)] = dot(ot[far, :], hid[...])
    for h in range(2):
        rs_send(1, 1, h, far_way(1, h))
    ysend[...] = dot(kt[...], gg[1 - y]).astype(BF16).reshape(NZ, ROWS, U)
    for h in range(2):
        lo, hi = CUT[h]
        send(ysend.at[zpos(4), lo:hi], yfar.at[lo:hi], k_ya + 8 + h, dr if h == 0 else dl)
    for step in (3, 2, 1, 0):
        for i, off in reversed(list(enumerate(offsets(step)))):
            at = zpos(off)
            send(ysend.at[at], yrecv.at[at], k_ya + 2 * step + i, ypeer)
    ga[zpos(4)] = dot(kt[far, :], gg[y])
    for h in range(2):
        rs_send(1, 0, h, far_way(0, h))
    gb[...] = dot(ot[...], hid[...]).reshape(NZ, ROWS, U)
    ga[...] = dot(kt[...], gg[y]).reshape(NZ, ROWS, U)

    for step in range(2, 5):
        for way in range(2):
            for h in range(2):
                rs_send(step, 1, h, way)
        for way, off in enumerate((5 - step, step - 5)):
            arrived(yrecv.at[zpos(off)], k_ya + 2 * (5 - step) + (1 - way), ypeer)
            for h in range(2):
                rs_send(step, 0, h, way)
        if step == 2:
            for m in range(3):
                sms[m:m + 1, :] = square_sums(wg[:, m].reshape(DC, U))
        if step == 3:
            x_relay(qbuf, k_q)

    def total(kind):
        for way in range(2):
            for h in range(2):
                lo, hi = CUT[h]
                arrived(rsr.at[way, 3, kind, lo:hi], ring_id(k_r, 4, kind, h, way), zl if way == 0 else zr)
        return (ga if kind == 0 else gb)[z] + rsr[0, 3, kind].astype(F32) + rsr[1, 3, kind].astype(F32)

    k_yb = ids(1)
    tb = total(1)
    gb[z] = tb
    ybs[...] = tb.astype(BF16)
    send(ybs, ybr, k_yb, ypeer)
    arrived(yrecv.at[z], k_ya, ypeer)
    ta = total(0) + yrecv[z].astype(F32)
    nw[z, 0] = (wg[z, 0].astype(F32) - ta).astype(BF16)
    k_n, k_np = ids(32), ids(10)
    for h in range(2):
        ring_send(nw, k_n, 1, 0, h)
    pair_send(nw, k_np, 0)
    arrived(ybr, k_yb, ypeer)
    nw[z, 2] = (wg[z, 2].astype(F32) - (gb[z] + ybr[...].astype(F32))).astype(BF16)
    for h in range(2):
        ring_send(nw, k_n, 1, 1, h)
    x_last(qbuf, k_q)
    for step in range(2, 5):
        gather(nw, k_n, k_np, step)
    far_arrived(nw, k_n)

    k_qp = ids(8)
    k_s = ids(1)

    def q_part(b, kind):
        qs[b, kind] = dot(qbuf[b], nw[:, kind].reshape(DC, U))
        send(qs.at[b, kind], qr.at[b, kind], k_qp + 2 * b + kind, peer)

    for b in range(4):
        q_part(b, 0)
    for h in range(2):
        ring_arrived(nw, k_n, 4, 1, h)
    sms[3:4, :] = square_sums(nw[:, 0].reshape(DC, U))
    sms[5:6, :] = square_sums(nw[:, 2].reshape(DC, U))
    sms[6:8, :] = jnp.zeros((2, U), F32)
    wout[...] = dot(perm[...], nw[:, 2].reshape(DC, U)).astype(BF16)
    pair_arrived(nw, k_np)
    q_part(OPP, 1)
    sms[4:5, :] = square_sums(nw[:, 1].reshape(DC, U))
    send(sms, smr, k_s, peer)
    q_part(LEFT, 1)
    q_part(RIGHT, 1)
    q_part(OWN, 1)
    arrived(smr, k_s, peer)
    sums = sms[...] + smr[...]
    ra, rb, r2 = [jnp.sqrt((sums[m:m + 1] + EPS) / (sums[3 + m:4 + m] + EPS)) for m in range(3)]
    r1, r3 = jnp.where(y == 0, ra, rb), jnp.where(y == 0, rb, ra)

    def out_part(b):
        for kind in range(2):
            arrived(qr.at[b, kind], k_qp + 2 * b + kind, peer)

        @pl.loop(0, TOK // STEP)
        def _(t):
            r = pl.ds(pl.multiple_of(t * STEP, STEP), STEP)
            qg = (qs[b, y, r, :] + qr[b, y, r, :]) * r1
            qu = (qs[b, 1 - y, r, :] + qr[b, 1 - y, r, :]) * r3
            qh[b, r, :] = (qg * jax.nn.sigmoid(qg) * qu * r2).astype(BF16)

        return dot_nt(qh[b], wout[...])

    k_x = ids(6)
    part = out_part(OPP)
    ob[OPP] = part.astype(BF16)
    send(ob.at[OPP, 0:HALF], obr.at[0:HALF], k_x, xr)
    send(ob.at[OPP, HALF:TOK], obr.at[HALF:TOK], k_x + 1, xl)
    part = out_part(LEFT)
    ob[LEFT, 0:HALF] = part[0:HALF].astype(BF16)
    send(ob.at[LEFT, 0:HALF], fin.at[1, 0:HALF], k_x + 2, xl)
    op[0] = part[HALF:TOK]
    part = out_part(RIGHT)
    ob[RIGHT, HALF:TOK] = part[HALF:TOK].astype(BF16)
    send(ob.at[RIGHT, HALF:TOK], fin.at[0, HALF:TOK], k_x + 4, xr)
    op[1] = part[0:HALF]
    arrived(obr.at[HALF:TOK], k_x + 1, xr)
    ob[LEFT, HALF:TOK] = (op[0] + obr[HALF:TOK].astype(F32)).astype(BF16)
    send(ob.at[LEFT, HALF:TOK], fin.at[1, HALF:TOK], k_x + 3, xl)
    arrived(obr.at[0:HALF], k_x, xl)
    ob[RIGHT, 0:HALF] = (op[1] + obr[0:HALF].astype(F32)).astype(BF16)
    send(ob.at[RIGHT, 0:HALF], fin.at[0, 0:HALF], k_x + 5, xr)
    part = out_part(OWN)
    arrived(fin.at[1, 0:HALF], k_x + 2, xr)
    arrived(fin.at[1, HALF:TOK], k_x + 3, xr)
    arrived(fin.at[0, HALF:TOK], k_x + 4, xl)
    arrived(fin.at[0, 0:HALF], k_x + 5, xl)
    out_ref[...] = (part + fin[0].astype(F32) + fin[1].astype(F32)).astype(BF16)

    for cp in sends:
        cp.wait_send()
    for is_self, cp in w_copies:
        pl.when(jnp.logical_not(is_self))(cp.wait_send)


N_SEM = 4 + 12 + 42 + 12 + 42 + 1 + 42 + 9 + 6


def body(keys, values, queries, step_size, gate_weight, up_weight, down_weight):
    hbm = pl.BlockSpec(memory_space=pl.ANY)
    return pl.pallas_call(
        kernel,
        out_shape=jax.ShapeDtypeStruct((TOK, DC), BF16),
        in_specs=[hbm] * 7,
        out_specs=pl.BlockSpec(memory_space=pltpu.VMEM),
        scratch_shapes=[
            pltpu.VMEM((3, PIECE, 2 * U), BF16),
            pltpu.VMEM((TOK, DC), BF16),
            pltpu.VMEM((TOK, DC), BF16),
            pltpu.VMEM((TOK, DC), BF16),
            pltpu.VMEM((2, TOK), F32),
            pltpu.VMEM((2, 2, PADDED, U), BF16),
            pltpu.VMEM((4, PADDED, U), BF16),
            pltpu.VMEM((NZ, 3, ROWS, U), BF16),
            pltpu.VMEM((DC, DC), BF16),
            pltpu.VMEM((DC, U), BF16),
            pltpu.VMEM((4, TOK, DC), BF16),
            pltpu.VMEM((4, TOK, DC), BF16),
            pltpu.VMEM((4, TOK, DC), BF16),
            pltpu.VMEM((DC, 4 * TOK), BF16),
            pltpu.VMEM((DC, 4 * TOK), BF16),
            pltpu.VMEM((4, 3, TOK, U), F32),
            pltpu.VMEM((4, 3, TOK, U), BF16),
            pltpu.VMEM((4, 3, TOK, U), BF16),
            pltpu.VMEM((2, 4 * TOK, U), BF16),
            pltpu.VMEM((4 * TOK, U), BF16),
            pltpu.VMEM((NZ, ROWS, U), F32),
            pltpu.VMEM((NZ, ROWS, U), F32),
            pltpu.VMEM((ROWS, U), BF16),
            pltpu.VMEM((NZ, ROWS, U), BF16),
            pltpu.VMEM((NZ, ROWS, U), BF16),
            pltpu.VMEM((2, 4, 2, ROWS, U), BF16),
            pltpu.VMEM((2, 4, 2, ROWS, U), BF16),
            pltpu.VMEM((ROWS, U), BF16),
            pltpu.VMEM((ROWS, U), BF16),
            pltpu.VMEM((NZ, 3, ROWS, U), BF16),
            pltpu.VMEM((8, U), F32),
            pltpu.VMEM((8, U), F32),
            pltpu.VMEM((4, 2, TOK, U), F32),
            pltpu.VMEM((4, 2, TOK, U), F32),
            pltpu.VMEM((4, TOK, U), BF16),
            pltpu.VMEM((4, TOK, DC), BF16),
            pltpu.VMEM((2, HALF, DC), F32),
            pltpu.VMEM((TOK, DC), BF16),
            pltpu.VMEM((2, TOK, DC), BF16),
            pltpu.SemaphoreType.DMA((N_SEM,)),
            pltpu.SemaphoreType.DMA((N_SEM,)),
            pltpu.SemaphoreType.DMA((9,)),
        ],
        compiler_params=pltpu.CompilerParams(
            collective_id=0, has_side_effects=True, vmem_limit_bytes=60 << 20
        ),
        name="ttt_layer",
    )(keys, values, queries, step_size.T, gate_weight, up_weight, down_weight)


def solution(mesh):
    finer = Mesh(mesh.devices.reshape(2, 2, 4, 2, 8), ("yh", "core", "x", "yl", "z"))
    seq, head = ("x", "yl", "z"), ("yh", "core")
    placed = (
        P(seq, head), P(seq, head), P(seq, head), P(seq, None),
        P(seq, head), P(seq, head), P(seq, head),
    )
    return jax.shard_map(body, mesh=finer, in_specs=placed, out_specs=P(seq, head), check_vma=False)
```
